512 devices in a mesh: smp: 32 (over y, z_lo), var: 16 (over x, z_hi, core).
Axes of the slice: x: 4, y: 4, z: 16 (z_hi: 2, z_lo: 8; z = z_hi * 8 + z_lo), core: 2. Of those that a mesh axis runs over, the one named last changes fastest.
Arguments:
- dosage: int32 [2048, 8192], P('smp', 'var'), may hold values from -2147483648 to 2147483647, as said below
- shares_init: float32 [12, 32768], P(None, ('smp', 'var')), may hold values from 0.1 to 1
- freqs_init: float32 [12, 8192], P(None, ('var', 'smp')), may hold values from 0.019 to 0.981
Outputs:
- shares: float32 [12, 32768], P(None, ('smp', 'var'))
- freqs: float32 [12, 8192], P(None, ('var', 'smp'))
The draws below stay inside these ranges and needn't reach their ends.
Inputs may be any that keep to these rules, and one draw needn't show every extreme that they name: Every 2-bit code in a word of dosage is 0, 1, 2 or 3, and 3 marks a missing genotype.
All inputs are finite; a program needn't handle non-finite values.
Results may differ from the reference program's by a relative error of at most 0.0003.
Values sent between devices are 32-bit elements; how exact they have to be, the bound alone decides.
No kernel may reach another device: no remote copies, remote signals or barrier semaphores. Data moves between devices by JAX's collectives and lax.ppermute only.
A program may use at most 64 MiB of HBM per device.

```python
import math
import jax
import jax.numpy as jnp
from jax import lax

K = 12
ITERS = 2
R_DEV = 1024
N = 32768
M = 8192


def planted_weights(key):
    weight_key = jax.random.fold_in(key, 201)
    cube_base = jax.random.randint(jax.random.fold_in(weight_key, 1), (K, N), 0, 16, dtype=jnp.int32)
    leading = jax.random.randint(jax.random.fold_in(weight_key, 2), (N,), 0, K, dtype=jnp.int32)
    boost = jnp.where(jnp.arange(K, dtype=jnp.int32)[:, None] == leading[None, :], 20000, 0)
    return cube_base * cube_base * cube_base + 1 + boost


def planted_levels(key):
    level_key = jax.random.fold_in(key, 202)
    spread = jax.random.randint(jax.random.fold_in(level_key, 1), (K, M), 0, 992, dtype=jnp.int32)
    flipped = jax.random.randint(jax.random.fold_in(level_key, 2), (K, M), 0, 2, dtype=jnp.int32)
    lower = 16 + spread * spread // 992
    return jnp.where(flipped == 1, 1024 - lower, lower)


def draw_dosage(key, part):
    weights = planted_weights(key)
    levels = planted_levels(key)
    grouped = weights.reshape(K, N // 16, 16)
    genotype_key = jax.random.fold_in(key, 203)

    def add_codes(position, packed):
        picked = lax.dynamic_index_in_dim(grouped, position, 2, keepdims=False)
        numerator = jnp.dot(picked.T, levels)
        denominator = jnp.sum(picked, axis=0) * 1024
        sample_key = jax.random.fold_in(genotype_key, position)
        limit = jnp.broadcast_to(denominator[:, None], numerator.shape)
        first_draw = jax.random.randint(jax.random.fold_in(sample_key, 1), numerator.shape, 0, limit, dtype=jnp.int32)
        second_draw = jax.random.randint(jax.random.fold_in(sample_key, 2), numerator.shape, 0, limit, dtype=jnp.int32)
        alleles = (first_draw < numerator).astype(jnp.int32) + (second_draw < numerator).astype(jnp.int32)
        absent = jax.random.randint(jax.random.fold_in(sample_key, 3), numerator.shape, 0, 10, dtype=jnp.int32) == 0
        codes = jnp.where(absent, 3, alleles)
        return jnp.bitwise_or(packed, jnp.left_shift(codes, 2 * position))
    return lax.fori_loop(0, 16, add_codes, jnp.zeros((N // 16, M), jnp.int32))


def draw_freqs_init(key, part):
    levels = planted_levels(key)
    base = levels.astype(jnp.float32) / 1024.0
    noise = jax.random.uniform(jax.random.fold_in(key, 204), (K, M), jnp.float32, 0.05, 0.95)
    return 0.9 * base + 0.1 * noise


def shard_levels(stream_key, dims, cuts, least, high):
    def one(dim, parts):
        heights = jax.random.uniform(jax.random.fold_in(jax.random.fold_in(stream_key, 6), dim), (parts,), jnp.float32, least / len(cuts), high / len(cuts))
        return jnp.repeat(jnp.exp(heights), dims[dim] // parts).reshape((-1,) + (1,) * (len(dims) - dim - 1))

    loudness = one(*cuts[0])
    for cut in cuts[1:]:
        loudness = loudness * one(*cut)
    return loudness


def setup_inputs(seed: int = 0) -> dict:
    key_list = jax.random.split(jax.random.key(seed), 4)
    dosage = draw_dosage(jax.random.fold_in(key_list[3], 71), 0)
    shares_init = jnp.clip(jnp.exp(math.log(1.0) - 2.3025851 * jax.random.uniform(key_list[1], (K, N), jnp.float32) ** shard_levels(key_list[1], (K, N), ((1, 512),), -0.2, 0.2)), 0.1, 1.0)
    freqs_init = draw_freqs_init(jax.random.fold_in(key_list[3], 71), 0)
    return dict(dosage=dosage, shares_init=shares_init, freqs_init=freqs_init)


HIGH = lax.Precision.HIGHEST


def unpack_codes(packed):
    shifts = 2 * jnp.arange(16, dtype=jnp.int32)
    codes = jnp.bitwise_and(jnp.right_shift(packed[:, None, :], shifts[None, :, None]), 3)
    return codes.reshape(packed.shape[0] * 16, packed.shape[1])


def expect_sums(packed, shares_block, freqs_block):
    codes = unpack_codes(packed)
    live = (codes < 3).astype(jnp.float32)
    allele_f = live * codes.astype(jnp.float32)
    probs = jnp.einsum("kn,km->nm", shares_block, freqs_block, precision=HIGH)
    ratio_alt = allele_f / probs
    ratio_ref = (2.0 * live - allele_f) / (1.0 - probs)
    sum_q = jnp.einsum("km,nm->kn", freqs_block, ratio_alt, precision=HIGH) + jnp.einsum("km,nm->kn", 1.0 - freqs_block, ratio_ref, precision=HIGH)
    sum_a = jnp.einsum("kn,nm->km", shares_block, ratio_alt, precision=HIGH)
    sum_b = jnp.einsum("kn,nm->km", shares_block, ratio_ref, precision=HIGH)
    return sum_q, sum_a, sum_b


def renew_shares(shares_block, sum_q):
    numer = shares_block * sum_q
    return (numer + 0.5) / (jnp.sum(numer, axis=0, keepdims=True) + 0.5 * shares_block.shape[0])


def renew_freqs(freqs_block, sum_a, sum_b):
    alt_part = freqs_block * sum_a
    ref_part = (1.0 - freqs_block) * sum_b
    return (alt_part + 0.5) / (alt_part + ref_part + 1.0)


def reference(dosage, shares_init, freqs_init):
    shares_now = shares_init / jnp.sum(shares_init, axis=0, keepdims=True)
    freqs_now = freqs_init
    blocks = dosage.shape[0] * 16 // R_DEV
    packed_blocks = dosage.reshape(blocks, R_DEV // 16, dosage.shape[1])
    for iteration in range(ITERS):
        share_blocks = shares_now.reshape(K, blocks, R_DEV).transpose(1, 0, 2)

        def one_block(carry, items):
            sum_q, sum_a, sum_b = expect_sums(items[0], items[1], freqs_now)
            return (carry[0] + sum_a, carry[1] + sum_b), sum_q

        start = (jnp.zeros(freqs_now.shape, jnp.float32), jnp.zeros(freqs_now.shape, jnp.float32))
        totals, sums_q = lax.scan(one_block, start, (packed_blocks, share_blocks))
        sum_q = sums_q.transpose(1, 0, 2).reshape(K, shares_now.shape[1])
        new_shares = renew_shares(shares_now, sum_q)
        freqs_now = renew_freqs(freqs_now, totals[0], totals[1])
        shares_now = new_shares
    return shares_now, freqs_now
```

```python
import jax
import jax.numpy as jnp
from jax import lax
from jax.experimental import pallas as pl
from jax.experimental.pallas import tpu as pltpu
from jax.sharding import Mesh, PartitionSpec as P

K = 12
PAD = 16
LANES = 128
ROWS = 256

AXES = ("y", "zl", "x", "zh", "c")
SIZES = (4, 8, 4, 2, 2)
SMP = ("y", "zl")
VAR = ("x", "zh", "c")
NEAR = ("y", "x", "c")
FAR = ("zl", "zh")
N_SMP, N_VAR, N_NEAR, N_FAR = 32, 16, 32, 16
N_Y, N_XC, N_ZL, N_ZH = 4, 8, 8, 2

f32 = jnp.float32
bf16 = jnp.bfloat16


def tile(i):
    return slice(i * LANES, (i + 1) * LANES)


def lane():
    return lax.broadcasted_iota(jnp.int32, (8, LANES), 1)


def roll(x, shift):
    shift = shift % LANES
    return pltpu.roll(x, shift, 1) if shift else x


def two_parts(x):
    high = x.astype(bf16)
    return high, (x - high.astype(f32)).astype(bf16)


def three_parts(x):
    high = x.astype(bf16)
    return (high, *two_parts(x - high.astype(f32)))


def dot(a, b, over_a, over_b):
    return lax.dot_general(
        a, b, (((over_a,), (over_b,)), ((), ())), preferred_element_type=f32
    )


def fold(x):
    return x[:PAD] + x[PAD:]


def block_sums(dosage_ref, shares, freqs):
    qh, qm, ql = three_parts(shares)
    fh, fm, fl = three_parts(freqs)
    q_side = jnp.concatenate([qh, qh, qm, qh, ql, qm], 0)
    f_side = jnp.concatenate([fh, fm, fh, fl, fh, fm], 0)
    q_two = jnp.concatenate([qh, qm], 0)
    f_two = jnp.concatenate([fh, fm], 0)
    g_two = jnp.concatenate(two_parts(1.0 - freqs), 0)
    shift = 2 * lax.broadcasted_iota(jnp.int32, (16, freqs.shape[1]), 0)
    sums_q, sum_a, sum_b = [], None, None
    for at in range(0, shares.shape[1], ROWS):
        probs = dot(q_side[:, at : at + ROWS], f_side, 0, 0)
        codes = jnp.concatenate(
            [
                jnp.bitwise_and(
                    jnp.right_shift(jnp.broadcast_to(dosage_ref[w : w + 1, :], shift.shape), shift), 3
                )
                for w in range(at // 16, (at + ROWS) // 16)
            ],
            0,
        )
        rest = 1.0 - probs
        inverse = jnp.where(codes < 3, 1.0 / (probs * rest), 0.0)
        allele = codes.astype(f32)
        ah, al = two_parts(allele * (rest * inverse))
        bh, bl = two_parts((2.0 - allele) * (probs * inverse))
        sums_q.append(
            dot(f_two, ah, 1, 1) + dot(f_two, al, 1, 1) + dot(g_two, bh, 1, 1) + dot(g_two, bl, 1, 1)
        )
        q_part = q_two[:, at : at + ROWS]
        part_a = dot(q_part, ah, 1, 0) + dot(q_part, al, 1, 0)
        part_b = dot(q_part, bh, 1, 0) + dot(q_part, bl, 1, 0)
        sum_a = part_a if sum_a is None else sum_a + part_a
        sum_b = part_b if sum_b is None else sum_b + part_b
    return fold(jnp.concatenate(sums_q, 1)), fold(sum_a), fold(sum_b)


def first_kernel(shares_ref, freqs_ref, v_out, s_out, q_tmp, f_tmp):
    raw = shares_ref[...]
    own = raw / jnp.sum(raw, axis=0, keepdims=True)
    q_tmp[...] = jnp.zeros_like(q_tmp)
    f_tmp[...] = jnp.zeros_like(f_tmp)
    q_tmp[:, 0:64] = own[0:8]
    q_tmp[0:4, 64:128] = own[8:12]
    f_tmp[:, 0:16] = freqs_ref[0:8, :]
    f_tmp[0:4, 16:32] = freqs_ref[8:12, :]
    for i in range(N_VAR):
        v_out[i] = q_tmp[...]
    for i in range(N_SMP):
        s_out[i] = f_tmp[...]


def shares_of(v_in):
    low, high = [], []
    left = lane() < 64
    for t in range(8):
        a, b = v_in[2 * t], v_in[2 * t + 1]
        low.append(jnp.where(left, a, roll(b, 64)))
        high.append(jnp.where(left, roll(a, 64), b))
    return jnp.concatenate([jnp.concatenate(low, 1), jnp.concatenate(high, 1)], 0)


def freqs_of(s_in):
    low, high = [], []
    place = lane() // 16
    for t in range(4):
        lo = hi = jnp.zeros((8, LANES), f32)
        for i in range(8):
            a = s_in[8 * t + i]
            lo = jnp.where(place == i, roll(a, 16 * i), lo)
            hi = jnp.where(place == i, roll(a, 16 * i - 16), hi)
        low.append(lo)
        high.append(hi)
    return jnp.concatenate([jnp.concatenate(low, 1), jnp.concatenate(high, 1)], 0)


def one_kernel(dosage_ref, v_in, s_in, slots, q_out, f_out, sq_tmp, sa_tmp):
    shares = shares_of(v_in)
    freqs = freqs_of(s_in)
    q_out[...] = shares
    f_out[...] = freqs
    sum_q, sum_a, sum_b = block_sums(dosage_ref, shares, freqs)
    sq_tmp[...] = sum_q
    sa_tmp[0:12] = sum_a[0:12]
    sa_tmp[12:24] = sum_b[0:12]
    slots[...] = jnp.zeros_like(slots)
    for s in range(N_NEAR):
        t, q = divmod(s, 4)
        slots[s, 0:3] = sq_tmp[3 * q : 3 * q + 3, tile(t)]
        t, g = divmod(s, 8)
        slots[s, 3:6] = sa_tmp[3 * g : 3 * g + 3, tile(t)]


def near_sums_kernel(idx, near_in, far_out, q_out, a_tmp):
    for y in range(N_Y):
        q_out[3 * y : 3 * y + 3] = sum(near_in[y * N_XC + g] for g in range(N_XC))[0:3]
    q_out[12:24] = jnp.zeros((12, LANES), f32)
    for g in range(N_XC):
        a_tmp[3 * g : 3 * g + 3] = sum(near_in[y * N_XC + g] for y in range(N_Y))[3:6]
    for h in range(N_ZH):
        sent = jnp.where(idx[3] == h, a_tmp[...], q_out[...])
        for i in range(N_ZL):
            far_out[i * N_ZH + h] = sent


def far_sums_kernel(idx, far_in, q_in, near_out, q_tmp, a_tmp):
    zh = idx[3]
    a_tmp[...] = sum(far_in[i * N_ZH + zh] for i in range(N_ZL))
    q_tmp[...] = q_in[...] + far_in[idx[2] * N_ZH + 1 - zh]
    near_out[...] = jnp.zeros_like(near_out)
    for y in range(N_Y):
        for g in range(N_XC):
            near_out[y * N_XC + g, 0:3] = q_tmp[3 * y : 3 * y + 3]
            near_out[y * N_XC + g, 3:6] = a_tmp[3 * g : 3 * g + 3]


def two_kernel(idx, dosage_ref, near_in, q_in, f_in, v_out, s_out, own_q, own_f, sq_tmp, sa_tmp, q_tmp, f_tmp):
    for s in range(N_NEAR):
        t, q = divmod(s, 4)
        sq_tmp[3 * q : 3 * q + 3, tile(t)] = near_in[s, 0:3]
        t, g = divmod(s, 8)
        sa_tmp[3 * g : 3 * g + 3, tile(t)] = near_in[s, 3:6]
    q_tmp[...] = q_in[...]
    f_tmp[...] = f_in[...]
    numer = q_tmp[0:12] * sq_tmp[0:12]
    q_tmp[0:12] = (numer + 0.5) / (jnp.sum(numer, axis=0, keepdims=True) + 0.5 * K)
    old = f_tmp[0:12]
    alt_part = old * sa_tmp[0:12]
    f_tmp[0:12] = (alt_part + 0.5) / (alt_part + (1.0 - old) * sa_tmp[12:24] + 1.0)

    left = lane() < 64
    t = pl.multiple_of(idx[0] // 2 * LANES, LANES)
    a, b = q_tmp[0:8, pl.ds(t, LANES)], q_tmp[8:16, pl.ds(t, LANES)]
    own_q[...] = jnp.where(
        idx[0] % 2 == 0, jnp.where(left, a, roll(b, 64)), jnp.where(left, roll(a, 64), b)
    )
    t = pl.multiple_of(idx[1] // 8 * LANES, LANES)
    a, b = f_tmp[0:8, pl.ds(t, LANES)], f_tmp[8:16, pl.ds(t, LANES)]
    back = LANES - 16 * (idx[1] % 8)
    own_f[...] = jnp.where(lane() < 16, pltpu.roll(a, back, 1), pltpu.roll(b, back + 16, 1))

    sum_q, sum_a, sum_b = block_sums(dosage_ref, q_tmp[...], f_tmp[...])
    for t in range(8):
        a, b = sum_q[0:8, tile(t)], sum_q[8:16, tile(t)]
        v_out[2 * t] = jnp.where(left, a, roll(b, 64))
        v_out[2 * t + 1] = jnp.where(left, roll(a, 64), b)
    place = lane() // 16
    for t in range(4):
        for i in range(8):
            got = roll(sum_a[0:8, tile(t)], -16 * i)
            got = jnp.where(place == 1, roll(sum_a[8:16, tile(t)], 16 - 16 * i), got)
            got = jnp.where(place == 2, roll(sum_b[0:8, tile(t)], 32 - 16 * i), got)
            s_out[8 * t + i] = jnp.where(place == 3, roll(sum_b[8:16, tile(t)], 48 - 16 * i), got)


def last_kernel(v_in, s_in, own_q, own_f, shares_out, freqs_out):
    row = lax.broadcasted_iota(jnp.int32, (8, LANES), 0)
    held = (lane() < 64) | (row < 4)
    sum_q = sum(v_in[i] for i in range(N_VAR))
    numer = jnp.where(held, own_q[...] * sum_q, 0.0)
    total = jnp.sum(numer, axis=0, keepdims=True)
    total = total + pltpu.roll(total, 64, 1)
    new = (numer + 0.5) / (total + 0.5 * K)
    shares_out[0:8] = new[:, 0:64]
    shares_out[8:12] = new[0:4, 64:128]
    sums = sum(s_in[i] for i in range(N_SMP))
    alt_part = own_f[...] * sums
    ref_part = (1.0 - own_f[...]) * roll(sums, -32)
    new = (alt_part + 0.5) / (alt_part + ref_part + 1.0)
    freqs_out[0:8] = new[:, 0:16]
    freqs_out[8:12] = new[0:4, 16:32]


def f32s(*shape):
    return jax.ShapeDtypeStruct(shape, f32)


def vmem(*shape):
    return pltpu.VMEM(shape, f32)


def call(kernel, scalars, n_in, outs, scratch):
    spec = pl.BlockSpec(memory_space=pltpu.VMEM)
    return pl.pallas_call(
        kernel,
        in_specs=[pl.BlockSpec(memory_space=pltpu.SMEM)] * scalars + [spec] * n_in,
        out_specs=[spec] * len(outs),
        out_shape=outs,
        scratch_shapes=scratch,
    )


def exchange(x, axes):
    return lax.all_to_all(x, axes, 0, 0, tiled=True)


def body(dosage, shares_init, freqs_init):
    idx = jnp.stack(
        [lax.axis_index(VAR), lax.axis_index(SMP), lax.axis_index("zl"), lax.axis_index("zh")]
    ).astype(jnp.int32)
    samples, variants = 16 * dosage.shape[0], dosage.shape[1]
    tiles = lambda n: f32s(n, 8, LANES)
    v_slots, s_slots = call(
        first_kernel, 0, 2, [tiles(N_VAR), tiles(N_SMP)], [vmem(8, LANES), vmem(8, LANES)]
    )(shares_init, freqs_init)
    v_got = exchange(v_slots, VAR)
    s_got = exchange(s_slots, SMP)
    slots, shares, freqs = call(
        one_kernel, 0, 3, [tiles(N_NEAR), f32s(PAD, samples), f32s(PAD, variants)],
        [vmem(PAD, samples), vmem(24, variants)],
    )(dosage, v_got, s_got)
    near_got = exchange(slots, NEAR)
    far_slots, own_sum = call(
        near_sums_kernel, 1, 1, [f32s(N_FAR, 24, LANES), f32s(24, LANES)], [vmem(24, LANES)]
    )(idx, near_got)
    far_got = exchange(far_slots, FAR)
    (near_slots,) = call(
        far_sums_kernel, 1, 2, [tiles(N_NEAR)], [vmem(24, LANES), vmem(24, LANES)]
    )(idx, far_got, own_sum)
    near_got = exchange(near_slots, NEAR)
    v_slots, s_slots, own_q, own_f = call(
        two_kernel, 1, 4, [tiles(N_VAR), tiles(N_SMP), f32s(8, LANES), f32s(8, LANES)],
        [vmem(PAD, samples), vmem(24, variants), vmem(PAD, samples), vmem(PAD, variants)],
    )(idx, dosage, near_got, shares, freqs)
    v_got = exchange(v_slots, VAR)
    s_got = exchange(s_slots, SMP)
    return tuple(
        call(last_kernel, 0, 4, [f32s(*shares_init.shape), f32s(*freqs_init.shape)], [])(
            v_got, s_got, own_q, own_f
        )
    )


def solution(mesh):
    fine = Mesh(mesh.devices.reshape(SIZES), AXES)
    return jax.shard_map(
        body,
        mesh=fine,
        in_specs=(P(SMP, VAR), P(None, SMP + VAR), P(None, VAR + SMP)),
        out_specs=(P(None, SMP + VAR), P(None, VAR + SMP)),
        check_vma=False,
    )
```

```python
import jax
import jax.numpy as jnp
from jax import lax
from jax.experimental import pallas as pl
from jax.experimental.pallas import tpu as pltpu
from jax.sharding import Mesh, PartitionSpec as P

K = 12
PAD = 16
LANES = 128
ROWS = 256

AXES = ("y", "zl", "x", "zh", "c")
SIZES = (4, 8, 4, 2, 2)
SMP = ("y", "zl")
VAR = ("x", "zh", "c")
NEAR = ("y", "x", "c")
FAR = ("zl", "zh")
N_SMP, N_VAR, N_NEAR, N_FAR = 32, 16, 32, 16
N_Y, N_XC, N_ZL, N_ZH = 4, 8, 8, 2

f32 = jnp.float32
bf16 = jnp.bfloat16


def tile(i):
    return slice(i * LANES, (i + 1) * LANES)


def var_of(idx):
    return idx[0] & 15


def smp_of(idx):
    return idx[0] >> 4


def zl_of(idx):
    return (idx[0] >> 4) & 7


def zh_of(idx):
    return (idx[0] >> 1) & 1


def lane():
    return lax.broadcasted_iota(jnp.int32, (8, LANES), 1)


def roll(x, shift):
    shift = shift % LANES
    return pltpu.roll(x, shift, 1) if shift else x


def two_parts(x):
    high = x.astype(bf16)
    return high, (x - high.astype(f32)).astype(bf16)


def three_parts(x):
    high = x.astype(bf16)
    return (high, *two_parts(x - high.astype(f32)))


def dot(a, b, over_a, over_b):
    return lax.dot_general(
        a, b, (((over_a,), (over_b,)), ((), ())), preferred_element_type=f32
    )


def fold(x):
    return x[:PAD] + x[PAD:]


def block_sums(dosage_ref, shares, freqs):
    qh, qm, ql = three_parts(shares)
    fh, fm, fl = three_parts(freqs)
    q_side = jnp.concatenate([qh, qh, qm, qh, ql, qm], 0)
    f_side = jnp.concatenate([fh, fm, fh, fl, fh, fm], 0)
    q_two = jnp.concatenate([qh, qm], 0)
    f_two = jnp.concatenate([fh, fm], 0)
    g_two = jnp.concatenate(two_parts(1.0 - freqs), 0)
    shift = 2 * lax.broadcasted_iota(jnp.int32, (16, freqs.shape[1]), 0)
    sums_q, sum_a, sum_b = [], None, None
    for at in range(0, shares.shape[1], ROWS):
        probs = dot(q_side[:, at : at + ROWS], f_side, 0, 0)
        codes = jnp.concatenate(
            [
                jnp.bitwise_and(
                    jnp.right_shift(jnp.broadcast_to(dosage_ref[w : w + 1, :], shift.shape), shift), 3
                )
                for w in range(at // 16, (at + ROWS) // 16)
            ],
            0,
        )
        rest = 1.0 - probs
        inverse = jnp.where(codes < 3, 1.0 / (probs * rest), 0.0)
        allele = codes.astype(f32)
        ah, al = two_parts(allele * (rest * inverse))
        bh, bl = two_parts((2.0 - allele) * (probs * inverse))
        sums_q.append(
            dot(f_two, ah, 1, 1) + dot(f_two, al, 1, 1) + dot(g_two, bh, 1, 1) + dot(g_two, bl, 1, 1)
        )
        q_part = q_two[:, at : at + ROWS]
        part_a = dot(q_part, ah, 1, 0) + dot(q_part, al, 1, 0)
        part_b = dot(q_part, bh, 1, 0) + dot(q_part, bl, 1, 0)
        sum_a = part_a if sum_a is None else sum_a + part_a
        sum_b = part_b if sum_b is None else sum_b + part_b
    return fold(jnp.concatenate(sums_q, 1)), fold(sum_a), fold(sum_b)


def first_kernel(idx, shares_ref, freqs_ref, v_out, s_out, q_tmp, f_tmp):
    raw = shares_ref[...]
    own = raw / jnp.sum(raw, axis=0, keepdims=True)
    q_tmp[...] = jnp.zeros_like(q_tmp)
    f_tmp[...] = jnp.zeros_like(f_tmp)
    q_tmp[:, 0:64] = own[0:8]
    q_tmp[0:4, 64:128] = own[8:12]
    for j in range(3):
        f_tmp[0:4, 16 * j : 16 * j + 16] = freqs_ref[4 * j : 4 * j + 4, :]
    turned = pltpu.roll(f_tmp[...], 16 * zl_of(idx), 1)[0:4]
    for i in range(N_VAR):
        v_out[i] = q_tmp[...]
    for i in range(N_SMP):
        s_out[i] = turned


def shares_of(v_in):
    low, high = [], []
    left = lane() < 64
    for t in range(8):
        a, b = v_in[2 * t], v_in[2 * t + 1]
        low.append(jnp.where(left, a, roll(b, 64)))
        high.append(jnp.where(left, roll(a, 64), b))
    return jnp.concatenate([jnp.concatenate(low, 1), jnp.concatenate(high, 1)], 0)


def block_of_lane():
    return lax.broadcasted_iota(jnp.int32, (4, LANES), 1) // 16


def freqs_of(s_in):
    tiles = []
    block = block_of_lane()
    for t in range(4):
        rows = []
        for j in range(3):
            got = s_in[8 * t]
            for i in range(1, 8):
                got = jnp.where(block == (i + j) % 8, s_in[8 * t + i], got)
            rows.append(roll(got, -16 * j))
        tiles.append(jnp.concatenate(rows + [jnp.zeros((4, LANES), f32)], 0))
    return jnp.concatenate(tiles, 1)


def one_kernel(dosage_ref, v_in, s_in, slots, q_out, f_out, sq_tmp, sa_tmp):
    shares = shares_of(v_in)
    freqs = freqs_of(s_in)
    q_out[...] = shares
    f_out[...] = freqs
    sum_q, sum_a, sum_b = block_sums(dosage_ref, shares, freqs)
    sq_tmp[...] = sum_q
    sa_tmp[0:12] = sum_a[0:12]
    sa_tmp[12:24] = sum_b[0:12]
    slots[...] = jnp.zeros_like(slots)
    for s in range(N_NEAR):
        t, q = divmod(s, 4)
        slots[s, 0:3] = sq_tmp[3 * q : 3 * q + 3, tile(t)]
        t, g = divmod(s, 8)
        slots[s, 3:6] = sa_tmp[3 * g : 3 * g + 3, tile(t)]


def near_sums_kernel(idx, near_in, far_out, q_out, a_tmp):
    for y in range(N_Y):
        q_out[3 * y : 3 * y + 3] = sum(near_in[y * N_XC + g] for g in range(N_XC))[0:3]
    q_out[12:24] = jnp.zeros((12, LANES), f32)
    for g in range(N_XC):
        a_tmp[3 * g : 3 * g + 3] = sum(near_in[y * N_XC + g] for y in range(N_Y))[3:6]
    for h in range(N_ZH):
        sent = jnp.where(zh_of(idx) == h, a_tmp[...], q_out[...])
        for i in range(N_ZL):
            far_out[i * N_ZH + h] = sent


def far_sums_kernel(idx, far_in, q_in, near_out, q_tmp, a_tmp):
    zh = zh_of(idx)
    a_tmp[...] = sum(far_in[i * N_ZH + zh] for i in range(N_ZL))
    q_tmp[...] = q_in[...] + far_in[zl_of(idx) * N_ZH + 1 - zh]
    near_out[...] = jnp.zeros_like(near_out)
    for y in range(N_Y):
        for g in range(N_XC):
            near_out[y * N_XC + g, 0:3] = q_tmp[3 * y : 3 * y + 3]
            near_out[y * N_XC + g, 3:6] = a_tmp[3 * g : 3 * g + 3]


def two_kernel(idx, dosage_ref, near_in, q_in, f_in, v_out, s_out, own_q, own_f, sq_tmp, sa_tmp, q_tmp, f_tmp):
    for s in range(N_NEAR):
        t, q = divmod(s, 4)
        sq_tmp[3 * q : 3 * q + 3, tile(t)] = near_in[s, 0:3]
        t, g = divmod(s, 8)
        sa_tmp[3 * g : 3 * g + 3, tile(t)] = near_in[s, 3:6]
    q_tmp[...] = q_in[...]
    f_tmp[...] = f_in[...]
    numer = q_tmp[0:12] * sq_tmp[0:12]
    q_tmp[0:12] = (numer + 0.5) / (jnp.sum(numer, axis=0, keepdims=True) + 0.5 * K)
    old = f_tmp[0:12]
    alt_part = old * sa_tmp[0:12]
    f_tmp[0:12] = (alt_part + 0.5) / (alt_part + (1.0 - old) * sa_tmp[12:24] + 1.0)

    left = lane() < 64
    t = pl.multiple_of((var_of(idx) >> 1) * LANES, LANES)
    a, b = q_tmp[0:8, pl.ds(t, LANES)], q_tmp[8:16, pl.ds(t, LANES)]
    own_q[...] = jnp.where(
        (var_of(idx) & 1) == 0, jnp.where(left, a, roll(b, 64)), jnp.where(left, roll(a, 64), b)
    )
    t = pl.multiple_of((smp_of(idx) >> 3) * LANES, LANES)
    block = block_of_lane()
    got = f_tmp[0:4, pl.ds(t, LANES)]
    for j in range(1, 3):
        got = jnp.where(
            block == ((zl_of(idx) + j) & 7), roll(f_tmp[4 * j : 4 * j + 4, pl.ds(t, LANES)], 16 * j), got
        )
    own_f[...] = got

    sum_q, sum_a, sum_b = block_sums(dosage_ref, q_tmp[...], f_tmp[...])
    for t in range(8):
        a, b = sum_q[0:8, tile(t)], sum_q[8:16, tile(t)]
        v_out[2 * t] = jnp.where(left, a, roll(b, 64))
        v_out[2 * t + 1] = jnp.where(left, roll(a, 64), b)
    for t in range(4):
        turned = [
            roll(sums[4 * j : 4 * j + 4, tile(t)], 16 * j + at)
            for sums, at in ((sum_a, 0), (sum_b, 48))
            for j in range(3)
        ]
        for i in range(8):
            got = turned[0]
            for j in range(1, 6):
                got = jnp.where(block == (i + j) % 8, turned[j], got)
            s_out[8 * t + i] = got


def last_kernel(idx, v_in, s_in, own_q, own_f, shares_out, freqs_out):
    row = lax.broadcasted_iota(jnp.int32, (8, LANES), 0)
    held = (lane() < 64) | (row < 4)
    sum_q = sum(v_in[i] for i in range(N_VAR))
    numer = jnp.where(held, own_q[...] * sum_q, 0.0)
    total = jnp.sum(numer, axis=0, keepdims=True)
    total = total + pltpu.roll(total, 64, 1)
    new = (numer + 0.5) / (total + 0.5 * K)
    shares_out[0:8] = new[:, 0:64]
    shares_out[8:12] = new[0:4, 64:128]
    sums = sum(s_in[i] for i in range(N_SMP))
    alt_part = own_f[...] * sums
    ref_part = (1.0 - own_f[...]) * roll(sums, -48)
    new = (alt_part + 0.5) / (alt_part + ref_part + 1.0)
    new = pltpu.roll(jnp.concatenate([new, new], 0), (LANES - 16 * zl_of(idx)) & (LANES - 1), 1)
    for j in range(3):
        freqs_out[4 * j : 4 * j + 4] = new[0:4, 16 * j : 16 * j + 16]


def f32s(*shape):
    return jax.ShapeDtypeStruct(shape, f32)


def vmem(*shape):
    return pltpu.VMEM(shape, f32)


def call(kernel, scalars, n_in, outs, scratch, kept=True):
    spec = pl.BlockSpec(memory_space=pltpu.VMEM)
    run = pl.pallas_call(
        kernel,
        in_specs=[pl.BlockSpec(memory_space=pltpu.SMEM)] * scalars + [spec] * n_in,
        out_specs=[spec] * len(outs),
        out_shape=[pltpu.VMEM(o.shape, o.dtype) for o in outs] if kept else outs,
        scratch_shapes=scratch,
    )

    def placed(*args):
        args = args[:scalars] + tuple(
            pltpu.with_memory_space_constraint(a, pltpu.VMEM) for a in args[scalars:]
        )
        return run(*args)

    return placed


def exchange(x, axes):
    return lax.all_to_all(x, axes, 0, 0, tiled=True)


def body(dosage, shares_init, freqs_init):
    idx = lax.axis_index(AXES).astype(jnp.int32).reshape(1)
    samples, variants = 16 * dosage.shape[0], dosage.shape[1]
    tiles = lambda n: f32s(n, 8, LANES)
    fours = lambda n: f32s(n, 4, LANES)
    v_slots, s_slots = call(
        first_kernel, 1, 2, [tiles(N_VAR), fours(N_SMP)], [vmem(8, LANES), vmem(8, LANES)]
    )(idx, shares_init, freqs_init)
    v_got = exchange(v_slots, VAR)
    s_got = exchange(s_slots, SMP)
    slots, shares, freqs = call(
        one_kernel, 0, 3, [tiles(N_NEAR), f32s(PAD, samples), f32s(PAD, variants)],
        [vmem(PAD, samples), vmem(24, variants)],
    )(dosage, v_got, s_got)
    near_got = exchange(slots, NEAR)
    far_slots, own_sum = call(
        near_sums_kernel, 1, 1, [f32s(N_FAR, 24, LANES), f32s(24, LANES)], [vmem(24, LANES)]
    )(idx, near_got)
    far_got = exchange(far_slots, FAR)
    (near_slots,) = call(
        far_sums_kernel, 1, 2, [tiles(N_NEAR)], [vmem(24, LANES), vmem(24, LANES)]
    )(idx, far_got, own_sum)
    near_got = exchange(near_slots, NEAR)
    v_slots, s_slots, own_q, own_f = call(
        two_kernel, 1, 4, [tiles(N_VAR), fours(N_SMP), f32s(8, LANES), f32s(4, LANES)],
        [vmem(PAD, samples), vmem(24, variants), vmem(PAD, samples), vmem(PAD, variants)],
    )(idx, dosage, near_got, shares, freqs)
    v_got = exchange(v_slots, VAR)
    s_got = exchange(s_slots, SMP)
    return tuple(
        call(last_kernel, 1, 4, [f32s(*shares_init.shape), f32s(*freqs_init.shape)], [], False)(
            idx, v_got, s_got, own_q, own_f
        )
    )


def solution(mesh):
    fine = Mesh(mesh.devices.reshape(SIZES), AXES)
    return jax.shard_map(
        body,
        mesh=fine,
        in_specs=(P(SMP, VAR), P(None, SMP + VAR), P(None, VAR + SMP)),
        out_specs=(P(None, SMP + VAR), P(None, VAR + SMP)),
        check_vma=False,
    )
```

```python
import jax
import jax.numpy as jnp
from jax import lax
from jax.experimental import pallas as pl
from jax.experimental.pallas import tpu as pltpu
from jax.sharding import Mesh, PartitionSpec as P

K = 12
PAD = 16
LANES = 128
ROWS = 256

AXES = ("y", "zl", "x", "zh", "c")
SIZES = (4, 8, 4, 2, 2)
SMP = ("y", "zl")
VAR = ("x", "zh", "c")
NEAR = ("y", "x", "c")
FAR = ("zl", "zh")
N_NEAR, N_FAR = 32, 16
N_Y, N_XC, N_ZL, N_ZH = 4, 8, 8, 2

f32 = jnp.float32
bf16 = jnp.bfloat16


def tile(i):
    return slice(i * LANES, (i + 1) * LANES)


def var_of(idx):
    return idx[0] & 15


def smp_of(idx):
    return idx[0] >> 4


def zl_of(idx):
    return (idx[0] >> 4) & 7


def zh_of(idx):
    return (idx[0] >> 1) & 1


def lane():
    return lax.broadcasted_iota(jnp.int32, (8, LANES), 1)


def roll(x, shift):
    shift = shift % LANES
    return pltpu.roll(x, shift, 1) if shift else x


def two_parts(x):
    high = x.astype(bf16)
    return high, (x - high.astype(f32)).astype(bf16)


def three_parts(x):
    high = x.astype(bf16)
    return (high, *two_parts(x - high.astype(f32)))


def dot(a, b, over_a, over_b):
    return lax.dot_general(
        a, b, (((over_a,), (over_b,)), ((), ())), preferred_element_type=f32
    )


def fold(x):
    return x[:PAD] + x[PAD:]


def block_sums(dosage_ref, shares, freqs):
    qh, qm, ql = three_parts(shares)
    fh, fm, fl = three_parts(freqs)
    q_side = jnp.concatenate([qh, qh, qm, qh, ql, qm], 0)
    f_side = jnp.concatenate([fh, fm, fh, fl, fh, fm], 0)
    q_two = jnp.concatenate([qh, qm], 0)
    f_two = jnp.concatenate([fh, fm], 0)
    g_two = jnp.concatenate(two_parts(1.0 - freqs), 0)
    shift = 2 * lax.broadcasted_iota(jnp.int32, (16, freqs.shape[1]), 0)
    sums_q, sum_a, sum_b = [], None, None
    for at in range(0, shares.shape[1], ROWS):
        probs = dot(q_side[:, at : at + ROWS], f_side, 0, 0)
        codes = jnp.concatenate(
            [
                jnp.bitwise_and(
                    jnp.right_shift(jnp.broadcast_to(dosage_ref[w : w + 1, :], shift.shape), shift), 3
                )
                for w in range(at // 16, (at + ROWS) // 16)
            ],
            0,
        )
        rest = 1.0 - probs
        inverse = jnp.where(codes < 3, 1.0 / (probs * rest), 0.0)
        allele = codes.astype(f32)
        ah, al = two_parts(allele * (rest * inverse))
        bh, bl = two_parts((2.0 - allele) * (probs * inverse))
        sums_q.append(
            dot(f_two, ah, 1, 1) + dot(f_two, al, 1, 1) + dot(g_two, bh, 1, 1) + dot(g_two, bl, 1, 1)
        )
        q_part = q_two[:, at : at + ROWS]
        part_a = dot(q_part, ah, 1, 0) + dot(q_part, al, 1, 0)
        part_b = dot(q_part, bh, 1, 0) + dot(q_part, bl, 1, 0)
        sum_a = part_a if sum_a is None else sum_a + part_a
        sum_b = part_b if sum_b is None else sum_b + part_b
    return fold(jnp.concatenate(sums_q, 1)), fold(sum_a), fold(sum_b)


def near_of(idx):
    return ((idx[0] >> 1) & 6) | (idx[0] & 1)


def y_of(idx):
    return idx[0] >> 7


def halves(a, b):
    left = lax.broadcasted_iota(jnp.int32, a.shape, 1) < 64
    return jnp.where(left, a, roll(b, 64)), jnp.where(left, roll(a, 64), b)


def block_of_lane():
    return lax.broadcasted_iota(jnp.int32, (4, LANES), 1) // 16


def first_kernel(idx, shares_ref, freqs_ref, far_out, q_out, f_tmp):
    raw = shares_ref[...]
    own = raw / jnp.sum(raw, axis=0, keepdims=True)
    q_out[...] = jnp.zeros_like(q_out)
    f_tmp[...] = jnp.zeros_like(f_tmp)
    q_out[:, 0:64] = own[0:8]
    q_out[0:4, 64:128] = own[8:12]
    for j in range(3):
        f_tmp[0:4, 16 * j : 16 * j + 16] = freqs_ref[4 * j : 4 * j + 4, :]
    turned = pltpu.roll(f_tmp[...], 16 * zl_of(idx), 1)
    for h in range(N_ZH):
        sent = jnp.where(zh_of(idx) == h, turned, q_out[...])
        for i in range(N_ZL):
            far_out[i * N_ZH + h] = sent


def first_near_kernel(idx, far_in, q_in, near_out, f_out):
    zh = zh_of(idx)
    block = block_of_lane()
    freqs = [far_in[i * N_ZH + zh, 0:4] for i in range(N_ZL)]
    for j in range(3):
        got = freqs[0]
        for i in range(1, N_ZL):
            got = jnp.where(block == (i + j) % 8, freqs[i], got)
        f_out[j] = roll(got, -16 * j)
    own, other = q_in[...], far_in[zl_of(idx) * N_ZH + 1 - zh]
    low, high = halves(jnp.where(zh == 0, own, other), jnp.where(zh == 0, other, own))
    for s in range(N_NEAR):
        near_out[3 * s : 3 * s + 3] = f_out[...]
    for g in range(N_XC):
        s = 3 * (y_of(idx) * N_XC + g)
        near_out[s] = low[0:4]
        near_out[s + 1] = low[4:8]
        near_out[s + 2] = high[0:4]


def shares_of(idx, near_in):
    rows = [[], [], []]
    for x in range(4):
        for j in range(3):
            s = 3 * (y_of(idx) * N_XC + 2 * x) + j
            rows[j].extend(halves(near_in[s], near_in[s + 3]))
    return padded(rows)


def freqs_of(idx, near_in, f_in):
    rows = [[], [], []]
    for y in range(N_Y):
        for j in range(3):
            got = near_in[3 * (y * N_XC + near_of(idx)) + j]
            rows[j].append(jnp.where(y_of(idx) == y, f_in[j], got))
    return padded(rows)


def padded(rows):
    rows = [jnp.concatenate(row, 1) for row in rows]
    return jnp.concatenate([*rows, jnp.zeros_like(rows[0])], 0)


def one_kernel(idx, dosage_ref, near_in, own_f_in, slots, q_out, f_out, sq_tmp, sa_tmp):
    shares = shares_of(idx, near_in)
    freqs = freqs_of(idx, near_in, own_f_in)
    q_out[...] = shares
    f_out[...] = freqs
    sum_q, sum_a, sum_b = block_sums(dosage_ref, shares, freqs)
    sq_tmp[...] = sum_q
    sa_tmp[0:12] = sum_a[0:12]
    sa_tmp[12:24] = sum_b[0:12]
    slots[...] = jnp.zeros_like(slots)
    for s in range(N_NEAR):
        t, q = divmod(s, 4)
        slots[s, 0:3] = sq_tmp[3 * q : 3 * q + 3, tile(t)]
        t, g = divmod(s, 8)
        slots[s, 3:6] = sa_tmp[3 * g : 3 * g + 3, tile(t)]


def near_sums_kernel(idx, near_in, far_out, q_out, a_tmp):
    for y in range(N_Y):
        q_out[3 * y : 3 * y + 3] = sum(near_in[y * N_XC + g] for g in range(N_XC))[0:3]
    q_out[12:24] = jnp.zeros((12, LANES), f32)
    for g in range(N_XC):
        a_tmp[3 * g : 3 * g + 3] = sum(near_in[y * N_XC + g] for y in range(N_Y))[3:6]
    for h in range(N_ZH):
        sent = jnp.where(zh_of(idx) == h, a_tmp[...], q_out[...])
        for i in range(N_ZL):
            far_out[i * N_ZH + h] = sent


def far_sums_kernel(idx, far_in, q_in, near_out, q_tmp, a_tmp):
    zh = zh_of(idx)
    a_tmp[...] = sum(far_in[i * N_ZH + zh] for i in range(N_ZL))
    q_tmp[...] = q_in[...] + far_in[zl_of(idx) * N_ZH + 1 - zh]
    near_out[...] = jnp.zeros_like(near_out)
    for y in range(N_Y):
        for g in range(N_XC):
            near_out[y * N_XC + g, 0:3] = q_tmp[3 * y : 3 * y + 3]
            near_out[y * N_XC + g, 3:6] = a_tmp[3 * g : 3 * g + 3]


def two_kernel(idx, dosage_ref, near_in, q_in, f_in, near_out, sq_out, own_q, own_f, sq_tmp, sa_tmp, q_tmp, f_tmp):
    for s in range(N_NEAR):
        t, q = divmod(s, 4)
        sq_tmp[3 * q : 3 * q + 3, tile(t)] = near_in[s, 0:3]
        t, g = divmod(s, 8)
        sa_tmp[3 * g : 3 * g + 3, tile(t)] = near_in[s, 3:6]
    q_tmp[...] = q_in[...]
    f_tmp[...] = f_in[...]
    numer = q_tmp[0:12] * sq_tmp[0:12]
    q_tmp[0:12] = (numer + 0.5) / (jnp.sum(numer, axis=0, keepdims=True) + 0.5 * K)
    old = f_tmp[0:12]
    alt_part = old * sa_tmp[0:12]
    f_tmp[0:12] = (alt_part + 0.5) / (alt_part + (1.0 - old) * sa_tmp[12:24] + 1.0)

    t = pl.multiple_of((var_of(idx) >> 1) * LANES, LANES)
    even, odd = halves(q_tmp[0:8, pl.ds(t, LANES)], q_tmp[8:16, pl.ds(t, LANES)])
    own_q[...] = jnp.where((var_of(idx) & 1) == 0, even, odd)
    t = pl.multiple_of((smp_of(idx) >> 3) * LANES, LANES)
    block = block_of_lane()
    got = f_tmp[0:4, pl.ds(t, LANES)]
    for j in range(1, 3):
        got = jnp.where(
            block == ((zl_of(idx) + j) & 7), roll(f_tmp[4 * j : 4 * j + 4, pl.ds(t, LANES)], 16 * j), got
        )
    own_f[...] = got

    sum_q, sum_a, sum_b = block_sums(dosage_ref, q_tmp[...], f_tmp[...])
    for x in range(4):
        pair = halves(sum_q[:, tile(2 * x)], sum_q[:, tile(2 * x + 1)])
        for c in range(2):
            for y in range(N_Y):
                near_out[y * N_XC + 2 * x + c, 0:16] = pair[c]
    sq_out[...] = near_out[near_of(idx), 0:16]
    sa_tmp[0:12] = sum_a[0:12]
    sa_tmp[12:24] = sum_b[0:12]
    for y in range(N_Y):
        near_out[y * N_XC + near_of(idx)] = sa_tmp[:, tile(y)]


def last_far_kernel(idx, near_in, sq_in, far_out, q_out):
    zh, near = zh_of(idx), near_of(idx)
    sum_q = sq_in[...]
    for g in range(N_XC):
        got = near_in[y_of(idx) * N_XC + g, 0:16]
        sum_q = sum_q + jnp.where(near == g, 0.0, got)
    sums = sum(near_in[y * N_XC + near] for y in range(N_Y))
    parts = halves(sum_q[0:8], sum_q[8:16])
    q_out[...] = jnp.where(zh == 0, parts[0], parts[1])
    block = block_of_lane()
    turned = [roll(sums[4 * j : 4 * j + 4], 16 * j) for j in range(6)]
    for i in range(N_ZL):
        got = turned[0]
        for j in range(1, 6):
            got = jnp.where(block == (i + j) % 8, turned[j], got)
        got = jnp.concatenate([got, got], 0)
        for h in range(N_ZH):
            far_out[i * N_ZH + h] = jnp.where(zh == h, got, parts[h])


def last_kernel(idx, far_in, sq_in, own_q, own_f, shares_out, freqs_out):
    zh = zh_of(idx)
    row = lax.broadcasted_iota(jnp.int32, (8, LANES), 0)
    held = (lane() < 64) | (row < 4)
    sum_q = sq_in[...] + far_in[zl_of(idx) * N_ZH + 1 - zh]
    numer = jnp.where(held, own_q[...] * sum_q, 0.0)
    total = jnp.sum(numer, axis=0, keepdims=True)
    total = total + pltpu.roll(total, 64, 1)
    new = (numer + 0.5) / (total + 0.5 * K)
    shares_out[0:8] = new[:, 0:64]
    shares_out[8:12] = new[0:4, 64:128]
    sums = sum(far_in[i * N_ZH + zh, 0:4] for i in range(N_ZL))
    alt_part = own_f[...] * sums
    ref_part = (1.0 - own_f[...]) * roll(sums, -48)
    new = (alt_part + 0.5) / (alt_part + ref_part + 1.0)
    new = pltpu.roll(jnp.concatenate([new, new], 0), (LANES - 16 * zl_of(idx)) & (LANES - 1), 1)
    for j in range(3):
        freqs_out[4 * j : 4 * j + 4] = new[0:4, 16 * j : 16 * j + 16]


def f32s(*shape):
    return jax.ShapeDtypeStruct(shape, f32)


def vmem(*shape):
    return pltpu.VMEM(shape, f32)


def call(kernel, scalars, n_in, outs, scratch, kept=True):
    spec = pl.BlockSpec(memory_space=pltpu.VMEM)
    run = pl.pallas_call(
        kernel,
        in_specs=[pl.BlockSpec(memory_space=pltpu.SMEM)] * scalars + [spec] * n_in,
        out_specs=[spec] * len(outs),
        out_shape=[pltpu.VMEM(o.shape, o.dtype) for o in outs] if kept else outs,
        scratch_shapes=scratch,
    )

    def placed(*args):
        args = args[:scalars] + tuple(
            pltpu.with_memory_space_constraint(a, pltpu.VMEM) for a in args[scalars:]
        )
        return run(*args)

    return placed


def exchange(x, axes):
    return lax.all_to_all(x, axes, 0, 0, tiled=True)


def body(dosage, shares_init, freqs_init):
    idx = lax.axis_index(AXES).astype(jnp.int32).reshape(1)
    samples, variants = 16 * dosage.shape[0], dosage.shape[1]
    tiles = lambda n: f32s(n, 8, LANES)
    far_slots, own_q = call(first_kernel, 1, 2, [tiles(N_FAR), f32s(8, LANES)], [vmem(8, LANES)])(
        idx, shares_init, freqs_init
    )
    far_got = exchange(far_slots, FAR)
    near_slots, own_f = call(
        first_near_kernel, 1, 2, [f32s(3 * N_NEAR, 4, LANES), f32s(3, 4, LANES)], []
    )(idx, far_got, own_q)
    near_got = exchange(near_slots, NEAR)
    slots, shares, freqs = call(
        one_kernel, 1, 3, [tiles(N_NEAR), f32s(PAD, samples), f32s(PAD, variants)],
        [vmem(PAD, samples), vmem(24, variants)],
    )(idx, dosage, near_got, own_f)
    near_got = exchange(slots, NEAR)
    far_slots, own_sum = call(
        near_sums_kernel, 1, 1, [f32s(N_FAR, 24, LANES), f32s(24, LANES)], [vmem(24, LANES)]
    )(idx, near_got)
    far_got = exchange(far_slots, FAR)
    (near_slots,) = call(
        far_sums_kernel, 1, 2, [tiles(N_NEAR)], [vmem(24, LANES), vmem(24, LANES)]
    )(idx, far_got, own_sum)
    near_got = exchange(near_slots, NEAR)
    near_slots, own_sum, own_q, own_f = call(
        two_kernel, 1, 4,
        [f32s(N_NEAR, 24, LANES), f32s(PAD, LANES), f32s(8, LANES), f32s(4, LANES)],
        [vmem(PAD, samples), vmem(24, variants), vmem(PAD, samples), vmem(PAD, variants)],
    )(idx, dosage, near_got, shares, freqs)
    near_got = exchange(near_slots, NEAR)
    far_slots, own_sum = call(last_far_kernel, 1, 2, [tiles(N_FAR), f32s(8, LANES)], [])(
        idx, near_got, own_sum
    )
    far_got = exchange(far_slots, FAR)
    return tuple(
        call(last_kernel, 1, 4, [f32s(*shares_init.shape), f32s(*freqs_init.shape)], [], False)(
            idx, far_got, own_sum, own_q, own_f
        )
    )


def solution(mesh):
    fine = Mesh(mesh.devices.reshape(SIZES), AXES)
    return jax.shard_map(
        body,
        mesh=fine,
        in_specs=(P(SMP, VAR), P(None, SMP + VAR), P(None, VAR + SMP)),
        out_specs=(P(None, SMP + VAR), P(None, VAR + SMP)),
        check_vma=False,
    )
```

```python
import jax
import jax.numpy as jnp
from jax import lax
from jax.experimental import pallas as pl
from jax.experimental.pallas import tpu as pltpu
from jax.sharding import Mesh, PartitionSpec as P

K = 12
PAD = 16
LANES = 128
ROWS = 256

AXES = ("y", "zl", "x", "zh", "c")
SIZES = (4, 8, 4, 2, 2)
SMP = ("y", "zl")
VAR = ("x", "zh", "c")
NEAR = ("y", "x", "c")
FAR = ("zl", "zh")
N_NEAR, N_FAR = 32, 16
N_Y, N_XC, N_ZL, N_ZH = 4, 8, 8, 2

f32 = jnp.float32
bf16 = jnp.bfloat16


def tile(i):
    return slice(i * LANES, (i + 1) * LANES)


def var_of(idx):
    return idx[0] & 15


def smp_of(idx):
    return idx[0] >> 4


def zl_of(idx):
    return (idx[0] >> 4) & 7


def zh_of(idx):
    return (idx[0] >> 1) & 1


def lane():
    return lax.broadcasted_iota(jnp.int32, (8, LANES), 1)


def roll(x, shift):
    shift = shift % LANES
    return pltpu.roll(x, shift, 1) if shift else x


def two_parts(x):
    high = x.astype(bf16)
    return high, (x - high.astype(f32)).astype(bf16)


def three_parts(x):
    high = x.astype(bf16)
    return (high, *two_parts(x - high.astype(f32)))


def dot(a, b, over_a, over_b):
    return lax.dot_general(
        a, b, (((over_a,), (over_b,)), ((), ())), preferred_element_type=f32
    )


def fold(x):
    return x[:PAD] + x[PAD:]


def block_sums(dosage_ref, shares, freqs):
    qh, qm, ql = three_parts(shares)
    fh, fm, fl = three_parts(freqs)
    q_side = jnp.concatenate([qh, qh, qm, qh, ql, qm], 0)
    f_side = jnp.concatenate([fh, fm, fh, fl, fh, fm], 0)
    q_two = jnp.concatenate([qh, qm], 0)
    f_two = jnp.concatenate([fh, fm], 0)
    g_two = jnp.concatenate(two_parts(1.0 - freqs), 0)
    shift = 2 * lax.broadcasted_iota(jnp.int32, (16, freqs.shape[1]), 0)

    def ratios(at):
        probs = dot(q_side[:, at : at + ROWS], f_side, 0, 0)
        codes = jnp.concatenate(
            [
                jnp.bitwise_and(
                    jnp.right_shift(jnp.broadcast_to(dosage_ref[w : w + 1, :], shift.shape), shift), 3
                )
                for w in range(at // 16, (at + ROWS) // 16)
            ],
            0,
        )
        live = codes < 3
        allele = codes.astype(f32)
        ratio_alt = jnp.where(live, allele, 0.0) * (1.0 / probs)
        ratio_ref = jnp.where(live, 2.0 - allele, 0.0) * (1.0 / (1.0 - probs))
        return two_parts(ratio_alt) + two_parts(ratio_ref)

    sums_q, sum_a, sum_b = [], 0.0, 0.0
    starts = range(0, shares.shape[1], ROWS)
    ready = ratios(0)
    for at in starts:
        ah, al, bh, bl = ready
        if at + ROWS in starts:
            ready = ratios(at + ROWS)
        sums_q.append(
            dot(f_two, ah, 1, 1) + dot(f_two, al, 1, 1) + dot(g_two, bh, 1, 1) + dot(g_two, bl, 1, 1)
        )
        q_part = q_two[:, at : at + ROWS]
        sum_a = sum_a + (dot(q_part, ah, 1, 0) + dot(q_part, al, 1, 0))
        sum_b = sum_b + (dot(q_part, bh, 1, 0) + dot(q_part, bl, 1, 0))
    return fold(jnp.concatenate(sums_q, 1)), fold(sum_a), fold(sum_b)


def near_of(idx):
    return ((idx[0] >> 1) & 6) | (idx[0] & 1)


def y_of(idx):
    return idx[0] >> 7


def halves(a, b):
    left = lax.broadcasted_iota(jnp.int32, a.shape, 1) < 64
    return jnp.where(left, a, roll(b, 64)), jnp.where(left, roll(a, 64), b)


def block_of_lane():
    return lax.broadcasted_iota(jnp.int32, (4, LANES), 1) // 16


def first_kernel(idx, shares_ref, freqs_ref, far_out, q_out, f_tmp):
    raw = shares_ref[...]
    own = raw / jnp.sum(raw, axis=0, keepdims=True)
    q_out[...] = jnp.zeros_like(q_out)
    f_tmp[...] = jnp.zeros_like(f_tmp)
    q_out[:, 0:64] = own[0:8]
    q_out[0:4, 64:128] = own[8:12]
    for j in range(3):
        f_tmp[0:4, 16 * j : 16 * j + 16] = freqs_ref[4 * j : 4 * j + 4, :]
    turned = pltpu.roll(f_tmp[...], 16 * zl_of(idx), 1)
    for h in range(N_ZH):
        sent = jnp.where(zh_of(idx) == h, turned, q_out[...])
        for i in range(N_ZL):
            far_out[i * N_ZH + h] = sent


def first_near_kernel(idx, far_in, q_in, near_out, f_out):
    zh = zh_of(idx)
    block = block_of_lane()
    freqs = [far_in[i * N_ZH + zh, 0:4] for i in range(N_ZL)]
    for j in range(3):
        got = freqs[0]
        for i in range(1, N_ZL):
            got = jnp.where(block == (i + j) % 8, freqs[i], got)
        f_out[j] = roll(got, -16 * j)
    own, other = q_in[...], far_in[zl_of(idx) * N_ZH + 1 - zh]
    low, high = halves(jnp.where(zh == 0, own, other), jnp.where(zh == 0, other, own))
    for s in range(N_NEAR):
        near_out[3 * s : 3 * s + 3] = f_out[...]
    for g in range(N_XC):
        s = 3 * (y_of(idx) * N_XC + g)
        near_out[s] = low[0:4]
        near_out[s + 1] = low[4:8]
        near_out[s + 2] = high[0:4]


def shares_of(idx, near_in):
    rows = [[], [], []]
    for x in range(4):
        for j in range(3):
            s = 3 * (y_of(idx) * N_XC + 2 * x) + j
            rows[j].extend(halves(near_in[s], near_in[s + 3]))
    return padded(rows)


def freqs_of(idx, near_in, f_in):
    rows = [[], [], []]
    for y in range(N_Y):
        for j in range(3):
            got = near_in[3 * (y * N_XC + near_of(idx)) + j]
            rows[j].append(jnp.where(y_of(idx) == y, f_in[j], got))
    return padded(rows)


def padded(rows):
    rows = [jnp.concatenate(row, 1) for row in rows]
    return jnp.concatenate([*rows, jnp.zeros_like(rows[0])], 0)


def one_kernel(idx, dosage_ref, near_in, own_f_in, slots, q_out, f_out, sq_tmp, sa_tmp):
    shares = shares_of(idx, near_in)
    freqs = freqs_of(idx, near_in, own_f_in)
    q_out[...] = shares
    f_out[...] = freqs
    sum_q, sum_a, sum_b = block_sums(dosage_ref, shares, freqs)
    sq_tmp[...] = sum_q
    sa_tmp[0:12] = sum_a[0:12]
    sa_tmp[12:24] = sum_b[0:12]
    slots[...] = jnp.zeros_like(slots)
    for s in range(N_NEAR):
        t, q = divmod(s, 4)
        slots[s, 0:3] = sq_tmp[3 * q : 3 * q + 3, tile(t)]
        t, g = divmod(s, 8)
        slots[s, 3:6] = sa_tmp[3 * g : 3 * g + 3, tile(t)]


def near_sums_kernel(idx, near_in, far_out, q_out, a_tmp):
    for y in range(N_Y):
        q_out[3 * y : 3 * y + 3] = sum(near_in[y * N_XC + g] for g in range(N_XC))[0:3]
    q_out[12:24] = jnp.zeros((12, LANES), f32)
    for g in range(N_XC):
        a_tmp[3 * g : 3 * g + 3] = sum(near_in[y * N_XC + g] for y in range(N_Y))[3:6]
    for h in range(N_ZH):
        sent = jnp.where(zh_of(idx) == h, a_tmp[...], q_out[...])
        for i in range(N_ZL):
            far_out[i * N_ZH + h] = sent


def far_sums_kernel(idx, far_in, q_in, near_out, q_tmp, a_tmp):
    zh = zh_of(idx)
    a_tmp[...] = sum(far_in[i * N_ZH + zh] for i in range(N_ZL))
    q_tmp[...] = q_in[...] + far_in[zl_of(idx) * N_ZH + 1 - zh]
    near_out[...] = jnp.zeros_like(near_out)
    for y in range(N_Y):
        for g in range(N_XC):
            near_out[y * N_XC + g, 0:3] = q_tmp[3 * y : 3 * y + 3]
            near_out[y * N_XC + g, 3:6] = a_tmp[3 * g : 3 * g + 3]


def two_kernel(idx, dosage_ref, near_in, q_in, f_in, near_out, sq_out, own_q, own_f, sq_tmp, sa_tmp, q_tmp, f_tmp):
    for s in range(N_NEAR):
        t, q = divmod(s, 4)
        sq_tmp[3 * q : 3 * q + 3, tile(t)] = near_in[s, 0:3]
        t, g = divmod(s, 8)
        sa_tmp[3 * g : 3 * g + 3, tile(t)] = near_in[s, 3:6]
    q_tmp[...] = q_in[...]
    f_tmp[...] = f_in[...]
    numer = q_tmp[0:12] * sq_tmp[0:12]
    q_tmp[0:12] = (numer + 0.5) / (jnp.sum(numer, axis=0, keepdims=True) + 0.5 * K)
    old = f_tmp[0:12]
    alt_part = old * sa_tmp[0:12]
    f_tmp[0:12] = (alt_part + 0.5) / (alt_part + (1.0 - old) * sa_tmp[12:24] + 1.0)

    t = pl.multiple_of((var_of(idx) >> 1) * LANES, LANES)
    even, odd = halves(q_tmp[0:8, pl.ds(t, LANES)], q_tmp[8:16, pl.ds(t, LANES)])
    own_q[...] = jnp.where((var_of(idx) & 1) == 0, even, odd)
    t = pl.multiple_of((smp_of(idx) >> 3) * LANES, LANES)
    block = block_of_lane()
    got = f_tmp[0:4, pl.ds(t, LANES)]
    for j in range(1, 3):
        got = jnp.where(
            block == ((zl_of(idx) + j) & 7), roll(f_tmp[4 * j : 4 * j + 4, pl.ds(t, LANES)], 16 * j), got
        )
    own_f[...] = got

    sum_q, sum_a, sum_b = block_sums(dosage_ref, q_tmp[...], f_tmp[...])
    for x in range(4):
        pair = halves(sum_q[:, tile(2 * x)], sum_q[:, tile(2 * x + 1)])
        for c in range(2):
            for y in range(N_Y):
                near_out[y * N_XC + 2 * x + c, 0:16] = pair[c]
    sq_out[...] = near_out[near_of(idx), 0:16]
    sa_tmp[0:12] = sum_a[0:12]
    sa_tmp[12:24] = sum_b[0:12]
    for y in range(N_Y):
        near_out[y * N_XC + near_of(idx)] = sa_tmp[:, tile(y)]


def last_far_kernel(idx, near_in, sq_in, far_out, q_out):
    zh, near = zh_of(idx), near_of(idx)
    sum_q = sq_in[...]
    for g in range(N_XC):
        got = near_in[y_of(idx) * N_XC + g, 0:16]
        sum_q = sum_q + jnp.where(near == g, 0.0, got)
    sums = sum(near_in[y * N_XC + near] for y in range(N_Y))
    parts = halves(sum_q[0:8], sum_q[8:16])
    q_out[...] = jnp.where(zh == 0, parts[0], parts[1])
    block = block_of_lane()
    turned = [roll(sums[4 * j : 4 * j + 4], 16 * j) for j in range(6)]
    for i in range(N_ZL):
        got = turned[0]
        for j in range(1, 6):
            got = jnp.where(block == (i + j) % 8, turned[j], got)
        got = jnp.concatenate([got, got], 0)
        for h in range(N_ZH):
            far_out[i * N_ZH + h] = jnp.where(zh == h, got, parts[h])


def last_kernel(idx, far_in, sq_in, own_q, own_f, shares_out, freqs_out):
    zh = zh_of(idx)
    row = lax.broadcasted_iota(jnp.int32, (8, LANES), 0)
    held = (lane() < 64) | (row < 4)
    sum_q = sq_in[...] + far_in[zl_of(idx) * N_ZH + 1 - zh]
    numer = jnp.where(held, own_q[...] * sum_q, 0.0)
    total = jnp.sum(numer, axis=0, keepdims=True)
    total = total + pltpu.roll(total, 64, 1)
    new = (numer + 0.5) / (total + 0.5 * K)
    shares_out[0:8] = new[:, 0:64]
    shares_out[8:12] = new[0:4, 64:128]
    sums = sum(far_in[i * N_ZH + zh, 0:4] for i in range(N_ZL))
    alt_part = own_f[...] * sums
    ref_part = (1.0 - own_f[...]) * roll(sums, -48)
    new = (alt_part + 0.5) / (alt_part + ref_part + 1.0)
    new = pltpu.roll(jnp.concatenate([new, new], 0), (LANES - 16 * zl_of(idx)) & (LANES - 1), 1)
    for j in range(3):
        freqs_out[4 * j : 4 * j + 4] = new[0:4, 16 * j : 16 * j + 16]


def f32s(*shape):
    return jax.ShapeDtypeStruct(shape, f32)


def vmem(*shape):
    return pltpu.VMEM(shape, f32)


def call(kernel, scalars, n_in, outs, scratch, kept=True):
    spec = pl.BlockSpec(memory_space=pltpu.VMEM)
    run = pl.pallas_call(
        kernel,
        in_specs=[pl.BlockSpec(memory_space=pltpu.SMEM)] * scalars + [spec] * n_in,
        out_specs=[spec] * len(outs),
        out_shape=[pltpu.VMEM(o.shape, o.dtype) for o in outs] if kept else outs,
        scratch_shapes=scratch,
    )

    def placed(*args):
        args = args[:scalars] + tuple(
            pltpu.with_memory_space_constraint(a, pltpu.VMEM) for a in args[scalars:]
        )
        return run(*args)

    return placed


def exchange(x, axes):
    return lax.all_to_all(x, axes, 0, 0, tiled=True)


def body(dosage, shares_init, freqs_init):
    idx = lax.axis_index(AXES).astype(jnp.int32).reshape(1)
    samples, variants = 16 * dosage.shape[0], dosage.shape[1]
    tiles = lambda n: f32s(n, 8, LANES)
    far_slots, own_q = call(first_kernel, 1, 2, [tiles(N_FAR), f32s(8, LANES)], [vmem(8, LANES)])(
        idx, shares_init, freqs_init
    )
    far_got = exchange(far_slots, FAR)
    near_slots, own_f = call(
        first_near_kernel, 1, 2, [f32s(3 * N_NEAR, 4, LANES), f32s(3, 4, LANES)], []
    )(idx, far_got, own_q)
    near_got = exchange(near_slots, NEAR)
    slots, shares, freqs = call(
        one_kernel, 1, 3, [tiles(N_NEAR), f32s(PAD, samples), f32s(PAD, variants)],
        [vmem(PAD, samples), vmem(24, variants)],
    )(idx, dosage, near_got, own_f)
    near_got = exchange(slots, NEAR)
    far_slots, own_sum = call(
        near_sums_kernel, 1, 1, [f32s(N_FAR, 24, LANES), f32s(24, LANES)], [vmem(24, LANES)]
    )(idx, near_got)
    far_got = exchange(far_slots, FAR)
    (near_slots,) = call(
        far_sums_kernel, 1, 2, [tiles(N_NEAR)], [vmem(24, LANES), vmem(24, LANES)]
    )(idx, far_got, own_sum)
    near_got = exchange(near_slots, NEAR)
    near_slots, own_sum, own_q, own_f = call(
        two_kernel, 1, 4,
        [f32s(N_NEAR, 24, LANES), f32s(PAD, LANES), f32s(8, LANES), f32s(4, LANES)],
        [vmem(PAD, samples), vmem(24, variants), vmem(PAD, samples), vmem(PAD, variants)],
    )(idx, dosage, near_got, shares, freqs)
    near_got = exchange(near_slots, NEAR)
    far_slots, own_sum = call(last_far_kernel, 1, 2, [tiles(N_FAR), f32s(8, LANES)], [])(
        idx, near_got, own_sum
    )
    far_got = exchange(far_slots, FAR)
    return tuple(
        call(last_kernel, 1, 4, [f32s(*shares_init.shape), f32s(*freqs_init.shape)], [], False)(
            idx, far_got, own_sum, own_q, own_f
        )
    )


def solution(mesh):
    fine = Mesh(mesh.devices.reshape(SIZES), AXES)
    return jax.shard_map(
        body,
        mesh=fine,
        in_specs=(P(SMP, VAR), P(None, SMP + VAR), P(None, VAR + SMP)),
        out_specs=(P(None, SMP + VAR), P(None, VAR + SMP)),
        check_vma=False,
    )
```

```python
import jax
import jax.numpy as jnp
from jax import lax
from jax.experimental import pallas as pl
from jax.experimental.pallas import tpu as pltpu
from jax.sharding import Mesh, PartitionSpec as P

K = 12
PAD = 16
LANES = 128
ROWS = 256

AXES = ("y", "zl", "x", "zh", "c")
SIZES = (4, 8, 4, 2, 2)
SMP = ("y", "zl")
VAR = ("x", "zh", "c")
NEAR = ("y", "x", "c")
FAR = ("zl", "zh")
N_NEAR, N_FAR = 32, 16
N_Y, N_XC, N_ZL, N_ZH = 4, 8, 8, 2
NEAR_FIRST = 21
FAR_FIRST = 1

f32 = jnp.float32
bf16 = jnp.bfloat16


def tile(i):
    return slice(i * LANES, (i + 1) * LANES)


def var_of(idx):
    return idx[0] & 15


def smp_of(idx):
    return idx[0] >> 4


def zl_of(idx):
    return (idx[0] >> 4) & 7


def zh_of(idx):
    return (idx[0] >> 1) & 1


def lane():
    return lax.broadcasted_iota(jnp.int32, (8, LANES), 1)


def roll(x, shift):
    shift = shift % LANES
    return pltpu.roll(x, shift, 1) if shift else x


def two_parts(x):
    high = x.astype(bf16)
    return high, (x - high.astype(f32)).astype(bf16)


def three_parts(x):
    high = x.astype(bf16)
    return (high, *two_parts(x - high.astype(f32)))


def dot(a, b, over_a, over_b):
    return lax.dot_general(
        a, b, (((over_a,), (over_b,)), ((), ())), preferred_element_type=f32
    )


def fold(x):
    return x[:PAD] + x[PAD:]


def block_sums(dosage_ref, shares, freqs):
    qh, qm, ql = three_parts(shares)
    fh, fm, fl = three_parts(freqs)
    q_side = jnp.concatenate([qh, qh, qm, qh, ql, qm], 0)
    f_side = jnp.concatenate([fh, fm, fh, fl, fh, fm], 0)
    q_two = jnp.concatenate([qh, qm], 0)
    f_two = jnp.concatenate([fh, fm], 0)
    g_two = jnp.concatenate(two_parts(1.0 - freqs), 0)
    shift = 2 * lax.broadcasted_iota(jnp.int32, (16, freqs.shape[1]), 0)

    def ratios(at):
        probs = dot(q_side[:, at : at + ROWS], f_side, 0, 0)
        codes = jnp.concatenate(
            [
                jnp.bitwise_and(
                    jnp.right_shift(jnp.broadcast_to(dosage_ref[w : w + 1, :], shift.shape), shift), 3
                )
                for w in range(at // 16, (at + ROWS) // 16)
            ],
            0,
        )
        live = codes < 3
        allele = codes.astype(f32)
        ratio_alt = jnp.where(live, allele, 0.0) * (1.0 / probs)
        ratio_ref = jnp.where(live, 2.0 - allele, 0.0) * (1.0 / (1.0 - probs))
        return two_parts(ratio_alt) + two_parts(ratio_ref)

    sums_q, sum_a, sum_b = [], 0.0, 0.0
    starts = range(0, shares.shape[1], ROWS)
    ready = ratios(0)
    for at in starts:
        ah, al, bh, bl = ready
        if at + ROWS in starts:
            ready = ratios(at + ROWS)
        sums_q.append(
            dot(f_two, ah, 1, 1) + dot(f_two, al, 1, 1) + dot(g_two, bh, 1, 1) + dot(g_two, bl, 1, 1)
        )
        q_part = q_two[:, at : at + ROWS]
        sum_a = sum_a + (dot(q_part, ah, 1, 0) + dot(q_part, al, 1, 0))
        sum_b = sum_b + (dot(q_part, bh, 1, 0) + dot(q_part, bl, 1, 0))
    return fold(jnp.concatenate(sums_q, 1)), fold(sum_a), fold(sum_b)


def near_at(y, g):
    return (y * N_XC + g) ^ NEAR_FIRST


def far_at(i, h):
    return (i * N_ZH + h) ^ FAR_FIRST


def near_of(idx):
    return ((idx[0] >> 1) & 6) | (idx[0] & 1)


def y_of(idx):
    return idx[0] >> 7


def halves(a, b):
    left = lax.broadcasted_iota(jnp.int32, a.shape, 1) < 64
    return jnp.where(left, a, roll(b, 64)), jnp.where(left, roll(a, 64), b)


def block_of_lane():
    return lax.broadcasted_iota(jnp.int32, (4, LANES), 1) // 16


def first_kernel(idx, shares_ref, freqs_ref, far_out, q_out, f_tmp):
    raw = shares_ref[...]
    own = raw / jnp.sum(raw, axis=0, keepdims=True)
    q_out[...] = jnp.zeros_like(q_out)
    f_tmp[...] = jnp.zeros_like(f_tmp)
    q_out[:, 0:64] = own[0:8]
    q_out[0:4, 64:128] = own[8:12]
    for j in range(3):
        f_tmp[0:4, 16 * j : 16 * j + 16] = freqs_ref[4 * j : 4 * j + 4, :]
    turned = pltpu.roll(f_tmp[...], 16 * zl_of(idx), 1)
    for h in range(N_ZH):
        sent = jnp.where(zh_of(idx) == h, turned, q_out[...])
        for i in range(N_ZL):
            far_out[far_at(i, h)] = sent


def first_near_kernel(idx, far_in, q_in, near_out, f_out):
    zh = zh_of(idx)
    block = block_of_lane()
    freqs = [far_in[far_at(i, zh), 0:4] for i in range(N_ZL)]
    for j in range(3):
        got = freqs[0]
        for i in range(1, N_ZL):
            got = jnp.where(block == (i + j) % 8, freqs[i], got)
        f_out[j] = roll(got, -16 * j)
    own, other = q_in[...], far_in[far_at(zl_of(idx), 1 - zh)]
    low, high = halves(jnp.where(zh == 0, own, other), jnp.where(zh == 0, other, own))
    for s in range(N_NEAR):
        near_out[3 * s : 3 * s + 3] = f_out[...]
    for g in range(N_XC):
        s = 3 * near_at(y_of(idx), g)
        near_out[s] = low[0:4]
        near_out[s + 1] = low[4:8]
        near_out[s + 2] = high[0:4]


def shares_of(idx, near_in):
    rows = [[], [], []]
    for x in range(4):
        for j in range(3):
            a, b = (near_in[3 * near_at(y_of(idx), 2 * x + c) + j] for c in range(2))
            rows[j].extend(halves(a, b))
    return padded(rows)


def freqs_of(idx, near_in, f_in):
    rows = [[], [], []]
    for y in range(N_Y):
        for j in range(3):
            got = near_in[3 * near_at(y, near_of(idx)) + j]
            rows[j].append(jnp.where(y_of(idx) == y, f_in[j], got))
    return padded(rows)


def padded(rows):
    rows = [jnp.concatenate(row, 1) for row in rows]
    return jnp.concatenate([*rows, jnp.zeros_like(rows[0])], 0)


def one_kernel(idx, dosage_ref, near_in, own_f_in, slots, q_out, f_out, sq_tmp, sa_tmp):
    shares = shares_of(idx, near_in)
    freqs = freqs_of(idx, near_in, own_f_in)
    q_out[...] = shares
    f_out[...] = freqs
    sum_q, sum_a, sum_b = block_sums(dosage_ref, shares, freqs)
    sq_tmp[...] = sum_q
    sa_tmp[0:12] = sum_a[0:12]
    sa_tmp[12:24] = sum_b[0:12]
    slots[...] = jnp.zeros_like(slots)
    for s in range(N_NEAR):
        t, q = divmod(s, 4)
        slots[s ^ NEAR_FIRST, 0:3] = sq_tmp[3 * q : 3 * q + 3, tile(t)]
        t, g = divmod(s, 8)
        slots[s ^ NEAR_FIRST, 3:6] = sa_tmp[3 * g : 3 * g + 3, tile(t)]


def near_sums_kernel(idx, near_in, far_out, q_out, a_tmp):
    for y in range(N_Y):
        q_out[3 * y : 3 * y + 3] = sum(near_in[near_at(y, g)] for g in range(N_XC))[0:3]
    q_out[12:24] = jnp.zeros((12, LANES), f32)
    for g in range(N_XC):
        a_tmp[3 * g : 3 * g + 3] = sum(near_in[near_at(y, g)] for y in range(N_Y))[3:6]
    for h in range(N_ZH):
        sent = jnp.where(zh_of(idx) == h, a_tmp[...], q_out[...])
        for i in range(N_ZL):
            far_out[far_at(i, h)] = sent


def far_sums_kernel(idx, far_in, q_in, near_out, q_tmp, a_tmp):
    zh = zh_of(idx)
    a_tmp[...] = sum(far_in[far_at(i, zh)] for i in range(N_ZL))
    q_tmp[...] = q_in[...] + far_in[far_at(zl_of(idx), 1 - zh)]
    near_out[...] = jnp.zeros_like(near_out)
    for y in range(N_Y):
        for g in range(N_XC):
            near_out[near_at(y, g), 0:3] = q_tmp[3 * y : 3 * y + 3]
            near_out[near_at(y, g), 3:6] = a_tmp[3 * g : 3 * g + 3]


def two_kernel(idx, dosage_ref, near_in, q_in, f_in, near_out, sq_out, own_q, own_f, sq_tmp, sa_tmp, q_tmp, f_tmp):
    for s in range(N_NEAR):
        t, q = divmod(s, 4)
        sq_tmp[3 * q : 3 * q + 3, tile(t)] = near_in[s ^ NEAR_FIRST, 0:3]
        t, g = divmod(s, 8)
        sa_tmp[3 * g : 3 * g + 3, tile(t)] = near_in[s ^ NEAR_FIRST, 3:6]
    q_tmp[...] = q_in[...]
    f_tmp[...] = f_in[...]
    numer = q_tmp[0:12] * sq_tmp[0:12]
    q_tmp[0:12] = (numer + 0.5) / (jnp.sum(numer, axis=0, keepdims=True) + 0.5 * K)
    old = f_tmp[0:12]
    alt_part = old * sa_tmp[0:12]
    f_tmp[0:12] = (alt_part + 0.5) / (alt_part + (1.0 - old) * sa_tmp[12:24] + 1.0)

    t = pl.multiple_of((var_of(idx) >> 1) * LANES, LANES)
    even, odd = halves(q_tmp[0:8, pl.ds(t, LANES)], q_tmp[8:16, pl.ds(t, LANES)])
    own_q[...] = jnp.where((var_of(idx) & 1) == 0, even, odd)
    t = pl.multiple_of((smp_of(idx) >> 3) * LANES, LANES)
    block = block_of_lane()
    got = f_tmp[0:4, pl.ds(t, LANES)]
    for j in range(1, 3):
        got = jnp.where(
            block == ((zl_of(idx) + j) & 7), roll(f_tmp[4 * j : 4 * j + 4, pl.ds(t, LANES)], 16 * j), got
        )
    own_f[...] = got

    sum_q, sum_a, sum_b = block_sums(dosage_ref, q_tmp[...], f_tmp[...])
    for x in range(4):
        pair = halves(sum_q[:, tile(2 * x)], sum_q[:, tile(2 * x + 1)])
        for c in range(2):
            for y in range(N_Y):
                near_out[near_at(y, 2 * x + c), 0:16] = pair[c]
    sq_out[...] = near_out[near_at(0, near_of(idx)), 0:16]
    sa_tmp[0:12] = sum_a[0:12]
    sa_tmp[12:24] = sum_b[0:12]
    for y in range(N_Y):
        near_out[near_at(y, near_of(idx))] = sa_tmp[:, tile(y)]


def last_far_kernel(idx, near_in, sq_in, far_out, q_out):
    zh, near = zh_of(idx), near_of(idx)
    sum_q = sq_in[...]
    for g in range(N_XC):
        got = near_in[near_at(y_of(idx), g), 0:16]
        sum_q = sum_q + jnp.where(near == g, 0.0, got)
    sums = sum(near_in[near_at(y, near)] for y in range(N_Y))
    parts = halves(sum_q[0:8], sum_q[8:16])
    q_out[...] = jnp.where(zh == 0, parts[0], parts[1])
    block = block_of_lane()
    turned = [roll(sums[4 * j : 4 * j + 4], 16 * j) for j in range(6)]
    for i in range(N_ZL):
        got = turned[0]
        for j in range(1, 6):
            got = jnp.where(block == (i + j) % 8, turned[j], got)
        got = jnp.concatenate([got, got], 0)
        for h in range(N_ZH):
            far_out[far_at(i, h)] = jnp.where(zh == h, got, parts[h])


def last_kernel(idx, far_in, sq_in, own_q, own_f, shares_out, freqs_out):
    zh = zh_of(idx)
    row = lax.broadcasted_iota(jnp.int32, (8, LANES), 0)
    held = (lane() < 64) | (row < 4)
    sum_q = sq_in[...] + far_in[far_at(zl_of(idx), 1 - zh)]
    numer = jnp.where(held, own_q[...] * sum_q, 0.0)
    total = jnp.sum(numer, axis=0, keepdims=True)
    total = total + pltpu.roll(total, 64, 1)
    new = (numer + 0.5) / (total + 0.5 * K)
    shares_out[0:8] = new[:, 0:64]
    shares_out[8:12] = new[0:4, 64:128]
    sums = sum(far_in[far_at(i, zh), 0:4] for i in range(N_ZL))
    alt_part = own_f[...] * sums
    ref_part = (1.0 - own_f[...]) * roll(sums, -48)
    new = (alt_part + 0.5) / (alt_part + ref_part + 1.0)
    new = pltpu.roll(jnp.concatenate([new, new], 0), (LANES - 16 * zl_of(idx)) & (LANES - 1), 1)
    for j in range(3):
        freqs_out[4 * j : 4 * j + 4] = new[0:4, 16 * j : 16 * j + 16]


def f32s(*shape):
    return jax.ShapeDtypeStruct(shape, f32)


def vmem(*shape):
    return pltpu.VMEM(shape, f32)


def call(kernel, scalars, n_in, outs, scratch, kept=True):
    spec = pl.BlockSpec(memory_space=pltpu.VMEM)
    run = pl.pallas_call(
        kernel,
        in_specs=[pl.BlockSpec(memory_space=pltpu.SMEM)] * scalars + [spec] * n_in,
        out_specs=[spec] * len(outs),
        out_shape=[pltpu.VMEM(o.shape, o.dtype) for o in outs] if kept else outs,
        scratch_shapes=scratch,
    )

    def placed(*args):
        args = args[:scalars] + tuple(
            pltpu.with_memory_space_constraint(a, pltpu.VMEM) for a in args[scalars:]
        )
        return run(*args)

    return placed


def exchange(x, axes):
    members, first = (N_NEAR, NEAR_FIRST) if axes is NEAR else (N_FAR, FAR_FIRST)
    order = [[i ^ first for i in range(members)]]
    return lax.all_to_all(x, axes, 0, 0, tiled=True, axis_index_groups=order)


def body(dosage, shares_init, freqs_init):
    idx = lax.axis_index(AXES).astype(jnp.int32).reshape(1)
    samples, variants = 16 * dosage.shape[0], dosage.shape[1]
    tiles = lambda n: f32s(n, 8, LANES)
    far_slots, own_q = call(first_kernel, 1, 2, [tiles(N_FAR), f32s(8, LANES)], [vmem(8, LANES)])(
        idx, shares_init, freqs_init
    )
    far_got = exchange(far_slots, FAR)
    near_slots, own_f = call(
        first_near_kernel, 1, 2, [f32s(3 * N_NEAR, 4, LANES), f32s(3, 4, LANES)], []
    )(idx, far_got, own_q)
    near_got = exchange(near_slots, NEAR)
    slots, shares, freqs = call(
        one_kernel, 1, 3, [tiles(N_NEAR), f32s(PAD, samples), f32s(PAD, variants)],
        [vmem(PAD, samples), vmem(24, variants)],
    )(idx, dosage, near_got, own_f)
    near_got = exchange(slots, NEAR)
    far_slots, own_sum = call(
        near_sums_kernel, 1, 1, [f32s(N_FAR, 24, LANES), f32s(24, LANES)], [vmem(24, LANES)]
    )(idx, near_got)
    far_got = exchange(far_slots, FAR)
    (near_slots,) = call(
        far_sums_kernel, 1, 2, [tiles(N_NEAR)], [vmem(24, LANES), vmem(24, LANES)]
    )(idx, far_got, own_sum)
    near_got = exchange(near_slots, NEAR)
    near_slots, own_sum, own_q, own_f = call(
        two_kernel, 1, 4,
        [f32s(N_NEAR, 24, LANES), f32s(PAD, LANES), f32s(8, LANES), f32s(4, LANES)],
        [vmem(PAD, samples), vmem(24, variants), vmem(PAD, samples), vmem(PAD, variants)],
    )(idx, dosage, near_got, shares, freqs)
    near_got = exchange(near_slots, NEAR)
    far_slots, own_sum = call(last_far_kernel, 1, 2, [tiles(N_FAR), f32s(8, LANES)], [])(
        idx, near_got, own_sum
    )
    far_got = exchange(far_slots, FAR)
    return tuple(
        call(last_kernel, 1, 4, [f32s(*shares_init.shape), f32s(*freqs_init.shape)], [], False)(
            idx, far_got, own_sum, own_q, own_f
        )
    )


def solution(mesh):
    fine = Mesh(mesh.devices.reshape(SIZES), AXES)
    return jax.shard_map(
        body,
        mesh=fine,
        in_specs=(P(SMP, VAR), P(None, SMP + VAR), P(None, VAR + SMP)),
        out_specs=(P(None, SMP + VAR), P(None, VAR + SMP)),
        check_vma=False,
    )
```

```python
import jax
import jax.numpy as jnp
from jax import lax
from jax.experimental import pallas as pl
from jax.experimental.pallas import tpu as pltpu
from jax.sharding import Mesh, PartitionSpec as P

K = 12
PAD = 16
LANES = 128
ROWS = 256

AXES = ("y", "zq", "zp", "x", "zh", "c")
SIZES = (4, 4, 2, 4, 2, 2)
SMP = ("y", "zq", "zp")
VAR = ("x", "zh", "c")
NEAR = ("y", "x", "c")
FAR = ("zq", "zp", "zh")
WIDE = ("y", "zp", "x", "c")
LINE = ("zq", "zh")
N_NEAR, N_FAR, N_WIDE, N_LINE = 32, 16, 64, 8
N_Y, N_XC, N_ZL, N_ZH, N_ZQ, N_ROW = 4, 8, 8, 2, 4, 8
NEAR_FIRST = 21
FAR_FIRST = 1
WIDE_FIRST = 37
LINE_FIRST = 1

f32 = jnp.float32
bf16 = jnp.bfloat16


def tile(i):
    return slice(i * LANES, (i + 1) * LANES)


def var_of(idx):
    return idx[0] & 15


def smp_of(idx):
    return idx[0] >> 4


def zl_of(idx):
    return (idx[0] >> 4) & 7


def zh_of(idx):
    return (idx[0] >> 1) & 1


def lane():
    return lax.broadcasted_iota(jnp.int32, (8, LANES), 1)


def roll(x, shift):
    shift = shift % LANES
    return pltpu.roll(x, shift, 1) if shift else x


def two_parts(x):
    high = x.astype(bf16)
    return high, (x - high.astype(f32)).astype(bf16)


def three_parts(x):
    high = x.astype(bf16)
    return (high, *two_parts(x - high.astype(f32)))


def dot(a, b, over_a, over_b):
    return lax.dot_general(
        a, b, (((over_a,), (over_b,)), ((), ())), preferred_element_type=f32
    )


def fold(x):
    return x[:PAD] + x[PAD:]


def block_sums(dosage_ref, shares, freqs):
    qh, qm, ql = three_parts(shares)
    fh, fm, fl = three_parts(freqs)
    q_side = jnp.concatenate([qh, qh, qm, qh, ql, qm], 0)
    f_side = jnp.concatenate([fh, fm, fh, fl, fh, fm], 0)
    q_two = jnp.concatenate([qh, qm], 0)
    f_two = jnp.concatenate([fh, fm], 0)
    g_two = jnp.concatenate(two_parts(1.0 - freqs), 0)
    shift = 2 * lax.broadcasted_iota(jnp.int32, (16, freqs.shape[1]), 0)

    def ratios(at):
        probs = dot(q_side[:, at : at + ROWS], f_side, 0, 0)
        codes = jnp.concatenate(
            [
                jnp.bitwise_and(
                    jnp.right_shift(jnp.broadcast_to(dosage_ref[w : w + 1, :], shift.shape), shift), 3
                )
                for w in range(at // 16, (at + ROWS) // 16)
            ],
            0,
        )
        live = codes < 3
        allele = codes.astype(f32)
        ratio_alt = jnp.where(live, allele, 0.0) * (1.0 / probs)
        ratio_ref = jnp.where(live, 2.0 - allele, 0.0) * (1.0 / (1.0 - probs))
        return two_parts(ratio_alt) + two_parts(ratio_ref)

    sums_q, sum_a, sum_b = [], 0.0, 0.0
    starts = range(0, shares.shape[1], ROWS)
    ready = ratios(0)
    for at in starts:
        ah, al, bh, bl = ready
        if at + ROWS in starts:
            ready = ratios(at + ROWS)
        sums_q.append(
            dot(f_two, ah, 1, 1) + dot(f_two, al, 1, 1) + dot(g_two, bh, 1, 1) + dot(g_two, bl, 1, 1)
        )
        q_part = q_two[:, at : at + ROWS]
        sum_a = sum_a + (dot(q_part, ah, 1, 0) + dot(q_part, al, 1, 0))
        sum_b = sum_b + (dot(q_part, bh, 1, 0) + dot(q_part, bl, 1, 0))
    return fold(jnp.concatenate(sums_q, 1)), fold(sum_a), fold(sum_b)


def near_at(y, g):
    return (y * N_XC + g) ^ NEAR_FIRST


def far_at(i, h):
    return (i * N_ZH + h) ^ FAR_FIRST


def wide_at(row, g):
    return (row * N_XC + g) ^ WIDE_FIRST


def line_at(q, h):
    return (q * N_ZH + h) ^ LINE_FIRST


def zq_of(idx):
    return (idx[0] >> 5) & 3


def near_of(idx):
    return ((idx[0] >> 1) & 6) | (idx[0] & 1)


def y_of(idx):
    return idx[0] >> 7


def halves(a, b):
    left = lax.broadcasted_iota(jnp.int32, a.shape, 1) < 64
    return jnp.where(left, a, roll(b, 64)), jnp.where(left, roll(a, 64), b)


def block_of_lane():
    return lax.broadcasted_iota(jnp.int32, (4, LANES), 1) // 16


def first_kernel(idx, shares_ref, freqs_ref, far_out, q_out, f_tmp):
    raw = shares_ref[...]
    own = raw / jnp.sum(raw, axis=0, keepdims=True)
    q_out[...] = jnp.zeros_like(q_out)
    f_tmp[...] = jnp.zeros_like(f_tmp)
    q_out[:, 0:64] = own[0:8]
    q_out[0:4, 64:128] = own[8:12]
    for j in range(3):
        f_tmp[0:4, 16 * j : 16 * j + 16] = freqs_ref[4 * j : 4 * j + 4, :]
    turned = pltpu.roll(f_tmp[...], 16 * zl_of(idx), 1)
    for h in range(N_ZH):
        sent = jnp.where(zh_of(idx) == h, turned, q_out[...])
        for i in range(N_ZL):
            far_out[far_at(i, h)] = sent


def first_near_kernel(idx, far_in, q_in, near_out, f_out):
    zh = zh_of(idx)
    block = block_of_lane()
    freqs = [far_in[far_at(i, zh), 0:4] for i in range(N_ZL)]
    for j in range(3):
        got = freqs[0]
        for i in range(1, N_ZL):
            got = jnp.where(block == (i + j) % 8, freqs[i], got)
        f_out[j] = roll(got, -16 * j)
    own, other = q_in[...], far_in[far_at(zl_of(idx), 1 - zh)]
    low, high = halves(jnp.where(zh == 0, own, other), jnp.where(zh == 0, other, own))
    for s in range(N_NEAR):
        near_out[3 * s : 3 * s + 3] = f_out[...]
    for g in range(N_XC):
        s = 3 * near_at(y_of(idx), g)
        near_out[s] = low[0:4]
        near_out[s + 1] = low[4:8]
        near_out[s + 2] = high[0:4]


def shares_of(idx, near_in):
    rows = [[], [], []]
    for x in range(4):
        for j in range(3):
            a, b = (near_in[3 * near_at(y_of(idx), 2 * x + c) + j] for c in range(2))
            rows[j].extend(halves(a, b))
    return padded(rows)


def freqs_of(idx, near_in, f_in):
    rows = [[], [], []]
    for y in range(N_Y):
        for j in range(3):
            got = near_in[3 * near_at(y, near_of(idx)) + j]
            rows[j].append(jnp.where(y_of(idx) == y, f_in[j], got))
    return padded(rows)


def padded(rows):
    rows = [jnp.concatenate(row, 1) for row in rows]
    return jnp.concatenate([*rows, jnp.zeros_like(rows[0])], 0)


def turned_tiles(x):
    return jnp.concatenate([roll(x[:, tile(t)], 64) for t in range(x.shape[1] // LANES)], 1)


def left_of(rows):
    return lax.broadcasted_iota(jnp.int32, (rows, LANES), 1) < 64


def one_kernel(idx, dosage_ref, near_in, own_f_in, slots, q_out, f_out, sq_tmp, sa_tmp, sq_turn, sa_turn):
    shares = shares_of(idx, near_in)
    freqs = freqs_of(idx, near_in, own_f_in)
    q_out[...] = shares
    f_out[...] = freqs
    sum_q, sum_a, sum_b = block_sums(dosage_ref, shares, freqs)
    sq_tmp[...] = sum_q
    sa_tmp[0:12] = sum_a[0:12]
    sa_tmp[12:24] = sum_b[0:12]
    sq_turn[...] = turned_tiles(sum_q)
    sa_turn[...] = turned_tiles(sa_tmp[...])
    left = left_of(3)
    for w in range(N_WIDE):
        t, q = divmod(w, 4)
        a = (sq_turn if t % 2 else sq_tmp)[3 * q : 3 * q + 3, tile(t // 2)]
        t, q = divmod(w, 8)
        b = (sa_tmp if t % 2 else sa_turn)[3 * q : 3 * q + 3, tile(t // 2)]
        slots[w ^ WIDE_FIRST, 0:3] = jnp.where(left, a, b)


def put_line(line_out, at, rows):
    for b in range(3):
        line_out[3 * at + b] = rows[4 * b : 4 * b + 4]


def wide_sums_kernel(idx, wide_in, line_out, q_out, a_tmp):
    left = left_of(4)
    row_sums = [sum(wide_in[wide_at(r, g)] for g in range(N_XC)) for r in range(N_ROW)]
    col_sums = [sum(wide_in[wide_at(r, g)] for r in range(N_ROW)) for g in range(N_XC)]
    for i in range(4):
        q_out[3 * i : 3 * i + 3] = jnp.where(left, row_sums[i], roll(row_sums[i + 4], 64))[0:3]
        a_tmp[3 * i : 3 * i + 3] = jnp.where(left, roll(col_sums[i], 64), col_sums[i + 4])[0:3]
    for h in range(N_ZH):
        sent = jnp.where(zh_of(idx) == h, a_tmp[...], q_out[...])
        for i in range(N_ZQ):
            put_line(line_out, line_at(i, h), sent)


def line_sums_kernel(idx, line_in, q_in, wide_out, q_tmp, a_tmp):
    zh = zh_of(idx)
    for b in range(3):
        a_tmp[4 * b : 4 * b + 4] = sum(line_in[3 * line_at(i, zh) + b] for i in range(N_ZQ))
        other = line_in[3 * line_at(zq_of(idx), 1 - zh) + b]
        q_tmp[4 * b : 4 * b + 4] = q_in[4 * b : 4 * b + 4] + other
    left = left_of(3)
    row_sums, col_sums = [], []
    for i in range(8):
        at = 3 * (i % 4)
        row_sums.append(roll(q_tmp[at : at + 3], 64 * (i // 4)))
        col_sums.append(roll(a_tmp[at : at + 3], 64 * (1 - i // 4)))
    for r in range(N_ROW):
        for g in range(N_XC):
            wide_out[wide_at(r, g), 0:3] = jnp.where(left, row_sums[r], col_sums[g])


def two_kernel(idx, dosage_ref, wide_in, q_in, f_in, near_out, sq_out, own_q, own_f, sq_tmp, sa_tmp, q_tmp, f_tmp):
    left = left_of(4)
    for t in range(8):
        for q in range(4):
            a, b = (wide_in[(8 * t + 4 * half + q) ^ WIDE_FIRST] for half in range(2))
            sq_tmp[3 * q : 3 * q + 3, tile(t)] = jnp.where(left, a, roll(b, 64))[0:3]
    for t in range(4):
        for q in range(8):
            a, b = (wide_in[(16 * t + 8 * half + q) ^ WIDE_FIRST] for half in range(2))
            sa_tmp[3 * q : 3 * q + 3, tile(t)] = jnp.where(left, roll(a, 64), b)[0:3]
    q_tmp[...] = q_in[...]
    f_tmp[...] = f_in[...]
    numer = q_tmp[0:12] * sq_tmp[0:12]
    q_tmp[0:12] = (numer + 0.5) / (jnp.sum(numer, axis=0, keepdims=True) + 0.5 * K)
    old = f_tmp[0:12]
    alt_part = old * sa_tmp[0:12]
    f_tmp[0:12] = (alt_part + 0.5) / (alt_part + (1.0 - old) * sa_tmp[12:24] + 1.0)

    t = pl.multiple_of((var_of(idx) >> 1) * LANES, LANES)
    even, odd = halves(q_tmp[0:8, pl.ds(t, LANES)], q_tmp[8:16, pl.ds(t, LANES)])
    own_q[...] = jnp.where((var_of(idx) & 1) == 0, even, odd)
    t = pl.multiple_of((smp_of(idx) >> 3) * LANES, LANES)
    block = block_of_lane()
    got = f_tmp[0:4, pl.ds(t, LANES)]
    for j in range(1, 3):
        got = jnp.where(
            block == ((zl_of(idx) + j) & 7), roll(f_tmp[4 * j : 4 * j + 4, pl.ds(t, LANES)], 16 * j), got
        )
    own_f[...] = got

    sum_q, sum_a, sum_b = block_sums(dosage_ref, q_tmp[...], f_tmp[...])
    for x in range(4):
        pair = halves(sum_q[:, tile(2 * x)], sum_q[:, tile(2 * x + 1)])
        for c in range(2):
            for y in range(N_Y):
                near_out[near_at(y, 2 * x + c), 0:16] = pair[c]
    sq_out[...] = near_out[near_at(0, near_of(idx)), 0:16]
    sa_tmp[0:12] = sum_a[0:12]
    sa_tmp[12:24] = sum_b[0:12]
    for y in range(N_Y):
        near_out[near_at(y, near_of(idx))] = sa_tmp[:, tile(y)]


def last_far_kernel(idx, near_in, sq_in, far_out, q_out):
    zh, near = zh_of(idx), near_of(idx)
    sum_q = sq_in[...]
    for g in range(N_XC):
        got = near_in[near_at(y_of(idx), g), 0:16]
        sum_q = sum_q + jnp.where(near == g, 0.0, got)
    sums = sum(near_in[near_at(y, near)] for y in range(N_Y))
    parts = halves(sum_q[0:8], sum_q[8:16])
    q_out[...] = jnp.where(zh == 0, parts[0], parts[1])
    block = block_of_lane()
    turned = [roll(sums[4 * j : 4 * j + 4], 16 * j) for j in range(6)]
    for i in range(N_ZL):
        got = turned[0]
        for j in range(1, 6):
            got = jnp.where(block == (i + j) % 8, turned[j], got)
        got = jnp.concatenate([got, got], 0)
        for h in range(N_ZH):
            far_out[far_at(i, h)] = jnp.where(zh == h, got, parts[h])


def last_kernel(idx, far_in, sq_in, own_q, own_f, shares_out, freqs_out):
    zh = zh_of(idx)
    row = lax.broadcasted_iota(jnp.int32, (8, LANES), 0)
    held = (lane() < 64) | (row < 4)
    sum_q = sq_in[...] + far_in[far_at(zl_of(idx), 1 - zh)]
    numer = jnp.where(held, own_q[...] * sum_q, 0.0)
    total = jnp.sum(numer, axis=0, keepdims=True)
    total = total + pltpu.roll(total, 64, 1)
    new = (numer + 0.5) / (total + 0.5 * K)
    shares_out[0:8] = new[:, 0:64]
    shares_out[8:12] = new[0:4, 64:128]
    sums = sum(far_in[far_at(i, zh), 0:4] for i in range(N_ZL))
    alt_part = own_f[...] * sums
    ref_part = (1.0 - own_f[...]) * roll(sums, -48)
    new = (alt_part + 0.5) / (alt_part + ref_part + 1.0)
    new = pltpu.roll(jnp.concatenate([new, new], 0), (LANES - 16 * zl_of(idx)) & (LANES - 1), 1)
    for j in range(3):
        freqs_out[4 * j : 4 * j + 4] = new[0:4, 16 * j : 16 * j + 16]


def f32s(*shape):
    return jax.ShapeDtypeStruct(shape, f32)


def vmem(*shape):
    return pltpu.VMEM(shape, f32)


def call(kernel, scalars, n_in, outs, scratch, kept=True):
    spec = pl.BlockSpec(memory_space=pltpu.VMEM)
    run = pl.pallas_call(
        kernel,
        in_specs=[pl.BlockSpec(memory_space=pltpu.SMEM)] * scalars + [spec] * n_in,
        out_specs=[spec] * len(outs),
        out_shape=[pltpu.VMEM(o.shape, o.dtype) for o in outs] if kept else outs,
        scratch_shapes=scratch,
    )

    def placed(*args):
        args = args[:scalars] + tuple(
            pltpu.with_memory_space_constraint(a, pltpu.VMEM) for a in args[scalars:]
        )
        return run(*args)

    return placed


def exchange(x, axes):
    members, first = {
        NEAR: (N_NEAR, NEAR_FIRST),
        FAR: (N_FAR, FAR_FIRST),
        WIDE: (N_WIDE, WIDE_FIRST),
        LINE: (N_LINE, LINE_FIRST),
    }[axes]
    order = [[i ^ first for i in range(members)]]
    return lax.all_to_all(x, axes, 0, 0, tiled=True, axis_index_groups=order)


def body(dosage, shares_init, freqs_init):
    idx = lax.axis_index(AXES).astype(jnp.int32).reshape(1)
    samples, variants = 16 * dosage.shape[0], dosage.shape[1]
    tiles = lambda n: f32s(n, 8, LANES)
    far_slots, own_q = call(first_kernel, 1, 2, [tiles(N_FAR), f32s(8, LANES)], [vmem(8, LANES)])(
        idx, shares_init, freqs_init
    )
    far_got = exchange(far_slots, FAR)
    near_slots, own_f = call(
        first_near_kernel, 1, 2, [f32s(3 * N_NEAR, 4, LANES), f32s(3, 4, LANES)], []
    )(idx, far_got, own_q)
    near_got = exchange(near_slots, NEAR)
    slots, shares, freqs = call(
        one_kernel, 1, 3, [f32s(N_WIDE, 4, LANES), f32s(PAD, samples), f32s(PAD, variants)],
        [vmem(PAD, samples), vmem(24, variants), vmem(PAD, samples), vmem(24, variants)],
    )(idx, dosage, near_got, own_f)
    wide_got = exchange(slots, WIDE)
    line_slots, own_sum = call(
        wide_sums_kernel, 1, 1, [f32s(3 * N_LINE, 4, LANES), f32s(12, LANES)], [vmem(12, LANES)]
    )(idx, wide_got)
    line_got = exchange(line_slots, LINE)
    (wide_slots,) = call(
        line_sums_kernel, 1, 2, [f32s(N_WIDE, 4, LANES)], [vmem(12, LANES), vmem(12, LANES)]
    )(idx, line_got, own_sum)
    wide_got = exchange(wide_slots, WIDE)
    near_slots, own_sum, own_q, own_f = call(
        two_kernel, 1, 4,
        [f32s(N_NEAR, 24, LANES), f32s(PAD, LANES), f32s(8, LANES), f32s(4, LANES)],
        [vmem(PAD, samples), vmem(24, variants), vmem(PAD, samples), vmem(PAD, variants)],
    )(idx, dosage, wide_got, shares, freqs)
    near_got = exchange(near_slots, NEAR)
    far_slots, own_sum = call(last_far_kernel, 1, 2, [tiles(N_FAR), f32s(8, LANES)], [])(
        idx, near_got, own_sum
    )
    far_got = exchange(far_slots, FAR)
    return tuple(
        call(last_kernel, 1, 4, [f32s(*shares_init.shape), f32s(*freqs_init.shape)], [], False)(
            idx, far_got, own_sum, own_q, own_f
        )
    )


def solution(mesh):
    fine = Mesh(mesh.devices.reshape(SIZES), AXES)
    return jax.shard_map(
        body,
        mesh=fine,
        in_specs=(P(SMP, VAR), P(None, SMP + VAR), P(None, VAR + SMP)),
        out_specs=(P(None, SMP + VAR), P(None, VAR + SMP)),
        check_vma=False,
    )
```

```python
import jax
import jax.numpy as jnp
from jax import lax
from jax.experimental import pallas as pl
from jax.experimental.pallas import tpu as pltpu
from jax.sharding import Mesh, PartitionSpec as P

K = 12
PAD = 16
LANES = 128
ROWS = 256

AXES = ("y", "zq", "zp", "x", "zh", "c")
SIZES = (4, 4, 2, 4, 2, 2)
SMP = ("y", "zq", "zp")
VAR = ("x", "zh", "c")
NEAR = ("y", "x", "c")
FAR = ("zq", "zp", "zh")
WIDE = ("y", "zp", "x", "c")
LINE = ("zq", "zh")
N_NEAR, N_FAR, N_WIDE, N_LINE = 32, 16, 64, 8
N_Y, N_XC, N_ZL, N_ZH, N_ZQ, N_ROW = 4, 8, 8, 2, 4, 8
FAR_1, NEAR_1, WIDE_1, LINE_1, WIDE_2, NEAR_2, FAR_2 = 1, 21, 35, 1, 37, 19, 14

f32 = jnp.float32
bf16 = jnp.bfloat16


def tile(i):
    return slice(i * LANES, (i + 1) * LANES)


def var_of(idx):
    return idx[0] & 15


def smp_of(idx):
    return idx[0] >> 4


def zl_of(idx):
    return (idx[0] >> 4) & 7


def zh_of(idx):
    return (idx[0] >> 1) & 1


def lane():
    return lax.broadcasted_iota(jnp.int32, (8, LANES), 1)


def roll(x, shift):
    shift = shift % LANES
    return pltpu.roll(x, shift, 1) if shift else x


def two_parts(x):
    high = x.astype(bf16)
    return high, (x - high.astype(f32)).astype(bf16)


def three_parts(x):
    high = x.astype(bf16)
    return (high, *two_parts(x - high.astype(f32)))


def dot(a, b, over_a, over_b):
    return lax.dot_general(
        a, b, (((over_a,), (over_b,)), ((), ())), preferred_element_type=f32
    )


def fold(x):
    return x[:PAD] + x[PAD:]


def block_sums(dosage_ref, shares, freqs):
    qh, qm, ql = three_parts(shares)
    fh, fm, fl = three_parts(freqs)
    q_side = jnp.concatenate([qh, qh, qm, qh, ql, qm], 0)
    f_side = jnp.concatenate([fh, fm, fh, fl, fh, fm], 0)
    q_two = jnp.concatenate([qh, qm], 0)
    f_two = jnp.concatenate([fh, fm], 0)
    g_two = jnp.concatenate(two_parts(1.0 - freqs), 0)
    shift = 2 * lax.broadcasted_iota(jnp.int32, (16, freqs.shape[1]), 0)

    def ratios(at):
        probs = dot(q_side[:, at : at + ROWS], f_side, 0, 0)
        codes = jnp.concatenate(
            [
                jnp.bitwise_and(
                    jnp.right_shift(jnp.broadcast_to(dosage_ref[w : w + 1, :], shift.shape), shift), 3
                )
                for w in range(at // 16, (at + ROWS) // 16)
            ],
            0,
        )
        live = codes < 3
        allele = codes.astype(f32)
        ratio_alt = jnp.where(live, allele, 0.0) * (1.0 / probs)
        ratio_ref = jnp.where(live, 2.0 - allele, 0.0) * (1.0 / (1.0 - probs))
        return two_parts(ratio_alt) + two_parts(ratio_ref)

    sums_q, sum_a, sum_b = [], 0.0, 0.0
    starts = range(0, shares.shape[1], ROWS)
    ready = ratios(0)
    for at in starts:
        ah, al, bh, bl = ready
        if at + ROWS in starts:
            ready = ratios(at + ROWS)
        sums_q.append(
            dot(f_two, ah, 1, 1) + dot(f_two, al, 1, 1) + dot(g_two, bh, 1, 1) + dot(g_two, bl, 1, 1)
        )
        q_part = q_two[:, at : at + ROWS]
        sum_a = sum_a + (dot(q_part, ah, 1, 0) + dot(q_part, al, 1, 0))
        sum_b = sum_b + (dot(q_part, bh, 1, 0) + dot(q_part, bl, 1, 0))
    return fold(jnp.concatenate(sums_q, 1)), fold(sum_a), fold(sum_b)


def in_plane(y, g):
    return y * N_XC + g


def in_line(i, h):
    return i * N_ZH + h


def zq_of(idx):
    return (idx[0] >> 5) & 3


def near_of(idx):
    return ((idx[0] >> 1) & 6) | (idx[0] & 1)


def y_of(idx):
    return idx[0] >> 7


def halves(a, b):
    left = lax.broadcasted_iota(jnp.int32, a.shape, 1) < 64
    return jnp.where(left, a, roll(b, 64)), jnp.where(left, roll(a, 64), b)


def block_of_lane():
    return lax.broadcasted_iota(jnp.int32, (4, LANES), 1) // 16


def first_kernel(idx, shares_ref, freqs_ref, far_out, q_out, f_tmp):
    raw = shares_ref[...]
    own = raw / jnp.sum(raw, axis=0, keepdims=True)
    q_out[...] = jnp.zeros_like(q_out)
    f_tmp[...] = jnp.zeros_like(f_tmp)
    q_out[:, 0:64] = own[0:8]
    q_out[0:4, 64:128] = own[8:12]
    for j in range(3):
        f_tmp[0:4, 16 * j : 16 * j + 16] = freqs_ref[4 * j : 4 * j + 4, :]
    turned = pltpu.roll(f_tmp[...], 16 * zl_of(idx), 1)
    for h in range(N_ZH):
        sent = jnp.where(zh_of(idx) == h, turned, q_out[...])
        for i in range(N_ZL):
            far_out[in_line(i, h) ^ FAR_1] = sent


def first_near_kernel(idx, far_in, q_in, near_out, f_out):
    zh = zh_of(idx)
    block = block_of_lane()
    freqs = [far_in[in_line(i, zh) ^ FAR_1, 0:4] for i in range(N_ZL)]
    for j in range(3):
        got = freqs[0]
        for i in range(1, N_ZL):
            got = jnp.where(block == (i + j) % 8, freqs[i], got)
        f_out[j] = roll(got, -16 * j)
    own, other = q_in[...], far_in[in_line(zl_of(idx), 1 - zh) ^ FAR_1]
    low, high = halves(jnp.where(zh == 0, own, other), jnp.where(zh == 0, other, own))
    for s in range(N_NEAR):
        near_out[3 * s : 3 * s + 3] = f_out[...]
    for g in range(N_XC):
        s = 3 * (in_plane(y_of(idx), g) ^ NEAR_1)
        near_out[s] = low[0:4]
        near_out[s + 1] = low[4:8]
        near_out[s + 2] = high[0:4]


def shares_of(idx, near_in):
    rows = [[], [], []]
    for x in range(4):
        for j in range(3):
            a, b = (near_in[3 * (in_plane(y_of(idx), 2 * x + c) ^ NEAR_1) + j] for c in range(2))
            rows[j].extend(halves(a, b))
    return padded(rows)


def freqs_of(idx, near_in, f_in):
    rows = [[], [], []]
    for y in range(N_Y):
        for j in range(3):
            got = near_in[3 * (in_plane(y, near_of(idx)) ^ NEAR_1) + j]
            rows[j].append(jnp.where(y_of(idx) == y, f_in[j], got))
    return padded(rows)


def padded(rows):
    rows = [jnp.concatenate(row, 1) for row in rows]
    return jnp.concatenate([*rows, jnp.zeros_like(rows[0])], 0)


def turned_tiles(x):
    return jnp.concatenate([roll(x[:, tile(t)], 64) for t in range(x.shape[1] // LANES)], 1)


def left_of(rows):
    return lax.broadcasted_iota(jnp.int32, (rows, LANES), 1) < 64


def one_kernel(idx, dosage_ref, near_in, own_f_in, slots, q_out, f_out, sq_tmp, sa_tmp, sq_turn, sa_turn):
    shares = shares_of(idx, near_in)
    freqs = freqs_of(idx, near_in, own_f_in)
    q_out[...] = shares
    f_out[...] = freqs
    sum_q, sum_a, sum_b = block_sums(dosage_ref, shares, freqs)
    sq_tmp[...] = sum_q
    sa_tmp[0:12] = sum_a[0:12]
    sa_tmp[12:24] = sum_b[0:12]
    sq_turn[...] = turned_tiles(sum_q)
    sa_turn[...] = turned_tiles(sa_tmp[...])
    left = left_of(3)
    for w in range(N_WIDE):
        t, q = divmod(w, 4)
        a = (sq_turn if t % 2 else sq_tmp)[3 * q : 3 * q + 3, tile(t // 2)]
        t, q = divmod(w, 8)
        b = (sa_tmp if t % 2 else sa_turn)[3 * q : 3 * q + 3, tile(t // 2)]
        slots[w ^ WIDE_1, 0:3] = jnp.where(left, a, b)


def put_line(line_out, at, rows):
    for b in range(3):
        line_out[3 * at + b] = rows[4 * b : 4 * b + 4]


def wide_sums_kernel(idx, wide_in, line_out, q_out, a_tmp):
    left = left_of(4)
    row_sums = [sum(wide_in[in_plane(r, g) ^ WIDE_1] for g in range(N_XC)) for r in range(N_ROW)]
    col_sums = [sum(wide_in[in_plane(r, g) ^ WIDE_1] for r in range(N_ROW)) for g in range(N_XC)]
    for i in range(4):
        q_out[3 * i : 3 * i + 3] = jnp.where(left, row_sums[i], roll(row_sums[i + 4], 64))[0:3]
        a_tmp[3 * i : 3 * i + 3] = jnp.where(left, roll(col_sums[i], 64), col_sums[i + 4])[0:3]
    for h in range(N_ZH):
        sent = jnp.where(zh_of(idx) == h, a_tmp[...], q_out[...])
        for i in range(N_ZQ):
            put_line(line_out, in_line(i, h) ^ LINE_1, sent)


def line_sums_kernel(idx, line_in, q_in, wide_out, q_tmp, a_tmp):
    zh = zh_of(idx)
    for b in range(3):
        a_tmp[4 * b : 4 * b + 4] = sum(line_in[3 * (in_line(i, zh) ^ LINE_1) + b] for i in range(N_ZQ))
        other = line_in[3 * (in_line(zq_of(idx), 1 - zh) ^ LINE_1) + b]
        q_tmp[4 * b : 4 * b + 4] = q_in[4 * b : 4 * b + 4] + other
    left = left_of(3)
    row_sums, col_sums = [], []
    for i in range(8):
        at = 3 * (i % 4)
        row_sums.append(roll(q_tmp[at : at + 3], 64 * (i // 4)))
        col_sums.append(roll(a_tmp[at : at + 3], 64 * (1 - i // 4)))
    for r in range(N_ROW):
        for g in range(N_XC):
            wide_out[in_plane(r, g) ^ WIDE_2, 0:3] = jnp.where(left, row_sums[r], col_sums[g])


def two_kernel(idx, dosage_ref, wide_in, q_in, f_in, near_out, sq_out, own_q, own_f, sq_tmp, sa_tmp, q_tmp, f_tmp):
    left = left_of(4)
    for t in range(8):
        for q in range(4):
            a, b = (wide_in[(8 * t + 4 * half + q) ^ WIDE_2] for half in range(2))
            sq_tmp[3 * q : 3 * q + 3, tile(t)] = jnp.where(left, a, roll(b, 64))[0:3]
    for t in range(4):
        for q in range(8):
            a, b = (wide_in[(16 * t + 8 * half + q) ^ WIDE_2] for half in range(2))
            sa_tmp[3 * q : 3 * q + 3, tile(t)] = jnp.where(left, roll(a, 64), b)[0:3]
    q_tmp[...] = q_in[...]
    f_tmp[...] = f_in[...]
    numer = q_tmp[0:12] * sq_tmp[0:12]
    q_tmp[0:12] = (numer + 0.5) / (jnp.sum(numer, axis=0, keepdims=True) + 0.5 * K)
    old = f_tmp[0:12]
    alt_part = old * sa_tmp[0:12]
    f_tmp[0:12] = (alt_part + 0.5) / (alt_part + (1.0 - old) * sa_tmp[12:24] + 1.0)

    t = pl.multiple_of((var_of(idx) >> 1) * LANES, LANES)
    even, odd = halves(q_tmp[0:8, pl.ds(t, LANES)], q_tmp[8:16, pl.ds(t, LANES)])
    own_q[...] = jnp.where((var_of(idx) & 1) == 0, even, odd)
    t = pl.multiple_of((smp_of(idx) >> 3) * LANES, LANES)
    block = block_of_lane()
    got = f_tmp[0:4, pl.ds(t, LANES)]
    for j in range(1, 3):
        got = jnp.where(
            block == ((zl_of(idx) + j) & 7), roll(f_tmp[4 * j : 4 * j + 4, pl.ds(t, LANES)], 16 * j), got
        )
    own_f[...] = got

    sum_q, sum_a, sum_b = block_sums(dosage_ref, q_tmp[...], f_tmp[...])
    for x in range(4):
        pair = halves(sum_q[:, tile(2 * x)], sum_q[:, tile(2 * x + 1)])
        for c in range(2):
            for y in range(N_Y):
                near_out[in_plane(y, 2 * x + c) ^ NEAR_2, 0:16] = pair[c]
    sq_out[...] = near_out[in_plane(0, near_of(idx)) ^ NEAR_2, 0:16]
    sa_tmp[0:12] = sum_a[0:12]
    sa_tmp[12:24] = sum_b[0:12]
    for y in range(N_Y):
        near_out[in_plane(y, near_of(idx)) ^ NEAR_2] = sa_tmp[:, tile(y)]


def last_far_kernel(idx, near_in, sq_in, far_out, q_out):
    zh, near = zh_of(idx), near_of(idx)
    sum_q = sq_in[...]
    for g in range(N_XC):
        got = near_in[in_plane(y_of(idx), g) ^ NEAR_2, 0:16]
        sum_q = sum_q + jnp.where(near == g, 0.0, got)
    sums = sum(near_in[in_plane(y, near) ^ NEAR_2] for y in range(N_Y))
    parts = halves(sum_q[0:8], sum_q[8:16])
    q_out[...] = jnp.where(zh == 0, parts[0], parts[1])
    block = block_of_lane()
    turned = [roll(sums[4 * j : 4 * j + 4], 16 * j) for j in range(6)]
    for i in range(N_ZL):
        got = turned[0]
        for j in range(1, 6):
            got = jnp.where(block == (i + j) % 8, turned[j], got)
        got = jnp.concatenate([got, got], 0)
        for h in range(N_ZH):
            far_out[in_line(i, h) ^ FAR_2] = jnp.where(zh == h, got, parts[h])


def last_kernel(idx, far_in, sq_in, own_q, own_f, shares_out, freqs_out):
    zh = zh_of(idx)
    row = lax.broadcasted_iota(jnp.int32, (8, LANES), 0)
    held = (lane() < 64) | (row < 4)
    sum_q = sq_in[...] + far_in[in_line(zl_of(idx), 1 - zh) ^ FAR_2]
    numer = jnp.where(held, own_q[...] * sum_q, 0.0)
    total = jnp.sum(numer, axis=0, keepdims=True)
    total = total + pltpu.roll(total, 64, 1)
    new = (numer + 0.5) / (total + 0.5 * K)
    shares_out[0:8] = new[:, 0:64]
    shares_out[8:12] = new[0:4, 64:128]
    sums = sum(far_in[in_line(i, zh) ^ FAR_2, 0:4] for i in range(N_ZL))
    alt_part = own_f[...] * sums
    ref_part = (1.0 - own_f[...]) * roll(sums, -48)
    new = (alt_part + 0.5) / (alt_part + ref_part + 1.0)
    new = pltpu.roll(jnp.concatenate([new, new], 0), (LANES - 16 * zl_of(idx)) & (LANES - 1), 1)
    for j in range(3):
        freqs_out[4 * j : 4 * j + 4] = new[0:4, 16 * j : 16 * j + 16]


def f32s(*shape):
    return jax.ShapeDtypeStruct(shape, f32)


def vmem(*shape):
    return pltpu.VMEM(shape, f32)


def call(kernel, scalars, n_in, outs, scratch, kept=True):
    spec = pl.BlockSpec(memory_space=pltpu.VMEM)
    run = pl.pallas_call(
        kernel,
        in_specs=[pl.BlockSpec(memory_space=pltpu.SMEM)] * scalars + [spec] * n_in,
        out_specs=[spec] * len(outs),
        out_shape=[pltpu.VMEM(o.shape, o.dtype) for o in outs] if kept else outs,
        scratch_shapes=scratch,
    )

    def placed(*args):
        args = args[:scalars] + tuple(
            pltpu.with_memory_space_constraint(a, pltpu.VMEM) for a in args[scalars:]
        )
        return run(*args)

    return placed


def exchange(x, axes, first):
    members = 1
    for axis in axes:
        members *= SIZES[AXES.index(axis)]
    order = [[i ^ first for i in range(members)]]
    return lax.all_to_all(x, axes, 0, 0, tiled=True, axis_index_groups=order)


def body(dosage, shares_init, freqs_init):
    idx = lax.axis_index(AXES).astype(jnp.int32).reshape(1)
    samples, variants = 16 * dosage.shape[0], dosage.shape[1]
    tiles = lambda n: f32s(n, 8, LANES)
    far_slots, own_q = call(first_kernel, 1, 2, [tiles(N_FAR), f32s(8, LANES)], [vmem(8, LANES)])(
        idx, shares_init, freqs_init
    )
    far_got = exchange(far_slots, FAR, FAR_1)
    near_slots, own_f = call(
        first_near_kernel, 1, 2, [f32s(3 * N_NEAR, 4, LANES), f32s(3, 4, LANES)], []
    )(idx, far_got, own_q)
    near_got = exchange(near_slots, NEAR, NEAR_1)
    slots, shares, freqs = call(
        one_kernel, 1, 3, [f32s(N_WIDE, 4, LANES), f32s(PAD, samples), f32s(PAD, variants)],
        [vmem(PAD, samples), vmem(24, variants), vmem(PAD, samples), vmem(24, variants)],
    )(idx, dosage, near_got, own_f)
    wide_got = exchange(slots, WIDE, WIDE_1)
    line_slots, own_sum = call(
        wide_sums_kernel, 1, 1, [f32s(3 * N_LINE, 4, LANES), f32s(12, LANES)], [vmem(12, LANES)]
    )(idx, wide_got)
    line_got = exchange(line_slots, LINE, LINE_1)
    (wide_slots,) = call(
        line_sums_kernel, 1, 2, [f32s(N_WIDE, 4, LANES)], [vmem(12, LANES), vmem(12, LANES)]
    )(idx, line_got, own_sum)
    wide_got = exchange(wide_slots, WIDE, WIDE_2)
    near_slots, own_sum, own_q, own_f = call(
        two_kernel, 1, 4,
        [f32s(N_NEAR, 24, LANES), f32s(PAD, LANES), f32s(8, LANES), f32s(4, LANES)],
        [vmem(PAD, samples), vmem(24, variants), vmem(PAD, samples), vmem(PAD, variants)],
    )(idx, dosage, wide_got, shares, freqs)
    near_got = exchange(near_slots, NEAR, NEAR_2)
    far_slots, own_sum = call(last_far_kernel, 1, 2, [tiles(N_FAR), f32s(8, LANES)], [])(
        idx, near_got, own_sum
    )
    far_got = exchange(far_slots, FAR, FAR_2)
    return tuple(
        call(last_kernel, 1, 4, [f32s(*shares_init.shape), f32s(*freqs_init.shape)], [], False)(
            idx, far_got, own_sum, own_q, own_f
        )
    )


def solution(mesh):
    fine = Mesh(mesh.devices.reshape(SIZES), AXES)
    return jax.shard_map(
        body,
        mesh=fine,
        in_specs=(P(SMP, VAR), P(None, SMP + VAR), P(None, VAR + SMP)),
        out_specs=(P(None, SMP + VAR), P(None, VAR + SMP)),
        check_vma=False,
    )
```

```python
import jax
import jax.numpy as jnp
from jax import lax
from jax.experimental import pallas as pl
from jax.experimental.pallas import tpu as pltpu
from jax.sharding import Mesh, PartitionSpec as P

K = 12
PAD = 16
LANES = 128
ROWS = 256

AXES = ("y", "zq", "zp", "x", "zh", "c")
SIZES = (4, 4, 2, 4, 2, 2)
SMP = ("y", "zq", "zp")
VAR = ("x", "zh", "c")
NEAR = ("y", "x", "c")
FAR = ("zq", "zp", "zh")
WIDE = ("y", "zp", "x", "c")
LINE = ("zq", "zh")
N_NEAR, N_FAR, N_WIDE, N_LINE = 32, 16, 64, 8
N_Y, N_XC, N_ZL, N_ZH, N_ZQ, N_ROW = 4, 8, 8, 2, 4, 8
FAR_1 = LINE_1 = FAR_2 = 1
NEAR_1 = NEAR_2 = 21
WIDE_1 = WIDE_2 = 37

f32 = jnp.float32
bf16 = jnp.bfloat16


def tile(i):
    return slice(i * LANES, (i + 1) * LANES)


def var_of(idx):
    return idx[0] & 15


def smp_of(idx):
    return idx[0] >> 4


def zl_of(idx):
    return (idx[0] >> 4) & 7


def zh_of(idx):
    return (idx[0] >> 1) & 1


def lane():
    return lax.broadcasted_iota(jnp.int32, (8, LANES), 1)


def roll(x, shift):
    shift = shift % LANES
    return pltpu.roll(x, shift, 1) if shift else x


def two_parts(x):
    high = x.astype(bf16)
    return high, (x - high.astype(f32)).astype(bf16)


def three_parts(x):
    high = x.astype(bf16)
    return (high, *two_parts(x - high.astype(f32)))


def dot(a, b, over_a, over_b):
    return lax.dot_general(
        a, b, (((over_a,), (over_b,)), ((), ())), preferred_element_type=f32
    )


def fold(x):
    return x[:PAD] + x[PAD:]


def block_sums(dosage_ref, shares, freqs):
    qh, qm, ql = three_parts(shares)
    fh, fm, fl = three_parts(freqs)
    q_side = jnp.concatenate([qh, qh, qm, qh, ql, qm], 0)
    f_side = jnp.concatenate([fh, fm, fh, fl, fh, fm], 0)
    q_two = jnp.concatenate([qh, qm], 0)
    f_two = jnp.concatenate([fh, fm], 0)
    g_two = jnp.concatenate(two_parts(1.0 - freqs), 0)
    shift = 2 * lax.broadcasted_iota(jnp.int32, (16, freqs.shape[1]), 0)

    def ratios(at):
        probs = dot(q_side[:, at : at + ROWS], f_side, 0, 0)
        codes = jnp.concatenate(
            [
                jnp.bitwise_and(
                    jnp.right_shift(jnp.broadcast_to(dosage_ref[w : w + 1, :], shift.shape), shift), 3
                )
                for w in range(at // 16, (at + ROWS) // 16)
            ],
            0,
        )
        live = codes < 3
        allele = codes.astype(f32)
        ratio_alt = jnp.where(live, allele, 0.0) * (1.0 / probs)
        ratio_ref = jnp.where(live, 2.0 - allele, 0.0) * (1.0 / (1.0 - probs))
        return two_parts(ratio_alt) + two_parts(ratio_ref)

    sums_q, sum_a, sum_b = [], 0.0, 0.0
    starts = range(0, shares.shape[1], ROWS)
    ready = ratios(0)
    for at in starts:
        ah, al, bh, bl = ready
        if at + ROWS in starts:
            ready = ratios(at + ROWS)
        sums_q.append(
            dot(f_two, ah, 1, 1) + dot(f_two, al, 1, 1) + dot(g_two, bh, 1, 1) + dot(g_two, bl, 1, 1)
        )
        q_part = q_two[:, at : at + ROWS]
        sum_a = sum_a + (dot(q_part, ah, 1, 0) + dot(q_part, al, 1, 0))
        sum_b = sum_b + (dot(q_part, bh, 1, 0) + dot(q_part, bl, 1, 0))
    return fold(jnp.concatenate(sums_q, 1)), fold(sum_a), fold(sum_b)


def in_plane(y, g):
    return y * N_XC + g


def in_line(i, h):
    return i * N_ZH + h


def zq_of(idx):
    return (idx[0] >> 5) & 3


def near_of(idx):
    return ((idx[0] >> 1) & 6) | (idx[0] & 1)


def y_of(idx):
    return idx[0] >> 7


def halves(a, b):
    left = lax.broadcasted_iota(jnp.int32, a.shape, 1) < 64
    return jnp.where(left, a, roll(b, 64)), jnp.where(left, roll(a, 64), b)


def block_of_lane():
    return lax.broadcasted_iota(jnp.int32, (4, LANES), 1) // 16


def put_far(far_out, at, rows):
    for b in range(3):
        far_out[3 * at + b] = rows[2 * b : 2 * b + 2]


def get_far(far_in, at, pairs):
    return jnp.concatenate([far_in[3 * at + b] for b in range(pairs)], 0)


def first_kernel(idx, shares_ref, freqs_ref, far_out, q_out, f_tmp):
    raw = shares_ref[...]
    own = raw / jnp.sum(raw, axis=0, keepdims=True)
    q_out[...] = jnp.zeros_like(q_out)
    f_tmp[...] = jnp.zeros_like(f_tmp)
    q_out[0:6, 0:64] = own[0:6]
    q_out[0:6, 64:128] = own[6:12]
    for j in range(3):
        f_tmp[0:4, 16 * j : 16 * j + 16] = freqs_ref[4 * j : 4 * j + 4, :]
    turned = pltpu.roll(f_tmp[...], 16 * zl_of(idx), 1)
    for h in range(N_ZH):
        sent = jnp.where(zh_of(idx) == h, turned, q_out[...])
        for i in range(N_ZL):
            put_far(far_out, in_line(i, h) ^ FAR_1, sent)


def first_near_kernel(idx, far_in, q_in, near_out, f_out, q_tmp):
    zh = zh_of(idx)
    block = block_of_lane()
    freqs = [get_far(far_in, in_line(i, zh) ^ FAR_1, 2) for i in range(N_ZL)]
    for j in range(3):
        got = freqs[0]
        for i in range(1, N_ZL):
            got = jnp.where(block == (i + j) % 8, freqs[i], got)
        f_out[j] = roll(got, -16 * j)
    own, other = q_in[0:6], get_far(far_in, in_line(zl_of(idx), 1 - zh) ^ FAR_1, 3)
    q_tmp[0:6], q_tmp[6:12] = halves(jnp.where(zh == 0, own, other), jnp.where(zh == 0, other, own))
    for s in range(N_NEAR):
        near_out[3 * s : 3 * s + 3] = f_out[...]
    for g in range(N_XC):
        s = 3 * (in_plane(y_of(idx), g) ^ NEAR_1)
        for j in range(3):
            near_out[s + j] = q_tmp[4 * j : 4 * j + 4]


def shares_of(idx, near_in):
    rows = [[], [], []]
    for x in range(4):
        for j in range(3):
            a, b = (near_in[3 * (in_plane(y_of(idx), 2 * x + c) ^ NEAR_1) + j] for c in range(2))
            rows[j].extend(halves(a, b))
    return padded(rows)


def freqs_of(idx, near_in, f_in):
    rows = [[], [], []]
    for y in range(N_Y):
        for j in range(3):
            got = near_in[3 * (in_plane(y, near_of(idx)) ^ NEAR_1) + j]
            rows[j].append(jnp.where(y_of(idx) == y, f_in[j], got))
    return padded(rows)


def padded(rows):
    rows = [jnp.concatenate(row, 1) for row in rows]
    return jnp.concatenate([*rows, jnp.zeros_like(rows[0])], 0)


def turned_tiles(x):
    return jnp.concatenate([roll(x[:, tile(t)], 64) for t in range(x.shape[1] // LANES)], 1)


def left_of(rows):
    return lax.broadcasted_iota(jnp.int32, (rows, LANES), 1) < 64


def one_kernel(idx, dosage_ref, near_in, own_f_in, slots, q_out, f_out, sq_tmp, sa_tmp, sq_turn, sa_turn):
    shares = shares_of(idx, near_in)
    freqs = freqs_of(idx, near_in, own_f_in)
    q_out[...] = shares
    f_out[...] = freqs
    sum_q, sum_a, sum_b = block_sums(dosage_ref, shares, freqs)
    sq_tmp[...] = sum_q
    sa_tmp[0:12] = sum_a[0:12]
    sa_tmp[12:24] = sum_b[0:12]
    sq_turn[...] = turned_tiles(sum_q)
    sa_turn[...] = turned_tiles(sa_tmp[...])
    left = left_of(3)
    for w in range(N_WIDE):
        t, q = divmod(w, 4)
        a = (sq_turn if t % 2 else sq_tmp)[3 * q : 3 * q + 3, tile(t // 2)]
        t, q = divmod(w, 8)
        b = (sa_tmp if t % 2 else sa_turn)[3 * q : 3 * q + 3, tile(t // 2)]
        slots[w ^ WIDE_1, 0:3] = jnp.where(left, a, b)


def put_line(line_out, at, rows):
    for b in range(3):
        line_out[3 * at + b] = rows[4 * b : 4 * b + 4]


def wide_sums_kernel(idx, wide_in, line_out, q_out, a_tmp):
    left = left_of(4)
    row_sums = [sum(wide_in[in_plane(r, g) ^ WIDE_1] for g in range(N_XC)) for r in range(N_ROW)]
    col_sums = [sum(wide_in[in_plane(r, g) ^ WIDE_1] for r in range(N_ROW)) for g in range(N_XC)]
    for i in range(4):
        q_out[3 * i : 3 * i + 3] = jnp.where(left, row_sums[i], roll(row_sums[i + 4], 64))[0:3]
        a_tmp[3 * i : 3 * i + 3] = jnp.where(left, roll(col_sums[i], 64), col_sums[i + 4])[0:3]
    for h in range(N_ZH):
        sent = jnp.where(zh_of(idx) == h, a_tmp[...], q_out[...])
        for i in range(N_ZQ):
            put_line(line_out, in_line(i, h) ^ LINE_1, sent)


def line_sums_kernel(idx, line_in, q_in, wide_out, q_tmp, a_tmp):
    zh = zh_of(idx)
    for b in range(3):
        a_tmp[4 * b : 4 * b + 4] = sum(line_in[3 * (in_line(i, zh) ^ LINE_1) + b] for i in range(N_ZQ))
        other = line_in[3 * (in_line(zq_of(idx), 1 - zh) ^ LINE_1) + b]
        q_tmp[4 * b : 4 * b + 4] = q_in[4 * b : 4 * b + 4] + other
    left = left_of(3)
    row_sums, col_sums = [], []
    for i in range(8):
        at = 3 * (i % 4)
        row_sums.append(roll(q_tmp[at : at + 3], 64 * (i // 4)))
        col_sums.append(roll(a_tmp[at : at + 3], 64 * (1 - i // 4)))
    for r in range(N_ROW):
        for g in range(N_XC):
            wide_out[in_plane(r, g) ^ WIDE_2, 0:3] = jnp.where(left, row_sums[r], col_sums[g])


def two_kernel(idx, dosage_ref, wide_in, q_in, f_in, near_out, sq_out, own_q, own_f, sq_tmp, sa_tmp, q_tmp, f_tmp):
    left = left_of(4)
    for t in range(8):
        for q in range(4):
            a, b = (wide_in[(8 * t + 4 * half + q) ^ WIDE_2] for half in range(2))
            sq_tmp[3 * q : 3 * q + 3, tile(t)] = jnp.where(left, a, roll(b, 64))[0:3]
    for t in range(4):
        for q in range(8):
            a, b = (wide_in[(16 * t + 8 * half + q) ^ WIDE_2] for half in range(2))
            sa_tmp[3 * q : 3 * q + 3, tile(t)] = jnp.where(left, roll(a, 64), b)[0:3]
    q_tmp[...] = q_in[...]
    f_tmp[...] = f_in[...]
    numer = q_tmp[0:12] * sq_tmp[0:12]
    q_tmp[0:12] = (numer + 0.5) / (jnp.sum(numer, axis=0, keepdims=True) + 0.5 * K)
    old = f_tmp[0:12]
    alt_part = old * sa_tmp[0:12]
    f_tmp[0:12] = (alt_part + 0.5) / (alt_part + (1.0 - old) * sa_tmp[12:24] + 1.0)

    t = pl.multiple_of((var_of(idx) >> 1) * LANES, LANES)
    even, odd = halves(q_tmp[0:6, pl.ds(t, LANES)], q_tmp[6:12, pl.ds(t, LANES)])
    own_q[...] = jnp.where((var_of(idx) & 1) == 0, even, odd)
    t = pl.multiple_of((smp_of(idx) >> 3) * LANES, LANES)
    block = block_of_lane()
    got = f_tmp[0:4, pl.ds(t, LANES)]
    for j in range(1, 3):
        got = jnp.where(
            block == ((zl_of(idx) + j) & 7), roll(f_tmp[4 * j : 4 * j + 4, pl.ds(t, LANES)], 16 * j), got
        )
    own_f[...] = got

    sum_q, sum_a, sum_b = block_sums(dosage_ref, q_tmp[...], f_tmp[...])
    for x in range(4):
        pair = halves(sum_q[:, tile(2 * x)], sum_q[:, tile(2 * x + 1)])
        for c in range(2):
            for y in range(N_Y):
                near_out[in_plane(y, 2 * x + c) ^ NEAR_2, 0:16] = pair[c]
    sq_out[...] = near_out[in_plane(0, near_of(idx)) ^ NEAR_2, 0:16]
    sa_tmp[0:12] = sum_a[0:12]
    sa_tmp[12:24] = sum_b[0:12]
    for y in range(N_Y):
        near_out[in_plane(y, near_of(idx)) ^ NEAR_2] = sa_tmp[:, tile(y)]


def last_far_kernel(idx, near_in, sq_in, far_out, q_out):
    zh, near = zh_of(idx), near_of(idx)
    sum_q = sq_in[...]
    for g in range(N_XC):
        got = near_in[in_plane(y_of(idx), g) ^ NEAR_2, 0:16]
        sum_q = sum_q + jnp.where(near == g, 0.0, got)
    sums = sum(near_in[in_plane(y, near) ^ NEAR_2] for y in range(N_Y))
    parts = halves(sum_q[0:6], sum_q[6:12])
    q_out[...] = jnp.where(zh == 0, parts[0], parts[1])
    block = block_of_lane()
    turned = [roll(sums[4 * j : 4 * j + 4], 16 * j) for j in range(6)]
    for i in range(N_ZL):
        got = turned[0]
        for j in range(1, 6):
            got = jnp.where(block == (i + j) % 8, turned[j], got)
        got = jnp.concatenate([got, got[0:2]], 0)
        for h in range(N_ZH):
            put_far(far_out, in_line(i, h) ^ FAR_2, jnp.where(zh == h, got, parts[h]))


def last_kernel(idx, far_in, sq_in, own_q, own_f, shares_out, freqs_out):
    zh = zh_of(idx)
    sum_q = sq_in[...] + get_far(far_in, in_line(zl_of(idx), 1 - zh) ^ FAR_2, 3)
    numer = own_q[...] * sum_q
    total = jnp.sum(numer, axis=0, keepdims=True)
    total = total + pltpu.roll(total, 64, 1)
    new = (numer + 0.5) / (total + 0.5 * K)
    shares_out[0:6] = new[:, 0:64]
    shares_out[6:12] = new[:, 64:128]
    sums = sum(get_far(far_in, in_line(i, zh) ^ FAR_2, 2) for i in range(N_ZL))
    alt_part = own_f[...] * sums
    ref_part = (1.0 - own_f[...]) * roll(sums, -48)
    new = (alt_part + 0.5) / (alt_part + ref_part + 1.0)
    new = pltpu.roll(jnp.concatenate([new, new], 0), (LANES - 16 * zl_of(idx)) & (LANES - 1), 1)
    for j in range(3):
        freqs_out[4 * j : 4 * j + 4] = new[0:4, 16 * j : 16 * j + 16]


def f32s(*shape):
    return jax.ShapeDtypeStruct(shape, f32)


def vmem(*shape):
    return pltpu.VMEM(shape, f32)


def call(kernel, scalars, n_in, outs, scratch, kept=True):
    spec = pl.BlockSpec(memory_space=pltpu.VMEM)
    run = pl.pallas_call(
        kernel,
        in_specs=[pl.BlockSpec(memory_space=pltpu.SMEM)] * scalars + [spec] * n_in,
        out_specs=[spec] * len(outs),
        out_shape=[pltpu.VMEM(o.shape, o.dtype) for o in outs] if kept else outs,
        scratch_shapes=scratch,
    )

    def placed(*args):
        args = args[:scalars] + tuple(
            pltpu.with_memory_space_constraint(a, pltpu.VMEM) for a in args[scalars:]
        )
        return run(*args)

    return placed


def exchange(x, axes, first):
    members = 1
    for axis in axes:
        members *= SIZES[AXES.index(axis)]
    order = [[i ^ first for i in range(members)]]
    return lax.all_to_all(x, axes, 0, 0, tiled=True, axis_index_groups=order)


def body(dosage, shares_init, freqs_init):
    idx = lax.axis_index(AXES).astype(jnp.int32).reshape(1)
    samples, variants = 16 * dosage.shape[0], dosage.shape[1]
    pairs = f32s(3 * N_FAR, 2, LANES)
    far_slots, own_q = call(first_kernel, 1, 2, [pairs, f32s(8, LANES)], [vmem(8, LANES)])(
        idx, shares_init, freqs_init
    )
    far_got = exchange(far_slots, FAR, FAR_1)
    near_slots, own_f = call(
        first_near_kernel, 1, 2, [f32s(3 * N_NEAR, 4, LANES), f32s(3, 4, LANES)], [vmem(12, LANES)]
    )(idx, far_got, own_q)
    near_got = exchange(near_slots, NEAR, NEAR_1)
    slots, shares, freqs = call(
        one_kernel, 1, 3, [f32s(N_WIDE, 4, LANES), f32s(PAD, samples), f32s(PAD, variants)],
        [vmem(PAD, samples), vmem(24, variants), vmem(PAD, samples), vmem(24, variants)],
    )(idx, dosage, near_got, own_f)
    wide_got = exchange(slots, WIDE, WIDE_1)
    line_slots, own_sum = call(
        wide_sums_kernel, 1, 1, [f32s(3 * N_LINE, 4, LANES), f32s(12, LANES)], [vmem(12, LANES)]
    )(idx, wide_got)
    line_got = exchange(line_slots, LINE, LINE_1)
    (wide_slots,) = call(
        line_sums_kernel, 1, 2, [f32s(N_WIDE, 4, LANES)], [vmem(12, LANES), vmem(12, LANES)]
    )(idx, line_got, own_sum)
    wide_got = exchange(wide_slots, WIDE, WIDE_2)
    near_slots, own_sum, own_q, own_f = call(
        two_kernel, 1, 4,
        [f32s(N_NEAR, 24, LANES), f32s(PAD, LANES), f32s(6, LANES), f32s(4, LANES)],
        [vmem(PAD, samples), vmem(24, variants), vmem(PAD, samples), vmem(PAD, variants)],
    )(idx, dosage, wide_got, shares, freqs)
    near_got = exchange(near_slots, NEAR, NEAR_2)
    far_slots, own_sum = call(last_far_kernel, 1, 2, [pairs, f32s(6, LANES)], [])(
        idx, near_got, own_sum
    )
    far_got = exchange(far_slots, FAR, FAR_2)
    return tuple(
        call(last_kernel, 1, 4, [f32s(*shares_init.shape), f32s(*freqs_init.shape)], [], False)(
            idx, far_got, own_sum, own_q, own_f
        )
    )


def solution(mesh):
    fine = Mesh(mesh.devices.reshape(SIZES), AXES)
    return jax.shard_map(
        body,
        mesh=fine,
        in_specs=(P(SMP, VAR), P(None, SMP + VAR), P(None, VAR + SMP)),
        out_specs=(P(None, SMP + VAR), P(None, VAR + SMP)),
        check_vma=False,
    )
```

```python
import jax
import jax.numpy as jnp
from jax import lax
from jax.experimental import pallas as pl
from jax.experimental.pallas import tpu as pltpu
from jax.sharding import Mesh, PartitionSpec as P

K = 12
PAD = 16
LANES = 128
ROWS = 256

AXES = ("y", "zq", "zp", "x", "zh", "c")
SIZES = (4, 4, 2, 4, 2, 2)
SMP = ("y", "zq", "zp")
VAR = ("x", "zh", "c")
NEAR = ("y", "x", "c")
FAR = ("zq", "zp", "zh")
WIDE = ("y", "zp", "x", "c")
LINE = ("zq", "zh")
N_NEAR, N_FAR, N_WIDE, N_LINE = 32, 16, 64, 8
N_Y, N_XC, N_ZL, N_ZH, N_ZQ, N_ROW = 4, 8, 8, 2, 4, 8
FAR_1 = LINE_1 = FAR_2 = 1
NEAR_1 = NEAR_2 = 20
WIDE_1 = WIDE_2 = 36

f32 = jnp.float32
bf16 = jnp.bfloat16


def tile(i):
    return slice(i * LANES, (i + 1) * LANES)


def var_of(idx):
    return idx[0] & 15


def smp_of(idx):
    return idx[0] >> 4


def zl_of(idx):
    return (idx[0] >> 4) & 7


def zh_of(idx):
    return (idx[0] >> 1) & 1


def lane():
    return lax.broadcasted_iota(jnp.int32, (8, LANES), 1)


def roll(x, shift):
    shift = shift % LANES
    return pltpu.roll(x, shift, 1) if shift else x


def two_parts(x):
    high = x.astype(bf16)
    return high, (x - high.astype(f32)).astype(bf16)


def three_parts(x):
    high = x.astype(bf16)
    return (high, *two_parts(x - high.astype(f32)))


def dot(a, b, over_a, over_b):
    return lax.dot_general(
        a, b, (((over_a,), (over_b,)), ((), ())), preferred_element_type=f32
    )


def fold(x):
    return x[:PAD] + x[PAD:]


def block_sums(dosage_ref, shares, freqs):
    qh, qm, ql = three_parts(shares)
    fh, fm, fl = three_parts(freqs)
    q_side = jnp.concatenate([qh, qh, qm, qh, ql, qm], 0)
    f_side = jnp.concatenate([fh, fm, fh, fl, fh, fm], 0)
    q_two = jnp.concatenate([qh, qm], 0)
    f_two = jnp.concatenate([fh, fm], 0)
    g_two = jnp.concatenate(two_parts(1.0 - freqs), 0)
    shift = 2 * lax.broadcasted_iota(jnp.int32, (16, freqs.shape[1]), 0)

    def ratios(at):
        probs = dot(q_side[:, at : at + ROWS], f_side, 0, 0)
        codes = jnp.concatenate(
            [
                jnp.bitwise_and(
                    jnp.right_shift(jnp.broadcast_to(dosage_ref[w : w + 1, :], shift.shape), shift), 3
                )
                for w in range(at // 16, (at + ROWS) // 16)
            ],
            0,
        )
        live = codes < 3
        allele = codes.astype(f32)
        ratio_alt = jnp.where(live, allele, 0.0) * (1.0 / probs)
        ratio_ref = jnp.where(live, 2.0 - allele, 0.0) * (1.0 / (1.0 - probs))
        return two_parts(ratio_alt) + two_parts(ratio_ref)

    sums_q, sum_a, sum_b = [], 0.0, 0.0
    starts = range(0, shares.shape[1], ROWS)
    ready = ratios(0)
    for at in starts:
        ah, al, bh, bl = ready
        if at + ROWS in starts:
            ready = ratios(at + ROWS)
        sums_q.append(
            dot(f_two, ah, 1, 1) + dot(f_two, al, 1, 1) + dot(g_two, bh, 1, 1) + dot(g_two, bl, 1, 1)
        )
        q_part = q_two[:, at : at + ROWS]
        sum_a = sum_a + (dot(q_part, ah, 1, 0) + dot(q_part, al, 1, 0))
        sum_b = sum_b + (dot(q_part, bh, 1, 0) + dot(q_part, bl, 1, 0))
    return fold(jnp.concatenate(sums_q, 1)), fold(sum_a), fold(sum_b)


def in_plane(y, g):
    return y * N_XC + g


def in_line(i, h):
    return i * N_ZH + h


def zq_of(idx):
    return (idx[0] >> 5) & 3


def near_of(idx):
    return ((idx[0] >> 1) & 6) | (idx[0] & 1)


def y_of(idx):
    return idx[0] >> 7


def halves(a, b):
    left = lax.broadcasted_iota(jnp.int32, a.shape, 1) < 64
    return jnp.where(left, a, roll(b, 64)), jnp.where(left, roll(a, 64), b)


def block_of_lane():
    return lax.broadcasted_iota(jnp.int32, (4, LANES), 1) // 16


def put_far(far_out, at, rows):
    for b in range(3):
        far_out[3 * at + b] = rows[2 * b : 2 * b + 2]


def get_far(far_in, at, pairs):
    return jnp.concatenate([far_in[3 * at + b] for b in range(pairs)], 0)


def first_kernel(idx, shares_ref, freqs_ref, far_out, q_out, f_tmp):
    raw = shares_ref[...]
    own = raw / jnp.sum(raw, axis=0, keepdims=True)
    q_out[...] = jnp.zeros_like(q_out)
    f_tmp[...] = jnp.zeros_like(f_tmp)
    q_out[0:6, 0:64] = own[0:6]
    q_out[0:6, 64:128] = own[6:12]
    for j in range(3):
        f_tmp[0:4, 16 * j : 16 * j + 16] = freqs_ref[4 * j : 4 * j + 4, :]
    turned = pltpu.roll(f_tmp[...], 16 * zl_of(idx), 1)
    for h in range(N_ZH):
        sent = jnp.where(zh_of(idx) == h, turned, q_out[...])
        for i in range(N_ZL):
            put_far(far_out, in_line(i, h) ^ FAR_1, sent)


def first_near_kernel(idx, far_in, q_in, near_out, f_out, q_tmp):
    zh = zh_of(idx)
    block = block_of_lane()
    freqs = [get_far(far_in, in_line(i, zh) ^ FAR_1, 2) for i in range(N_ZL)]
    for j in range(3):
        got = freqs[0]
        for i in range(1, N_ZL):
            got = jnp.where(block == (i + j) % 8, freqs[i], got)
        f_out[j] = roll(got, -16 * j)
    own, other = q_in[0:6], get_far(far_in, in_line(zl_of(idx), 1 - zh) ^ FAR_1, 3)
    q_tmp[0:6], q_tmp[6:12] = halves(jnp.where(zh == 0, own, other), jnp.where(zh == 0, other, own))
    for s in range(N_NEAR):
        near_out[3 * s : 3 * s + 3] = f_out[...]
    for g in range(N_XC):
        s = 3 * (in_plane(y_of(idx), g) ^ NEAR_1)
        for j in range(3):
            near_out[s + j] = q_tmp[4 * j : 4 * j + 4]


def shares_of(idx, near_in):
    rows = [[], [], []]
    for x in range(4):
        for j in range(3):
            a, b = (near_in[3 * (in_plane(y_of(idx), 2 * x + c) ^ NEAR_1) + j] for c in range(2))
            rows[j].extend(halves(a, b))
    return padded(rows)


def freqs_of(idx, near_in, f_in):
    rows = [[], [], []]
    for y in range(N_Y):
        for j in range(3):
            got = near_in[3 * (in_plane(y, near_of(idx)) ^ NEAR_1) + j]
            rows[j].append(jnp.where(y_of(idx) == y, f_in[j], got))
    return padded(rows)


def padded(rows):
    rows = [jnp.concatenate(row, 1) for row in rows]
    return jnp.concatenate([*rows, jnp.zeros_like(rows[0])], 0)


def turned_tiles(x):
    return jnp.concatenate([roll(x[:, tile(t)], 64) for t in range(x.shape[1] // LANES)], 1)


def left_of(rows):
    return lax.broadcasted_iota(jnp.int32, (rows, LANES), 1) < 64


def one_kernel(idx, dosage_ref, near_in, own_f_in, slots, q_out, f_out, sq_tmp, sa_tmp, sq_turn, sa_turn):
    shares = shares_of(idx, near_in)
    freqs = freqs_of(idx, near_in, own_f_in)
    q_out[...] = shares
    f_out[...] = freqs
    sum_q, sum_a, sum_b = block_sums(dosage_ref, shares, freqs)
    sq_tmp[...] = sum_q
    sa_tmp[0:12] = sum_a[0:12]
    sa_tmp[12:24] = sum_b[0:12]
    sq_turn[...] = turned_tiles(sum_q)
    sa_turn[...] = turned_tiles(sa_tmp[...])
    left = left_of(3)
    for w in range(N_WIDE):
        t, q = divmod(w, 4)
        a = (sq_turn if t % 2 else sq_tmp)[3 * q : 3 * q + 3, tile(t // 2)]
        t, q = divmod(w, 8)
        b = (sa_tmp if t % 2 else sa_turn)[3 * q : 3 * q + 3, tile(t // 2)]
        slots[w ^ WIDE_1, 0:3] = jnp.where(left, a, b)


def put_line(line_out, at, rows):
    for b in range(3):
        line_out[3 * at + b] = rows[4 * b : 4 * b + 4]


def wide_sums_kernel(idx, wide_in, line_out, q_out, a_tmp):
    left = left_of(4)
    row_sums = [sum(wide_in[in_plane(r, g) ^ WIDE_1] for g in range(N_XC)) for r in range(N_ROW)]
    col_sums = [sum(wide_in[in_plane(r, g) ^ WIDE_1] for r in range(N_ROW)) for g in range(N_XC)]
    for i in range(4):
        q_out[3 * i : 3 * i + 3] = jnp.where(left, row_sums[i], roll(row_sums[i + 4], 64))[0:3]
        a_tmp[3 * i : 3 * i + 3] = jnp.where(left, roll(col_sums[i], 64), col_sums[i + 4])[0:3]
    for h in range(N_ZH):
        sent = jnp.where(zh_of(idx) == h, a_tmp[...], q_out[...])
        for i in range(N_ZQ):
            put_line(line_out, in_line(i, h) ^ LINE_1, sent)


def line_sums_kernel(idx, line_in, q_in, wide_out, q_tmp, a_tmp):
    zh = zh_of(idx)
    for b in range(3):
        a_tmp[4 * b : 4 * b + 4] = sum(line_in[3 * (in_line(i, zh) ^ LINE_1) + b] for i in range(N_ZQ))
        other = line_in[3 * (in_line(zq_of(idx), 1 - zh) ^ LINE_1) + b]
        q_tmp[4 * b : 4 * b + 4] = q_in[4 * b : 4 * b + 4] + other
    left = left_of(3)
    row_sums, col_sums = [], []
    for i in range(8):
        at = 3 * (i % 4)
        row_sums.append(roll(q_tmp[at : at + 3], 64 * (i // 4)))
        col_sums.append(roll(a_tmp[at : at + 3], 64 * (1 - i // 4)))
    for r in range(N_ROW):
        for g in range(N_XC):
            wide_out[in_plane(r, g) ^ WIDE_2, 0:3] = jnp.where(left, row_sums[r], col_sums[g])


def two_kernel(idx, dosage_ref, wide_in, q_in, f_in, near_out, sq_out, own_q, own_f, sq_tmp, sa_tmp, q_tmp, f_tmp):
    left = left_of(4)
    for t in range(8):
        for q in range(4):
            a, b = (wide_in[(8 * t + 4 * half + q) ^ WIDE_2] for half in range(2))
            sq_tmp[3 * q : 3 * q + 3, tile(t)] = jnp.where(left, a, roll(b, 64))[0:3]
    for t in range(4):
        for q in range(8):
            a, b = (wide_in[(16 * t + 8 * half + q) ^ WIDE_2] for half in range(2))
            sa_tmp[3 * q : 3 * q + 3, tile(t)] = jnp.where(left, roll(a, 64), b)[0:3]
    q_tmp[...] = q_in[...]
    f_tmp[...] = f_in[...]
    numer = q_tmp[0:12] * sq_tmp[0:12]
    q_tmp[0:12] = (numer + 0.5) / (jnp.sum(numer, axis=0, keepdims=True) + 0.5 * K)
    old = f_tmp[0:12]
    alt_part = old * sa_tmp[0:12]
    f_tmp[0:12] = (alt_part + 0.5) / (alt_part + (1.0 - old) * sa_tmp[12:24] + 1.0)

    t = pl.multiple_of((var_of(idx) >> 1) * LANES, LANES)
    even, odd = halves(q_tmp[0:6, pl.ds(t, LANES)], q_tmp[6:12, pl.ds(t, LANES)])
    own_q[...] = jnp.where((var_of(idx) & 1) == 0, even, odd)
    t = pl.multiple_of((smp_of(idx) >> 3) * LANES, LANES)
    block = block_of_lane()
    got = f_tmp[0:4, pl.ds(t, LANES)]
    for j in range(1, 3):
        got = jnp.where(
            block == ((zl_of(idx) + j) & 7), roll(f_tmp[4 * j : 4 * j + 4, pl.ds(t, LANES)], 16 * j), got
        )
    own_f[...] = got

    sum_q, sum_a, sum_b = block_sums(dosage_ref, q_tmp[...], f_tmp[...])
    for x in range(4):
        pair = halves(sum_q[:, tile(2 * x)], sum_q[:, tile(2 * x + 1)])
        for c in range(2):
            for y in range(N_Y):
                near_out[in_plane(y, 2 * x + c) ^ NEAR_2, 0:16] = pair[c]
    sq_out[...] = near_out[in_plane(0, near_of(idx)) ^ NEAR_2, 0:16]
    sa_tmp[0:12] = sum_a[0:12]
    sa_tmp[12:24] = sum_b[0:12]
    for y in range(N_Y):
        near_out[in_plane(y, near_of(idx)) ^ NEAR_2] = sa_tmp[:, tile(y)]


def last_far_kernel(idx, near_in, sq_in, far_out, q_out):
    zh, near = zh_of(idx), near_of(idx)
    sum_q = sq_in[...]
    for g in range(N_XC):
        got = near_in[in_plane(y_of(idx), g) ^ NEAR_2, 0:16]
        sum_q = sum_q + jnp.where(near == g, 0.0, got)
    sums = sum(near_in[in_plane(y, near) ^ NEAR_2] for y in range(N_Y))
    parts = halves(sum_q[0:6], sum_q[6:12])
    q_out[...] = jnp.where(zh == 0, parts[0], parts[1])
    block = block_of_lane()
    turned = [roll(sums[4 * j : 4 * j + 4], 16 * j) for j in range(6)]
    for i in range(N_ZL):
        got = turned[0]
        for j in range(1, 6):
            got = jnp.where(block == (i + j) % 8, turned[j], got)
        got = jnp.concatenate([got, got[0:2]], 0)
        for h in range(N_ZH):
            put_far(far_out, in_line(i, h) ^ FAR_2, jnp.where(zh == h, got, parts[h]))


def last_kernel(idx, far_in, sq_in, own_q, own_f, shares_out, freqs_out):
    zh = zh_of(idx)
    sum_q = sq_in[...] + get_far(far_in, in_line(zl_of(idx), 1 - zh) ^ FAR_2, 3)
    numer = own_q[...] * sum_q
    total = jnp.sum(numer, axis=0, keepdims=True)
    total = total + pltpu.roll(total, 64, 1)
    new = (numer + 0.5) / (total + 0.5 * K)
    shares_out[0:6] = new[:, 0:64]
    shares_out[6:12] = new[:, 64:128]
    sums = sum(get_far(far_in, in_line(i, zh) ^ FAR_2, 2) for i in range(N_ZL))
    alt_part = own_f[...] * sums
    ref_part = (1.0 - own_f[...]) * roll(sums, -48)
    new = (alt_part + 0.5) / (alt_part + ref_part + 1.0)
    new = pltpu.roll(jnp.concatenate([new, new], 0), (LANES - 16 * zl_of(idx)) & (LANES - 1), 1)
    for j in range(3):
        freqs_out[4 * j : 4 * j + 4] = new[0:4, 16 * j : 16 * j + 16]


def f32s(*shape):
    return jax.ShapeDtypeStruct(shape, f32)


def vmem(*shape):
    return pltpu.VMEM(shape, f32)


def call(kernel, scalars, n_in, outs, scratch, kept=True):
    spec = pl.BlockSpec(memory_space=pltpu.VMEM)
    run = pl.pallas_call(
        kernel,
        in_specs=[pl.BlockSpec(memory_space=pltpu.SMEM)] * scalars + [spec] * n_in,
        out_specs=[spec] * len(outs),
        out_shape=[pltpu.VMEM(o.shape, o.dtype) for o in outs] if kept else outs,
        scratch_shapes=scratch,
    )

    def placed(*args):
        args = args[:scalars] + tuple(
            pltpu.with_memory_space_constraint(a, pltpu.VMEM) for a in args[scalars:]
        )
        return run(*args)

    return placed


def exchange(x, axes, first):
    members = 1
    for axis in axes:
        members *= SIZES[AXES.index(axis)]
    order = [[i ^ first for i in range(members)]]
    return lax.all_to_all(x, axes, 0, 0, tiled=True, axis_index_groups=order)


def body(dosage, shares_init, freqs_init):
    idx = lax.axis_index(AXES).astype(jnp.int32).reshape(1)
    samples, variants = 16 * dosage.shape[0], dosage.shape[1]
    pairs = f32s(3 * N_FAR, 2, LANES)
    far_slots, own_q = call(first_kernel, 1, 2, [pairs, f32s(8, LANES)], [vmem(8, LANES)])(
        idx, shares_init, freqs_init
    )
    far_got = exchange(far_slots, FAR, FAR_1)
    near_slots, own_f = call(
        first_near_kernel, 1, 2, [f32s(3 * N_NEAR, 4, LANES), f32s(3, 4, LANES)], [vmem(12, LANES)]
    )(idx, far_got, own_q)
    near_got = exchange(near_slots, NEAR, NEAR_1)
    slots, shares, freqs = call(
        one_kernel, 1, 3, [f32s(N_WIDE, 4, LANES), f32s(PAD, samples), f32s(PAD, variants)],
        [vmem(PAD, samples), vmem(24, variants), vmem(PAD, samples), vmem(24, variants)],
    )(idx, dosage, near_got, own_f)
    wide_got = exchange(slots, WIDE, WIDE_1)
    line_slots, own_sum = call(
        wide_sums_kernel, 1, 1, [f32s(3 * N_LINE, 4, LANES), f32s(12, LANES)], [vmem(12, LANES)]
    )(idx, wide_got)
    line_got = exchange(line_slots, LINE, LINE_1)
    (wide_slots,) = call(
        line_sums_kernel, 1, 2, [f32s(N_WIDE, 4, LANES)], [vmem(12, LANES), vmem(12, LANES)]
    )(idx, line_got, own_sum)
    wide_got = exchange(wide_slots, WIDE, WIDE_2)
    near_slots, own_sum, own_q, own_f = call(
        two_kernel, 1, 4,
        [f32s(N_NEAR, 24, LANES), f32s(PAD, LANES), f32s(6, LANES), f32s(4, LANES)],
        [vmem(PAD, samples), vmem(24, variants), vmem(PAD, samples), vmem(PAD, variants)],
    )(idx, dosage, wide_got, shares, freqs)
    near_got = exchange(near_slots, NEAR, NEAR_2)
    far_slots, own_sum = call(last_far_kernel, 1, 2, [pairs, f32s(6, LANES)], [])(
        idx, near_got, own_sum
    )
    far_got = exchange(far_slots, FAR, FAR_2)
    return tuple(
        call(last_kernel, 1, 4, [f32s(*shares_init.shape), f32s(*freqs_init.shape)], [], False)(
            idx, far_got, own_sum, own_q, own_f
        )
    )


def solution(mesh):
    fine = Mesh(mesh.devices.reshape(SIZES), AXES)
    return jax.shard_map(
        body,
        mesh=fine,
        in_specs=(P(SMP, VAR), P(None, SMP + VAR), P(None, VAR + SMP)),
        out_specs=(P(None, SMP + VAR), P(None, VAR + SMP)),
        check_vma=False,
    )
```

```python
import jax
import jax.numpy as jnp
from jax import lax
from jax.experimental import pallas as pl
from jax.experimental.pallas import tpu as pltpu
from jax.sharding import Mesh, PartitionSpec as P

K = 12
PAD = 16
LANES = 128
ROWS = 256

AXES = ("y", "zq", "zp", "x", "zh", "c")
SIZES = (4, 4, 2, 4, 2, 2)
SMP = ("y", "zq", "zp")
VAR = ("x", "zh", "c")
NEAR = ("y", "x", "c")
FAR = ("zq", "zp", "zh")
LINE = ("zq", "zh")
N_NEAR, N_FAR, N_WIDE, N_LINE = 32, 16, 64, 8
N_Y, N_XC, N_ZL, N_ZH, N_ZQ, N_ROW = 4, 8, 8, 2, 4, 8
FAR_FIRST = 1
NEAR_FIRST = 21
WIDE_FIRST = 37

f32 = jnp.float32
bf16 = jnp.bfloat16


def tile(i):
    return slice(i * LANES, (i + 1) * LANES)


def var_of(idx):
    return idx[0] & 15


def smp_of(idx):
    return idx[0] >> 4


def zl_of(idx):
    return (idx[0] >> 4) & 7


def zh_of(idx):
    return (idx[0] >> 1) & 1


def lane():
    return lax.broadcasted_iota(jnp.int32, (8, LANES), 1)


def roll(x, shift):
    shift = shift % LANES
    return pltpu.roll(x, shift, 1) if shift else x


def two_parts(x):
    high = x.astype(bf16)
    return high, (x - high.astype(f32)).astype(bf16)


def three_parts(x):
    high = x.astype(bf16)
    return (high, *two_parts(x - high.astype(f32)))


def dot(a, b, over_a, over_b):
    return lax.dot_general(
        a, b, (((over_a,), (over_b,)), ((), ())), preferred_element_type=f32
    )


def fold(x):
    return x[:PAD] + x[PAD:]


def block_sums(dosage_ref, shares, freqs):
    qh, qm, ql = three_parts(shares)
    fh, fm, fl = three_parts(freqs)
    q_side = jnp.concatenate([qh, qh, qm, qh, ql, qm], 0)
    f_side = jnp.concatenate([fh, fm, fh, fl, fh, fm], 0)
    q_two = jnp.concatenate([qh, qm], 0)
    f_two = jnp.concatenate([fh, fm], 0)
    g_two = jnp.concatenate(two_parts(1.0 - freqs), 0)
    shift = 2 * lax.broadcasted_iota(jnp.int32, (16, freqs.shape[1]), 0)

    def ratios(at):
        probs = dot(q_side[:, at : at + ROWS], f_side, 0, 0)
        codes = jnp.concatenate(
            [
                jnp.bitwise_and(
                    jnp.right_shift(jnp.broadcast_to(dosage_ref[w : w + 1, :], shift.shape), shift), 3
                )
                for w in range(at // 16, (at + ROWS) // 16)
            ],
            0,
        )
        live = codes < 3
        allele = codes.astype(f32)
        ratio_alt = jnp.where(live, allele, 0.0) * (1.0 / probs)
        ratio_ref = jnp.where(live, 2.0 - allele, 0.0) * (1.0 / (1.0 - probs))
        return two_parts(ratio_alt) + two_parts(ratio_ref)

    sums_q, sum_a, sum_b = [], 0.0, 0.0
    starts = range(0, shares.shape[1], ROWS)
    ready = ratios(0)
    for at in starts:
        ah, al, bh, bl = ready
        if at + ROWS in starts:
            ready = ratios(at + ROWS)
        sums_q.append(
            dot(f_two, ah, 1, 1) + dot(f_two, al, 1, 1) + dot(g_two, bh, 1, 1) + dot(g_two, bl, 1, 1)
        )
        q_part = q_two[:, at : at + ROWS]
        sum_a = sum_a + (dot(q_part, ah, 1, 0) + dot(q_part, al, 1, 0))
        sum_b = sum_b + (dot(q_part, bh, 1, 0) + dot(q_part, bl, 1, 0))
    return fold(jnp.concatenate(sums_q, 1)), fold(sum_a), fold(sum_b)


def in_plane(y, g):
    return y * N_XC + g


def in_line(i, h):
    return i * N_ZH + h


def in_wide(idx, member):
    return (member ^ WIDE_FIRST) ^ (8 - 8 * zh_of(idx))


def zq_of(idx):
    return (idx[0] >> 5) & 3


def near_of(idx):
    return ((idx[0] >> 1) & 6) | (idx[0] & 1)


def y_of(idx):
    return idx[0] >> 7


def halves(a, b):
    left = lax.broadcasted_iota(jnp.int32, a.shape, 1) < 64
    return jnp.where(left, a, roll(b, 64)), jnp.where(left, roll(a, 64), b)


def block_of_lane():
    return lax.broadcasted_iota(jnp.int32, (4, LANES), 1) // 16


def put_far(far_out, at, rows):
    for b in range(3):
        far_out[3 * at + b] = rows[2 * b : 2 * b + 2]


def get_far(far_in, at, pairs):
    return jnp.concatenate([far_in[3 * at + b] for b in range(pairs)], 0)


def first_kernel(idx, shares_ref, freqs_ref, far_out, q_out, f_tmp):
    raw = shares_ref[...]
    own = raw / jnp.sum(raw, axis=0, keepdims=True)
    q_out[...] = jnp.zeros_like(q_out)
    f_tmp[...] = jnp.zeros_like(f_tmp)
    q_out[0:6, 0:64] = own[0:6]
    q_out[0:6, 64:128] = own[6:12]
    for j in range(3):
        f_tmp[0:4, 16 * j : 16 * j + 16] = freqs_ref[4 * j : 4 * j + 4, :]
    turned = pltpu.roll(f_tmp[...], 16 * zl_of(idx), 1)
    for h in range(N_ZH):
        sent = jnp.where(zh_of(idx) == h, turned, q_out[...])
        for i in range(N_ZL):
            put_far(far_out, in_line(i, h) ^ FAR_FIRST, sent)


def first_near_kernel(idx, far_in, q_in, near_out, f_out, q_tmp):
    zh = zh_of(idx)
    block = block_of_lane()
    freqs = [get_far(far_in, in_line(i, zh) ^ FAR_FIRST, 2) for i in range(N_ZL)]
    for j in range(3):
        got = freqs[0]
        for i in range(1, N_ZL):
            got = jnp.where(block == (i + j) % 8, freqs[i], got)
        f_out[j] = roll(got, -16 * j)
    own, other = q_in[0:6], get_far(far_in, in_line(zl_of(idx), 1 - zh) ^ FAR_FIRST, 3)
    q_tmp[0:6], q_tmp[6:12] = halves(jnp.where(zh == 0, own, other), jnp.where(zh == 0, other, own))
    for s in range(N_NEAR):
        near_out[3 * s : 3 * s + 3] = f_out[...]
    for g in range(N_XC):
        s = 3 * (in_plane(y_of(idx), g) ^ NEAR_FIRST)
        for j in range(3):
            near_out[s + j] = q_tmp[4 * j : 4 * j + 4]


def shares_of(idx, near_in):
    rows = [[], [], []]
    for x in range(4):
        for j in range(3):
            a, b = (near_in[3 * (in_plane(y_of(idx), 2 * x + c) ^ NEAR_FIRST) + j] for c in range(2))
            rows[j].extend(halves(a, b))
    return padded(rows)


def freqs_of(idx, near_in, f_in):
    rows = [[], [], []]
    for y in range(N_Y):
        for j in range(3):
            got = near_in[3 * (in_plane(y, near_of(idx)) ^ NEAR_FIRST) + j]
            rows[j].append(jnp.where(y_of(idx) == y, f_in[j], got))
    return padded(rows)


def padded(rows):
    rows = [jnp.concatenate(row, 1) for row in rows]
    return jnp.concatenate([*rows, jnp.zeros_like(rows[0])], 0)


def turned_tiles(x):
    return jnp.concatenate([roll(x[:, tile(t)], 64) for t in range(x.shape[1] // LANES)], 1)


def left_of(rows):
    return lax.broadcasted_iota(jnp.int32, (rows, LANES), 1) < 64


def one_kernel(idx, dosage_ref, near_in, own_f_in, slots, q_out, f_out, sq_tmp, sa_tmp, sq_turn, sa_turn):
    shares = shares_of(idx, near_in)
    freqs = freqs_of(idx, near_in, own_f_in)
    q_out[...] = shares
    f_out[...] = freqs
    sum_q, sum_a, sum_b = block_sums(dosage_ref, shares, freqs)
    sq_tmp[...] = sum_q
    sa_tmp[0:12] = sum_a[0:12]
    sa_tmp[12:24] = sum_b[0:12]
    sq_turn[...] = turned_tiles(sum_q)
    sa_turn[...] = turned_tiles(sa_tmp[...])
    left = left_of(3)
    for w in range(N_WIDE):
        t, q = divmod(w, 4)
        a = (sq_turn if t % 2 else sq_tmp)[3 * q : 3 * q + 3, tile(t // 2)]
        t, q = divmod(w, 8)
        b = (sa_tmp if t % 2 else sa_turn)[3 * q : 3 * q + 3, tile(t // 2)]
        slots[in_wide(idx, w), 0:3] = jnp.where(left, a, b)


def put_line(line_out, at, rows):
    for b in range(3):
        line_out[3 * at + b] = rows[4 * b : 4 * b + 4]


def wide_sums_kernel(idx, wide_in, line_out, q_out, a_tmp):
    left = left_of(4)
    row_sums = [sum(wide_in[in_wide(idx, in_plane(r, g))] for g in range(N_XC)) for r in range(N_ROW)]
    col_sums = [sum(wide_in[in_wide(idx, in_plane(r, g))] for r in range(N_ROW)) for g in range(N_XC)]
    for i in range(4):
        q_out[3 * i : 3 * i + 3] = jnp.where(left, row_sums[i], roll(row_sums[i + 4], 64))[0:3]
        a_tmp[3 * i : 3 * i + 3] = jnp.where(left, roll(col_sums[i], 64), col_sums[i + 4])[0:3]
    for h in range(N_ZH):
        sent = jnp.where(zh_of(idx) == h, a_tmp[...], q_out[...])
        for i in range(N_ZQ):
            put_line(line_out, in_line(i, h) ^ FAR_FIRST, sent)


def line_sums_kernel(idx, line_in, q_in, wide_out, q_tmp, a_tmp):
    zh = zh_of(idx)
    for b in range(3):
        a_tmp[4 * b : 4 * b + 4] = sum(line_in[3 * (in_line(i, zh) ^ FAR_FIRST) + b] for i in range(N_ZQ))
        other = line_in[3 * (in_line(zq_of(idx), 1 - zh) ^ FAR_FIRST) + b]
        q_tmp[4 * b : 4 * b + 4] = q_in[4 * b : 4 * b + 4] + other
    left = left_of(3)
    row_sums, col_sums = [], []
    for i in range(8):
        at = 3 * (i % 4)
        row_sums.append(roll(q_tmp[at : at + 3], 64 * (i // 4)))
        col_sums.append(roll(a_tmp[at : at + 3], 64 * (1 - i // 4)))
    for r in range(N_ROW):
        for g in range(N_XC):
            wide_out[in_wide(idx, in_plane(r, g)), 0:3] = jnp.where(left, row_sums[r], col_sums[g])


def two_kernel(idx, dosage_ref, wide_in, q_in, f_in, near_out, sq_out, own_q, own_f, sq_tmp, sa_tmp, q_tmp, f_tmp):
    left = left_of(4)
    for t in range(8):
        for q in range(4):
            a, b = (wide_in[in_wide(idx, 8 * t + 4 * half + q)] for half in range(2))
            sq_tmp[3 * q : 3 * q + 3, tile(t)] = jnp.where(left, a, roll(b, 64))[0:3]
    for t in range(4):
        for q in range(8):
            a, b = (wide_in[in_wide(idx, 16 * t + 8 * half + q)] for half in range(2))
            sa_tmp[3 * q : 3 * q + 3, tile(t)] = jnp.where(left, roll(a, 64), b)[0:3]
    q_tmp[...] = q_in[...]
    f_tmp[...] = f_in[...]
    numer = q_tmp[0:12] * sq_tmp[0:12]
    q_tmp[0:12] = (numer + 0.5) / (jnp.sum(numer, axis=0, keepdims=True) + 0.5 * K)
    old = f_tmp[0:12]
    alt_part = old * sa_tmp[0:12]
    f_tmp[0:12] = (alt_part + 0.5) / (alt_part + (1.0 - old) * sa_tmp[12:24] + 1.0)

    t = pl.multiple_of((var_of(idx) >> 1) * LANES, LANES)
    even, odd = halves(q_tmp[0:6, pl.ds(t, LANES)], q_tmp[6:12, pl.ds(t, LANES)])
    own_q[...] = jnp.where((var_of(idx) & 1) == 0, even, odd)
    t = pl.multiple_of((smp_of(idx) >> 3) * LANES, LANES)
    block = block_of_lane()
    got = f_tmp[0:4, pl.ds(t, LANES)]
    for j in range(1, 3):
        got = jnp.where(
            block == ((zl_of(idx) + j) & 7), roll(f_tmp[4 * j : 4 * j + 4, pl.ds(t, LANES)], 16 * j), got
        )
    own_f[...] = got

    sum_q, sum_a, sum_b = block_sums(dosage_ref, q_tmp[...], f_tmp[...])
    for x in range(4):
        pair = halves(sum_q[:, tile(2 * x)], sum_q[:, tile(2 * x + 1)])
        for c in range(2):
            for y in range(N_Y):
                near_out[in_plane(y, 2 * x + c) ^ NEAR_FIRST, 0:16] = pair[c]
    sq_out[...] = near_out[in_plane(0, near_of(idx)) ^ NEAR_FIRST, 0:16]
    sa_tmp[0:12] = sum_a[0:12]
    sa_tmp[12:24] = sum_b[0:12]
    for y in range(N_Y):
        near_out[in_plane(y, near_of(idx)) ^ NEAR_FIRST] = sa_tmp[:, tile(y)]


def last_far_kernel(idx, near_in, sq_in, far_out, q_out):
    zh, near = zh_of(idx), near_of(idx)
    sum_q = sq_in[...]
    for g in range(N_XC):
        got = near_in[in_plane(y_of(idx), g) ^ NEAR_FIRST, 0:16]
        sum_q = sum_q + jnp.where(near == g, 0.0, got)
    sums = sum(near_in[in_plane(y, near) ^ NEAR_FIRST] for y in range(N_Y))
    parts = halves(sum_q[0:6], sum_q[6:12])
    q_out[...] = jnp.where(zh == 0, parts[0], parts[1])
    block = block_of_lane()
    turned = [roll(sums[4 * j : 4 * j + 4], 16 * j) for j in range(6)]
    for i in range(N_ZL):
        got = turned[0]
        for j in range(1, 6):
            got = jnp.where(block == (i + j) % 8, turned[j], got)
        got = jnp.concatenate([got, got[0:2]], 0)
        for h in range(N_ZH):
            put_far(far_out, in_line(i, h) ^ FAR_FIRST, jnp.where(zh == h, got, parts[h]))


def last_kernel(idx, far_in, sq_in, own_q, own_f, shares_out, freqs_out):
    zh = zh_of(idx)
    sum_q = sq_in[...] + get_far(far_in, in_line(zl_of(idx), 1 - zh) ^ FAR_FIRST, 3)
    numer = own_q[...] * sum_q
    total = jnp.sum(numer, axis=0, keepdims=True)
    total = total + pltpu.roll(total, 64, 1)
    new = (numer + 0.5) / (total + 0.5 * K)
    shares_out[0:6] = new[:, 0:64]
    shares_out[6:12] = new[:, 64:128]
    sums = sum(get_far(far_in, in_line(i, zh) ^ FAR_FIRST, 2) for i in range(N_ZL))
    alt_part = own_f[...] * sums
    ref_part = (1.0 - own_f[...]) * roll(sums, -48)
    new = (alt_part + 0.5) / (alt_part + ref_part + 1.0)
    new = pltpu.roll(jnp.concatenate([new, new], 0), (LANES - 16 * zl_of(idx)) & (LANES - 1), 1)
    for j in range(3):
        freqs_out[4 * j : 4 * j + 4] = new[0:4, 16 * j : 16 * j + 16]


def f32s(*shape):
    return jax.ShapeDtypeStruct(shape, f32)


def vmem(*shape):
    return pltpu.VMEM(shape, f32)


def call(kernel, scalars, n_in, outs, scratch, kept=True):
    spec = pl.BlockSpec(memory_space=pltpu.VMEM)
    run = pl.pallas_call(
        kernel,
        in_specs=[pl.BlockSpec(memory_space=pltpu.SMEM)] * scalars + [spec] * n_in,
        out_specs=[spec] * len(outs),
        out_shape=[pltpu.VMEM(o.shape, o.dtype) for o in outs] if kept else outs,
        scratch_shapes=scratch,
    )

    def placed(*args):
        args = args[:scalars] + tuple(
            pltpu.with_memory_space_constraint(a, pltpu.VMEM) for a in args[scalars:]
        )
        return run(*args)

    return placed


def exchange(x, axes, first):
    members = 1
    for axis in axes:
        members *= SIZES[AXES.index(axis)]
    order = [[i ^ first for i in range(members)]]
    return lax.all_to_all(x, axes, 0, 0, tiled=True, axis_index_groups=order)


def wide_exchange(x):
    groups = []
    for zq in range(N_ZQ):
        for zh in range(N_ZH):
            first = WIDE_FIRST ^ (8 - 8 * zh)
            members = [i ^ first for i in range(N_WIDE)]
            groups.append(
                [
                    (m >> 4) << 7 | zq << 5 | (m >> 3 & 1) << 4 | (m >> 1 & 3) << 2 | zh << 1 | (m & 1)
                    for m in members
                ]
            )
    return lax.all_to_all(x, AXES, 0, 0, tiled=True, axis_index_groups=groups)


def body(dosage, shares_init, freqs_init):
    idx = lax.axis_index(AXES).astype(jnp.int32).reshape(1)
    samples, variants = 16 * dosage.shape[0], dosage.shape[1]
    pairs = f32s(3 * N_FAR, 2, LANES)
    far_slots, own_q = call(first_kernel, 1, 2, [pairs, f32s(8, LANES)], [vmem(8, LANES)])(
        idx, shares_init, freqs_init
    )
    far_got = exchange(far_slots, FAR, FAR_FIRST)
    near_slots, own_f = call(
        first_near_kernel, 1, 2, [f32s(3 * N_NEAR, 4, LANES), f32s(3, 4, LANES)], [vmem(12, LANES)]
    )(idx, far_got, own_q)
    near_got = exchange(near_slots, NEAR, NEAR_FIRST)
    slots, shares, freqs = call(
        one_kernel, 1, 3, [f32s(N_WIDE, 4, LANES), f32s(PAD, samples), f32s(PAD, variants)],
        [vmem(PAD, samples), vmem(24, variants), vmem(PAD, samples), vmem(24, variants)],
    )(idx, dosage, near_got, own_f)
    wide_got = wide_exchange(slots)
    line_slots, own_sum = call(
        wide_sums_kernel, 1, 1, [f32s(3 * N_LINE, 4, LANES), f32s(12, LANES)], [vmem(12, LANES)]
    )(idx, wide_got)
    line_got = exchange(line_slots, LINE, FAR_FIRST)
    (wide_slots,) = call(
        line_sums_kernel, 1, 2, [f32s(N_WIDE, 4, LANES)], [vmem(12, LANES), vmem(12, LANES)]
    )(idx, line_got, own_sum)
    wide_got = wide_exchange(wide_slots)
    near_slots, own_sum, own_q, own_f = call(
        two_kernel, 1, 4,
        [f32s(N_NEAR, 24, LANES), f32s(PAD, LANES), f32s(6, LANES), f32s(4, LANES)],
        [vmem(PAD, samples), vmem(24, variants), vmem(PAD, samples), vmem(PAD, variants)],
    )(idx, dosage, wide_got, shares, freqs)
    near_got = exchange(near_slots, NEAR, NEAR_FIRST)
    far_slots, own_sum = call(last_far_kernel, 1, 2, [pairs, f32s(6, LANES)], [])(
        idx, near_got, own_sum
    )
    far_got = exchange(far_slots, FAR, FAR_FIRST)
    return tuple(
        call(last_kernel, 1, 4, [f32s(*shares_init.shape), f32s(*freqs_init.shape)], [], False)(
            idx, far_got, own_sum, own_q, own_f
        )
    )


def solution(mesh):
    fine = Mesh(mesh.devices.reshape(SIZES), AXES)
    return jax.shard_map(
        body,
        mesh=fine,
        in_specs=(P(SMP, VAR), P(None, SMP + VAR), P(None, VAR + SMP)),
        out_specs=(P(None, SMP + VAR), P(None, VAR + SMP)),
        check_vma=False,
    )
```

```python
import jax
import jax.numpy as jnp
from jax import lax
from jax.experimental import pallas as pl
from jax.experimental.pallas import tpu as pltpu
from jax.sharding import Mesh, PartitionSpec as P

K = 12
PAD = 16
LANES = 128
ROWS = 256

AXES = ("y", "zq", "zp", "x", "zh", "c")
SIZES = (4, 4, 2, 4, 2, 2)
SMP = ("y", "zq", "zp")
VAR = ("x", "zh", "c")
NEAR = ("y", "x", "c")
FAR = ("zq", "zp", "zh")
LINE = ("zq", "zh")
N_NEAR, N_FAR, N_WIDE, N_LINE = 32, 16, 64, 8
N_Y, N_XC, N_ZL, N_ZH, N_ZQ, N_ROW = 4, 8, 8, 2, 4, 8
FAR_FIRST = 1
NEAR_FIRST = 21
WIDE_FIRST = 37

f32 = jnp.float32
bf16 = jnp.bfloat16


def tile(i):
    return slice(i * LANES, (i + 1) * LANES)


def var_of(idx):
    return idx[0] & 15


def smp_of(idx):
    return idx[0] >> 4


def zl_of(idx):
    return (idx[0] >> 4) & 7


def zh_of(idx):
    return (idx[0] >> 1) & 1


def lane():
    return lax.broadcasted_iota(jnp.int32, (8, LANES), 1)


def roll(x, shift):
    shift = shift % LANES
    return pltpu.roll(x, shift, 1) if shift else x


def two_parts(x):
    high = x.astype(bf16)
    return high, (x - high.astype(f32)).astype(bf16)


def three_parts(x):
    high = x.astype(bf16)
    return (high, *two_parts(x - high.astype(f32)))


def dot(a, b, over_a, over_b):
    return lax.dot_general(
        a, b, (((over_a,), (over_b,)), ((), ())), preferred_element_type=f32
    )


def fold(x):
    return x[:PAD] + x[PAD:]


def block_sums(dosage_ref, shares, freqs):
    qh, qm, ql = three_parts(shares)
    fh, fm, fl = three_parts(freqs)
    q_side = jnp.concatenate([qh, qh, qm, qh, ql, qm], 0)
    f_side = jnp.concatenate([fh, fm, fh, fl, fh, fm], 0)
    q_two = jnp.concatenate([qh, qm], 0)
    f_two = jnp.concatenate([fh, fm], 0)
    g_two = jnp.concatenate(two_parts(1.0 - freqs), 0)
    shift = 2 * lax.broadcasted_iota(jnp.int32, (16, freqs.shape[1]), 0)

    def ratios(at):
        probs = dot(q_side[:, at : at + ROWS], f_side, 0, 0)
        codes = jnp.concatenate(
            [
                jnp.bitwise_and(
                    jnp.right_shift(jnp.broadcast_to(dosage_ref[w : w + 1, :], shift.shape), shift), 3
                )
                for w in range(at // 16, (at + ROWS) // 16)
            ],
            0,
        )
        live = codes < 3
        allele = codes.astype(f32)
        ratio_alt = jnp.where(live, allele, 0.0) * (1.0 / probs)
        ratio_ref = jnp.where(live, 2.0 - allele, 0.0) * (1.0 / (1.0 - probs))
        return two_parts(ratio_alt) + two_parts(ratio_ref)

    sums_q, sum_a, sum_b = [], 0.0, 0.0
    starts = range(0, shares.shape[1], ROWS)
    ready = ratios(0)
    for at in starts:
        ah, al, bh, bl = ready
        if at + ROWS in starts:
            ready = ratios(at + ROWS)
        sums_q.append(
            dot(f_two, ah, 1, 1) + dot(f_two, al, 1, 1) + dot(g_two, bh, 1, 1) + dot(g_two, bl, 1, 1)
        )
        q_part = q_two[:, at : at + ROWS]
        sum_a = sum_a + (dot(q_part, ah, 1, 0) + dot(q_part, al, 1, 0))
        sum_b = sum_b + (dot(q_part, bh, 1, 0) + dot(q_part, bl, 1, 0))
    return fold(jnp.concatenate(sums_q, 1)), fold(sum_a), fold(sum_b)


def in_plane(y, g):
    return y * N_XC + g


def in_line(i, h):
    return i * N_ZH + h


def near_slot(y, g):
    m = in_plane(y, g) ^ NEAR_FIRST
    return m & 1 | (m >> 4 & 1) << 1 | (m >> 2 & 1) << 2 | (m >> 3 & 1) << 3 | (m >> 1 & 1) << 4


def in_wide(idx, member):
    return (member ^ WIDE_FIRST) ^ (8 - 8 * zh_of(idx))


def zq_of(idx):
    return (idx[0] >> 5) & 3


def near_of(idx):
    return ((idx[0] >> 1) & 6) | (idx[0] & 1)


def y_of(idx):
    return idx[0] >> 7


def halves(a, b):
    left = lax.broadcasted_iota(jnp.int32, a.shape, 1) < 64
    return jnp.where(left, a, roll(b, 64)), jnp.where(left, roll(a, 64), b)


def block_of_lane():
    return lax.broadcasted_iota(jnp.int32, (4, LANES), 1) // 16


def put_far(far_out, at, rows):
    for b in range(3):
        far_out[3 * at + b] = rows[2 * b : 2 * b + 2]


def get_far(far_in, at, pairs):
    return jnp.concatenate([far_in[3 * at + b] for b in range(pairs)], 0)


def first_kernel(idx, shares_ref, freqs_ref, far_out, q_out, f_tmp):
    raw = shares_ref[...]
    own = raw / jnp.sum(raw, axis=0, keepdims=True)
    q_out[...] = jnp.zeros_like(q_out)
    f_tmp[...] = jnp.zeros_like(f_tmp)
    q_out[0:6, 0:64] = own[0:6]
    q_out[0:6, 64:128] = own[6:12]
    for j in range(3):
        f_tmp[0:4, 16 * j : 16 * j + 16] = freqs_ref[4 * j : 4 * j + 4, :]
    turned = pltpu.roll(f_tmp[...], 16 * zl_of(idx), 1)
    for h in range(N_ZH):
        sent = jnp.where(zh_of(idx) == h, turned, q_out[...])
        for i in range(N_ZL):
            put_far(far_out, in_line(i, h) ^ FAR_FIRST, sent)


def first_near_kernel(idx, far_in, q_in, near_out, f_out, q_tmp):
    zh = zh_of(idx)
    block = block_of_lane()
    freqs = [get_far(far_in, in_line(i, zh) ^ FAR_FIRST, 2) for i in range(N_ZL)]
    for j in range(3):
        got = freqs[0]
        for i in range(1, N_ZL):
            got = jnp.where(block == (i + j) % 8, freqs[i], got)
        f_out[j] = roll(got, -16 * j)
    own, other = q_in[0:6], get_far(far_in, in_line(zl_of(idx), 1 - zh) ^ FAR_FIRST, 3)
    q_tmp[0:6], q_tmp[6:12] = halves(jnp.where(zh == 0, own, other), jnp.where(zh == 0, other, own))
    for s in range(N_NEAR):
        near_out[3 * s : 3 * s + 3] = f_out[...]
    for g in range(N_XC):
        s = 3 * near_slot(y_of(idx), g)
        for j in range(3):
            near_out[s + j] = q_tmp[4 * j : 4 * j + 4]


def shares_of(idx, near_in):
    rows = [[], [], []]
    for x in range(4):
        for j in range(3):
            a, b = (near_in[3 * near_slot(y_of(idx), 2 * x + c) + j] for c in range(2))
            rows[j].extend(halves(a, b))
    return padded(rows)


def freqs_of(idx, near_in, f_in):
    rows = [[], [], []]
    for y in range(N_Y):
        for j in range(3):
            got = near_in[3 * near_slot(y, near_of(idx)) + j]
            rows[j].append(jnp.where(y_of(idx) == y, f_in[j], got))
    return padded(rows)


def padded(rows):
    rows = [jnp.concatenate(row, 1) for row in rows]
    return jnp.concatenate([*rows, jnp.zeros_like(rows[0])], 0)


def turned_tiles(x):
    return jnp.concatenate([roll(x[:, tile(t)], 64) for t in range(x.shape[1] // LANES)], 1)


def left_of(rows):
    return lax.broadcasted_iota(jnp.int32, (rows, LANES), 1) < 64


def one_kernel(idx, dosage_ref, near_in, own_f_in, slots, q_out, f_out, sq_tmp, sa_tmp, sq_turn, sa_turn):
    shares = shares_of(idx, near_in)
    freqs = freqs_of(idx, near_in, own_f_in)
    q_out[...] = shares
    f_out[...] = freqs
    sum_q, sum_a, sum_b = block_sums(dosage_ref, shares, freqs)
    sq_tmp[...] = sum_q
    sa_tmp[0:12] = sum_a[0:12]
    sa_tmp[12:24] = sum_b[0:12]
    sq_turn[...] = turned_tiles(sum_q)
    sa_turn[...] = turned_tiles(sa_tmp[...])
    left = left_of(3)
    for w in range(N_WIDE):
        t, q = divmod(w, 4)
        a = (sq_turn if t % 2 else sq_tmp)[3 * q : 3 * q + 3, tile(t // 2)]
        t, q = divmod(w, 8)
        b = (sa_tmp if t % 2 else sa_turn)[3 * q : 3 * q + 3, tile(t // 2)]
        slots[in_wide(idx, w), 0:3] = jnp.where(left, a, b)


def put_line(line_out, at, rows):
    for b in range(3):
        line_out[3 * at + b] = rows[4 * b : 4 * b + 4]


def wide_sums_kernel(idx, wide_in, line_out, q_out, a_tmp):
    left = left_of(4)
    row_sums = [sum(wide_in[in_wide(idx, in_plane(r, g))] for g in range(N_XC)) for r in range(N_ROW)]
    col_sums = [sum(wide_in[in_wide(idx, in_plane(r, g))] for r in range(N_ROW)) for g in range(N_XC)]
    for i in range(4):
        q_out[3 * i : 3 * i + 3] = jnp.where(left, row_sums[i], roll(row_sums[i + 4], 64))[0:3]
        a_tmp[3 * i : 3 * i + 3] = jnp.where(left, roll(col_sums[i], 64), col_sums[i + 4])[0:3]
    for h in range(N_ZH):
        sent = jnp.where(zh_of(idx) == h, a_tmp[...], q_out[...])
        for i in range(N_ZQ):
            put_line(line_out, in_line(i, h) ^ FAR_FIRST, sent)


def line_sums_kernel(idx, line_in, q_in, wide_out, q_tmp, a_tmp):
    zh = zh_of(idx)
    for b in range(3):
        a_tmp[4 * b : 4 * b + 4] = sum(line_in[3 * (in_line(i, zh) ^ FAR_FIRST) + b] for i in range(N_ZQ))
        other = line_in[3 * (in_line(zq_of(idx), 1 - zh) ^ FAR_FIRST) + b]
        q_tmp[4 * b : 4 * b + 4] = q_in[4 * b : 4 * b + 4] + other
    left = left_of(3)
    row_sums, col_sums = [], []
    for i in range(8):
        at = 3 * (i % 4)
        row_sums.append(roll(q_tmp[at : at + 3], 64 * (i // 4)))
        col_sums.append(roll(a_tmp[at : at + 3], 64 * (1 - i // 4)))
    for r in range(N_ROW):
        for g in range(N_XC):
            wide_out[in_wide(idx, in_plane(r, g)), 0:3] = jnp.where(left, row_sums[r], col_sums[g])


def two_kernel(idx, dosage_ref, wide_in, q_in, f_in, near_out, sq_out, own_q, own_f, sq_tmp, sa_tmp, q_tmp, f_tmp):
    left = left_of(4)
    for t in range(8):
        for q in range(4):
            a, b = (wide_in[in_wide(idx, 8 * t + 4 * half + q)] for half in range(2))
            sq_tmp[3 * q : 3 * q + 3, tile(t)] = jnp.where(left, a, roll(b, 64))[0:3]
    for t in range(4):
        for q in range(8):
            a, b = (wide_in[in_wide(idx, 16 * t + 8 * half + q)] for half in range(2))
            sa_tmp[3 * q : 3 * q + 3, tile(t)] = jnp.where(left, roll(a, 64), b)[0:3]
    q_tmp[...] = q_in[...]
    f_tmp[...] = f_in[...]
    numer = q_tmp[0:12] * sq_tmp[0:12]
    q_tmp[0:12] = (numer + 0.5) / (jnp.sum(numer, axis=0, keepdims=True) + 0.5 * K)
    old = f_tmp[0:12]
    alt_part = old * sa_tmp[0:12]
    f_tmp[0:12] = (alt_part + 0.5) / (alt_part + (1.0 - old) * sa_tmp[12:24] + 1.0)

    t = pl.multiple_of((var_of(idx) >> 1) * LANES, LANES)
    even, odd = halves(q_tmp[0:6, pl.ds(t, LANES)], q_tmp[6:12, pl.ds(t, LANES)])
    own_q[...] = jnp.where((var_of(idx) & 1) == 0, even, odd)
    t = pl.multiple_of((smp_of(idx) >> 3) * LANES, LANES)
    block = block_of_lane()
    got = f_tmp[0:4, pl.ds(t, LANES)]
    for j in range(1, 3):
        got = jnp.where(
            block == ((zl_of(idx) + j) & 7), roll(f_tmp[4 * j : 4 * j + 4, pl.ds(t, LANES)], 16 * j), got
        )
    own_f[...] = got

    sum_q, sum_a, sum_b = block_sums(dosage_ref, q_tmp[...], f_tmp[...])
    for x in range(4):
        pair = halves(sum_q[:, tile(2 * x)], sum_q[:, tile(2 * x + 1)])
        for c in range(2):
            for y in range(N_Y):
                near_out[near_slot(y, 2 * x + c), 0:16] = pair[c]
    sq_out[...] = near_out[near_slot(0, near_of(idx)), 0:16]
    sa_tmp[0:12] = sum_a[0:12]
    sa_tmp[12:24] = sum_b[0:12]
    for y in range(N_Y):
        near_out[near_slot(y, near_of(idx))] = sa_tmp[:, tile(y)]


def last_far_kernel(idx, near_in, sq_in, far_out, q_out):
    zh, near = zh_of(idx), near_of(idx)
    sum_q = sq_in[...]
    for g in range(N_XC):
        got = near_in[near_slot(y_of(idx), g), 0:16]
        sum_q = sum_q + jnp.where(near == g, 0.0, got)
    sums = sum(near_in[near_slot(y, near)] for y in range(N_Y))
    parts = halves(sum_q[0:6], sum_q[6:12])
    q_out[...] = jnp.where(zh == 0, parts[0], parts[1])
    block = block_of_lane()
    turned = [roll(sums[4 * j : 4 * j + 4], 16 * j) for j in range(6)]
    for i in range(N_ZL):
        got = turned[0]
        for j in range(1, 6):
            got = jnp.where(block == (i + j) % 8, turned[j], got)
        got = jnp.concatenate([got, got[0:2]], 0)
        for h in range(N_ZH):
            put_far(far_out, in_line(i, h) ^ FAR_FIRST, jnp.where(zh == h, got, parts[h]))


def last_kernel(idx, far_in, sq_in, own_q, own_f, shares_out, freqs_out):
    zh = zh_of(idx)
    sum_q = sq_in[...] + get_far(far_in, in_line(zl_of(idx), 1 - zh) ^ FAR_FIRST, 3)
    numer = own_q[...] * sum_q
    total = jnp.sum(numer, axis=0, keepdims=True)
    total = total + pltpu.roll(total, 64, 1)
    new = (numer + 0.5) / (total + 0.5 * K)
    shares_out[0:6] = new[:, 0:64]
    shares_out[6:12] = new[:, 64:128]
    sums = sum(get_far(far_in, in_line(i, zh) ^ FAR_FIRST, 2) for i in range(N_ZL))
    alt_part = own_f[...] * sums
    ref_part = (1.0 - own_f[...]) * roll(sums, -48)
    new = (alt_part + 0.5) / (alt_part + ref_part + 1.0)
    new = pltpu.roll(jnp.concatenate([new, new], 0), (LANES - 16 * zl_of(idx)) & (LANES - 1), 1)
    for j in range(3):
        freqs_out[4 * j : 4 * j + 4] = new[0:4, 16 * j : 16 * j + 16]


def f32s(*shape):
    return jax.ShapeDtypeStruct(shape, f32)


def vmem(*shape):
    return pltpu.VMEM(shape, f32)


def call(kernel, scalars, n_in, outs, scratch, kept=True):
    spec = pl.BlockSpec(memory_space=pltpu.VMEM)
    run = pl.pallas_call(
        kernel,
        in_specs=[pl.BlockSpec(memory_space=pltpu.SMEM)] * scalars + [spec] * n_in,
        out_specs=[spec] * len(outs),
        out_shape=[pltpu.VMEM(o.shape, o.dtype) for o in outs] if kept else outs,
        scratch_shapes=scratch,
    )

    def placed(*args):
        args = args[:scalars] + tuple(
            pltpu.with_memory_space_constraint(a, pltpu.VMEM) for a in args[scalars:]
        )
        return run(*args)

    return placed


def exchange(x, axes, order):
    return lax.all_to_all(x, axes, 0, 0, tiled=True, axis_index_groups=[order])


def near_exchange(x):
    slots = [near_slot(m // N_XC, m % N_XC) for m in range(N_NEAR)]
    return exchange(x, NEAR, [slots.index(i) for i in range(N_NEAR)])


def line_exchange(x, axes, members):
    return exchange(x, axes, [i ^ FAR_FIRST for i in range(members)])


def wide_exchange(x):
    groups = []
    for zq in range(N_ZQ):
        for zh in range(N_ZH):
            first = WIDE_FIRST ^ (8 - 8 * zh)
            members = [i ^ first for i in range(N_WIDE)]
            groups.append(
                [
                    (m >> 4) << 7 | zq << 5 | (m >> 3 & 1) << 4 | (m >> 1 & 3) << 2 | zh << 1 | (m & 1)
                    for m in members
                ]
            )
    return lax.all_to_all(x, AXES, 0, 0, tiled=True, axis_index_groups=groups)


def body(dosage, shares_init, freqs_init):
    idx = lax.axis_index(AXES).astype(jnp.int32).reshape(1)
    samples, variants = 16 * dosage.shape[0], dosage.shape[1]
    pairs = f32s(3 * N_FAR, 2, LANES)
    far_slots, own_q = call(first_kernel, 1, 2, [pairs, f32s(8, LANES)], [vmem(8, LANES)])(
        idx, shares_init, freqs_init
    )
    far_got = line_exchange(far_slots, FAR, N_FAR)
    near_slots, own_f = call(
        first_near_kernel, 1, 2, [f32s(3 * N_NEAR, 4, LANES), f32s(3, 4, LANES)], [vmem(12, LANES)]
    )(idx, far_got, own_q)
    near_got = near_exchange(near_slots)
    slots, shares, freqs = call(
        one_kernel, 1, 3, [f32s(N_WIDE, 4, LANES), f32s(PAD, samples), f32s(PAD, variants)],
        [vmem(PAD, samples), vmem(24, variants), vmem(PAD, samples), vmem(24, variants)],
    )(idx, dosage, near_got, own_f)
    wide_got = wide_exchange(slots)
    line_slots, own_sum = call(
        wide_sums_kernel, 1, 1, [f32s(3 * N_LINE, 4, LANES), f32s(12, LANES)], [vmem(12, LANES)]
    )(idx, wide_got)
    line_got = line_exchange(line_slots, LINE, N_LINE)
    (wide_slots,) = call(
        line_sums_kernel, 1, 2, [f32s(N_WIDE, 4, LANES)], [vmem(12, LANES), vmem(12, LANES)]
    )(idx, line_got, own_sum)
    wide_got = wide_exchange(wide_slots)
    near_slots, own_sum, own_q, own_f = call(
        two_kernel, 1, 4,
        [f32s(N_NEAR, 24, LANES), f32s(PAD, LANES), f32s(6, LANES), f32s(4, LANES)],
        [vmem(PAD, samples), vmem(24, variants), vmem(PAD, samples), vmem(PAD, variants)],
    )(idx, dosage, wide_got, shares, freqs)
    near_got = near_exchange(near_slots)
    far_slots, own_sum = call(last_far_kernel, 1, 2, [pairs, f32s(6, LANES)], [])(
        idx, near_got, own_sum
    )
    far_got = line_exchange(far_slots, FAR, N_FAR)
    return tuple(
        call(last_kernel, 1, 4, [f32s(*shares_init.shape), f32s(*freqs_init.shape)], [], False)(
            idx, far_got, own_sum, own_q, own_f
        )
    )


def solution(mesh):
    fine = Mesh(mesh.devices.reshape(SIZES), AXES)
    return jax.shard_map(
        body,
        mesh=fine,
        in_specs=(P(SMP, VAR), P(None, SMP + VAR), P(None, VAR + SMP)),
        out_specs=(P(None, SMP + VAR), P(None, VAR + SMP)),
        check_vma=False,
    )
```

```python
import jax
import jax.numpy as jnp
from jax import lax
from jax.experimental import pallas as pl
from jax.experimental.pallas import tpu as pltpu
from jax.sharding import Mesh, PartitionSpec as P

K = 12
PAD = 16
LANES = 128
ROWS = 256

AXES = ("y", "zq", "zp", "x", "zh", "c")
SIZES = (4, 4, 2, 4, 2, 2)
SMP = ("y", "zq", "zp")
VAR = ("x", "zh", "c")
NEAR = ("y", "x", "c")
FAR = ("zq", "zp", "zh")
WIDE = ("y", "zp", "x", "c")
LINE = ("zq", "zh")
N_NEAR, N_FAR, N_WIDE, N_LINE = 32, 16, 64, 8
N_Y, N_XC, N_ZL, N_ZH, N_ZQ, N_ROW = 4, 8, 8, 2, 4, 8
FAR_1 = LINE_1 = FAR_2 = 1
NEAR_1 = NEAR_2 = 21
WIDE_1 = WIDE_2 = 37

f32 = jnp.float32
bf16 = jnp.bfloat16


def tile(i):
    return slice(i * LANES, (i + 1) * LANES)


def var_of(idx):
    return idx[0] & 15


def smp_of(idx):
    return idx[0] >> 4


def zl_of(idx):
    return (idx[0] >> 4) & 7


def zh_of(idx):
    return (idx[0] >> 1) & 1


def lane():
    return lax.broadcasted_iota(jnp.int32, (8, LANES), 1)


def roll(x, shift):
    shift = shift % LANES
    return pltpu.roll(x, shift, 1) if shift else x


def two_parts(x):
    high = x.astype(bf16)
    return high, (x - high.astype(f32)).astype(bf16)


def three_parts(x):
    high = x.astype(bf16)
    return (high, *two_parts(x - high.astype(f32)))


def dot(a, b, over_a, over_b):
    return lax.dot_general(
        a, b, (((over_a,), (over_b,)), ((), ())), preferred_element_type=f32
    )


def fold(x):
    return x[:PAD] + x[PAD:]


def block_sums(dosage_ref, shares, freqs):
    qh, qm, ql = three_parts(shares)
    fh, fm, fl = three_parts(freqs)
    q_side = jnp.concatenate([qh, qh, qm, qh, ql, qm], 0)
    f_side = jnp.concatenate([fh, fm, fh, fl, fh, fm], 0)
    q_two = jnp.concatenate([qh, qm], 0)
    f_two = jnp.concatenate([fh, fm], 0)
    g_two = jnp.concatenate(two_parts(1.0 - freqs), 0)
    shift = 2 * lax.broadcasted_iota(jnp.int32, (16, freqs.shape[1]), 0)

    def ratios(at):
        probs = dot(q_side[:, at : at + ROWS], f_side, 0, 0)
        codes = jnp.concatenate(
            [
                jnp.bitwise_and(
                    jnp.right_shift(jnp.broadcast_to(dosage_ref[w : w + 1, :], shift.shape), shift), 3
                )
                for w in range(at // 16, (at + ROWS) // 16)
            ],
            0,
        )
        live = codes < 3
        allele = codes.astype(f32)
        ratio_alt = jnp.where(live, allele, 0.0) * (1.0 / probs)
        ratio_ref = jnp.where(live, 2.0 - allele, 0.0) * (1.0 / (1.0 - probs))
        return two_parts(ratio_alt) + two_parts(ratio_ref)

    sums_q, sum_a, sum_b = [], 0.0, 0.0
    starts = range(0, shares.shape[1], ROWS)
    ready = ratios(0)
    for at in starts:
        ah, al, bh, bl = ready
        if at + ROWS in starts:
            ready = ratios(at + ROWS)
        sums_q.append(
            dot(f_two, ah, 1, 1) + dot(f_two, al, 1, 1) + dot(g_two, bh, 1, 1) + dot(g_two, bl, 1, 1)
        )
        q_part = q_two[:, at : at + ROWS]
        sum_a = sum_a + (dot(q_part, ah, 1, 0) + dot(q_part, al, 1, 0))
        sum_b = sum_b + (dot(q_part, bh, 1, 0) + dot(q_part, bl, 1, 0))
    return fold(jnp.concatenate(sums_q, 1)), fold(sum_a), fold(sum_b)


def in_plane(y, g):
    return y * N_XC + g


def in_line(i, h):
    return i * N_ZH + h


def zq_of(idx):
    return (idx[0] >> 5) & 3


def near_of(idx):
    return ((idx[0] >> 1) & 6) | (idx[0] & 1)


def y_of(idx):
    return idx[0] >> 7


def halves(a, b):
    left = lax.broadcasted_iota(jnp.int32, a.shape, 1) < 64
    return jnp.where(left, a, roll(b, 64)), jnp.where(left, roll(a, 64), b)


def block_of_lane():
    return lax.broadcasted_iota(jnp.int32, (4, LANES), 1) // 16


def put_far(far_out, at, rows):
    for b in range(3):
        far_out[3 * at + b] = rows[2 * b : 2 * b + 2]


def get_far(far_in, at, pairs):
    return jnp.concatenate([far_in[3 * at + b] for b in range(pairs)], 0)


def first_kernel(idx, shares_ref, freqs_ref, far_out, q_out, f_tmp):
    raw = shares_ref[...]
    own = raw / jnp.sum(raw, axis=0, keepdims=True)
    q_out[...] = jnp.zeros_like(q_out)
    f_tmp[...] = jnp.zeros_like(f_tmp)
    q_out[0:6, 0:64] = own[0:6]
    q_out[0:6, 64:128] = own[6:12]
    for j in range(3):
        f_tmp[0:4, 16 * j : 16 * j + 16] = freqs_ref[4 * j : 4 * j + 4, :]
    turned = pltpu.roll(f_tmp[...], 16 * zl_of(idx), 1)
    for h in range(N_ZH):
        sent = jnp.where(zh_of(idx) == h, turned, q_out[...])
        for i in range(N_ZL):
            put_far(far_out, in_line(i, h) ^ FAR_1, sent)


def first_near_kernel(idx, far_in, q_in, near_out, f_out, q_tmp):
    zh = zh_of(idx)
    block = block_of_lane()
    freqs = [get_far(far_in, in_line(i, zh) ^ FAR_1, 2) for i in range(N_ZL)]
    for j in range(3):
        got = freqs[0]
        for i in range(1, N_ZL):
            got = jnp.where(block == (i + j) % 8, freqs[i], got)
        f_out[j] = roll(got, -16 * j)
    own, other = q_in[0:6], get_far(far_in, in_line(zl_of(idx), 1 - zh) ^ FAR_1, 3)
    q_tmp[0:6], q_tmp[6:12] = halves(jnp.where(zh == 0, own, other), jnp.where(zh == 0, other, own))
    for s in range(N_NEAR):
        near_out[3 * s : 3 * s + 3] = f_out[...]
    for g in range(N_XC):
        s = 3 * (in_plane(y_of(idx), g) ^ NEAR_1)
        for j in range(3):
            near_out[s + j] = q_tmp[4 * j : 4 * j + 4]


def shares_of(idx, near_in):
    rows = [[], [], []]
    for x in range(4):
        for j in range(3):
            a, b = (near_in[3 * (in_plane(y_of(idx), 2 * x + c) ^ NEAR_1) + j] for c in range(2))
            rows[j].extend(halves(a, b))
    return padded(rows)


def freqs_of(idx, near_in, f_in):
    rows = [[], [], []]
    for y in range(N_Y):
        for j in range(3):
            got = near_in[3 * (in_plane(y, near_of(idx)) ^ NEAR_1) + j]
            rows[j].append(jnp.where(y_of(idx) == y, f_in[j], got))
    return padded(rows)


def padded(rows):
    rows = [jnp.concatenate(row, 1) for row in rows]
    return jnp.concatenate([*rows, jnp.zeros_like(rows[0])], 0)


def turned_tiles(x):
    return jnp.concatenate([roll(x[:, tile(t)], 64) for t in range(x.shape[1] // LANES)], 1)


def left_of(rows):
    return lax.broadcasted_iota(jnp.int32, (rows, LANES), 1) < 64


def one_kernel(idx, dosage_ref, near_in, own_f_in, slots, q_out, f_out, sq_tmp, sa_tmp, sq_turn, sa_turn):
    shares = shares_of(idx, near_in)
    freqs = freqs_of(idx, near_in, own_f_in)
    q_out[...] = shares
    f_out[...] = freqs
    sum_q, sum_a, sum_b = block_sums(dosage_ref, shares, freqs)
    sq_tmp[...] = sum_q
    sa_tmp[0:12] = sum_a[0:12]
    sa_tmp[12:24] = sum_b[0:12]
    sq_turn[...] = turned_tiles(sum_q)
    sa_turn[...] = turned_tiles(sa_tmp[...])
    left = left_of(3)
    for w in range(N_WIDE):
        t, q = divmod(w, 4)
        a = (sq_turn if t % 2 else sq_tmp)[3 * q : 3 * q + 3, tile(t // 2)]
        t, q = divmod(w, 8)
        b = (sa_tmp if t % 2 else sa_turn)[3 * q : 3 * q + 3, tile(t // 2)]
        put_wide(slots, w ^ WIDE_1, jnp.where(left, a, b))


def put_wide(wide_out, at, rows):
    for r in range(3):
        wide_out[3 * at + r] = rows[r : r + 1]


def put_line(line_out, at, rows):
    for b in range(3):
        line_out[3 * at + b] = rows[4 * b : 4 * b + 4]


def wide_sums_kernel(idx, wide_in, line_out, q_out, a_tmp):
    left = left_of(1)
    for r in range(3):
        got = [[wide_in[3 * (in_plane(i, g) ^ WIDE_1) + r] for g in range(N_XC)] for i in range(N_ROW)]
        row_sums = [sum(row) for row in got]
        col_sums = [sum(row[g] for row in got) for g in range(N_XC)]
        for i in range(4):
            at = 3 * i + r
            q_out[at : at + 1] = jnp.where(left, row_sums[i], roll(row_sums[i + 4], 64))
            a_tmp[at : at + 1] = jnp.where(left, roll(col_sums[i], 64), col_sums[i + 4])
    for h in range(N_ZH):
        sent = jnp.where(zh_of(idx) == h, a_tmp[...], q_out[...])
        for i in range(N_ZQ):
            put_line(line_out, in_line(i, h) ^ LINE_1, sent)


def line_sums_kernel(idx, line_in, q_in, wide_out, q_tmp, a_tmp):
    zh = zh_of(idx)
    for b in range(3):
        a_tmp[4 * b : 4 * b + 4] = sum(line_in[3 * (in_line(i, zh) ^ LINE_1) + b] for i in range(N_ZQ))
        other = line_in[3 * (in_line(zq_of(idx), 1 - zh) ^ LINE_1) + b]
        q_tmp[4 * b : 4 * b + 4] = q_in[4 * b : 4 * b + 4] + other
    left = left_of(3)
    row_sums, col_sums = [], []
    for i in range(8):
        at = 3 * (i % 4)
        row_sums.append(roll(q_tmp[at : at + 3], 64 * (i // 4)))
        col_sums.append(roll(a_tmp[at : at + 3], 64 * (1 - i // 4)))
    for r in range(N_ROW):
        for g in range(N_XC):
            put_wide(wide_out, in_plane(r, g) ^ WIDE_2, jnp.where(left, row_sums[r], col_sums[g]))


def two_kernel(idx, dosage_ref, wide_in, q_in, f_in, near_out, sq_out, own_q, own_f, sq_tmp, sa_tmp, q_tmp, f_tmp):
    left = left_of(1)
    for t in range(8):
        for q in range(4):
            for r in range(3):
                a, b = (wide_in[3 * ((8 * t + 4 * half + q) ^ WIDE_2) + r] for half in range(2))
                sq_tmp[3 * q + r : 3 * q + r + 1, tile(t)] = jnp.where(left, a, roll(b, 64))
    for t in range(4):
        for q in range(8):
            for r in range(3):
                a, b = (wide_in[3 * ((16 * t + 8 * half + q) ^ WIDE_2) + r] for half in range(2))
                sa_tmp[3 * q + r : 3 * q + r + 1, tile(t)] = jnp.where(left, roll(a, 64), b)
    q_tmp[...] = q_in[...]
    f_tmp[...] = f_in[...]
    numer = q_tmp[0:12] * sq_tmp[0:12]
    q_tmp[0:12] = (numer + 0.5) / (jnp.sum(numer, axis=0, keepdims=True) + 0.5 * K)
    old = f_tmp[0:12]
    alt_part = old * sa_tmp[0:12]
    f_tmp[0:12] = (alt_part + 0.5) / (alt_part + (1.0 - old) * sa_tmp[12:24] + 1.0)

    t = pl.multiple_of((var_of(idx) >> 1) * LANES, LANES)
    even, odd = halves(q_tmp[0:6, pl.ds(t, LANES)], q_tmp[6:12, pl.ds(t, LANES)])
    own_q[...] = jnp.where((var_of(idx) & 1) == 0, even, odd)
    t = pl.multiple_of((smp_of(idx) >> 3) * LANES, LANES)
    block = block_of_lane()
    got = f_tmp[0:4, pl.ds(t, LANES)]
    for j in range(1, 3):
        got = jnp.where(
            block == ((zl_of(idx) + j) & 7), roll(f_tmp[4 * j : 4 * j + 4, pl.ds(t, LANES)], 16 * j), got
        )
    own_f[...] = got

    sum_q, sum_a, sum_b = block_sums(dosage_ref, q_tmp[...], f_tmp[...])
    for x in range(4):
        pair = halves(sum_q[:, tile(2 * x)], sum_q[:, tile(2 * x + 1)])
        for c in range(2):
            for y in range(N_Y):
                near_out[in_plane(y, 2 * x + c) ^ NEAR_2, 0:16] = pair[c]
    sq_out[...] = near_out[in_plane(0, near_of(idx)) ^ NEAR_2, 0:16]
    sa_tmp[0:12] = sum_a[0:12]
    sa_tmp[12:24] = sum_b[0:12]
    for y in range(N_Y):
        near_out[in_plane(y, near_of(idx)) ^ NEAR_2] = sa_tmp[:, tile(y)]


def last_far_kernel(idx, near_in, sq_in, far_out, q_out):
    zh, near = zh_of(idx), near_of(idx)
    sum_q = sq_in[...]
    for g in range(N_XC):
        got = near_in[in_plane(y_of(idx), g) ^ NEAR_2, 0:16]
        sum_q = sum_q + jnp.where(near == g, 0.0, got)
    sums = sum(near_in[in_plane(y, near) ^ NEAR_2] for y in range(N_Y))
    parts = halves(sum_q[0:6], sum_q[6:12])
    q_out[...] = jnp.where(zh == 0, parts[0], parts[1])
    block = block_of_lane()
    turned = [roll(sums[4 * j : 4 * j + 4], 16 * j) for j in range(6)]
    for i in range(N_ZL):
        got = turned[0]
        for j in range(1, 6):
            got = jnp.where(block == (i + j) % 8, turned[j], got)
        got = jnp.concatenate([got, got[0:2]], 0)
        for h in range(N_ZH):
            put_far(far_out, in_line(i, h) ^ FAR_2, jnp.where(zh == h, got, parts[h]))


def last_kernel(idx, far_in, sq_in, own_q, own_f, shares_out, freqs_out):
    zh = zh_of(idx)
    sum_q = sq_in[...] + get_far(far_in, in_line(zl_of(idx), 1 - zh) ^ FAR_2, 3)
    numer = own_q[...] * sum_q
    total = jnp.sum(numer, axis=0, keepdims=True)
    total = total + pltpu.roll(total, 64, 1)
    new = (numer + 0.5) / (total + 0.5 * K)
    shares_out[0:6] = new[:, 0:64]
    shares_out[6:12] = new[:, 64:128]
    sums = sum(get_far(far_in, in_line(i, zh) ^ FAR_2, 2) for i in range(N_ZL))
    alt_part = own_f[...] * sums
    ref_part = (1.0 - own_f[...]) * roll(sums, -48)
    new = (alt_part + 0.5) / (alt_part + ref_part + 1.0)
    new = pltpu.roll(jnp.concatenate([new, new], 0), (LANES - 16 * zl_of(idx)) & (LANES - 1), 1)
    for j in range(3):
        freqs_out[4 * j : 4 * j + 4] = new[0:4, 16 * j : 16 * j + 16]


def f32s(*shape):
    return jax.ShapeDtypeStruct(shape, f32)


def vmem(*shape):
    return pltpu.VMEM(shape, f32)


def call(kernel, scalars, n_in, outs, scratch, kept=True):
    spec = pl.BlockSpec(memory_space=pltpu.VMEM)
    run = pl.pallas_call(
        kernel,
        in_specs=[pl.BlockSpec(memory_space=pltpu.SMEM)] * scalars + [spec] * n_in,
        out_specs=[spec] * len(outs),
        out_shape=[pltpu.VMEM(o.shape, o.dtype) for o in outs] if kept else outs,
        scratch_shapes=scratch,
    )

    def placed(*args):
        args = args[:scalars] + tuple(
            pltpu.with_memory_space_constraint(a, pltpu.VMEM) for a in args[scalars:]
        )
        return run(*args)

    return placed


def exchange(x, axes, first):
    members = 1
    for axis in axes:
        members *= SIZES[AXES.index(axis)]
    order = [[i ^ first for i in range(members)]]
    return lax.all_to_all(x, axes, 0, 0, tiled=True, axis_index_groups=order)


def body(dosage, shares_init, freqs_init):
    idx = lax.axis_index(AXES).astype(jnp.int32).reshape(1)
    samples, variants = 16 * dosage.shape[0], dosage.shape[1]
    pairs = f32s(3 * N_FAR, 2, LANES)
    far_slots, own_q = call(first_kernel, 1, 2, [pairs, f32s(8, LANES)], [vmem(8, LANES)])(
        idx, shares_init, freqs_init
    )
    far_got = exchange(far_slots, FAR, FAR_1)
    near_slots, own_f = call(
        first_near_kernel, 1, 2, [f32s(3 * N_NEAR, 4, LANES), f32s(3, 4, LANES)], [vmem(12, LANES)]
    )(idx, far_got, own_q)
    near_got = exchange(near_slots, NEAR, NEAR_1)
    slots, shares, freqs = call(
        one_kernel, 1, 3, [f32s(3 * N_WIDE, 1, LANES), f32s(PAD, samples), f32s(PAD, variants)],
        [vmem(PAD, samples), vmem(24, variants), vmem(PAD, samples), vmem(24, variants)],
    )(idx, dosage, near_got, own_f)
    wide_got = exchange(slots, WIDE, WIDE_1)
    line_slots, own_sum = call(
        wide_sums_kernel, 1, 1, [f32s(3 * N_LINE, 4, LANES), f32s(12, LANES)], [vmem(12, LANES)]
    )(idx, wide_got)
    line_got = exchange(line_slots, LINE, LINE_1)
    (wide_slots,) = call(
        line_sums_kernel, 1, 2, [f32s(3 * N_WIDE, 1, LANES)], [vmem(12, LANES), vmem(12, LANES)]
    )(idx, line_got, own_sum)
    wide_got = exchange(wide_slots, WIDE, WIDE_2)
    near_slots, own_sum, own_q, own_f = call(
        two_kernel, 1, 4,
        [f32s(N_NEAR, 24, LANES), f32s(PAD, LANES), f32s(6, LANES), f32s(4, LANES)],
        [vmem(PAD, samples), vmem(24, variants), vmem(PAD, samples), vmem(PAD, variants)],
    )(idx, dosage, wide_got, shares, freqs)
    near_got = exchange(near_slots, NEAR, NEAR_2)
    far_slots, own_sum = call(last_far_kernel, 1, 2, [pairs, f32s(6, LANES)], [])(
        idx, near_got, own_sum
    )
    far_got = exchange(far_slots, FAR, FAR_2)
    return tuple(
        call(last_kernel, 1, 4, [f32s(*shares_init.shape), f32s(*freqs_init.shape)], [], False)(
            idx, far_got, own_sum, own_q, own_f
        )
    )


def solution(mesh):
    fine = Mesh(mesh.devices.reshape(SIZES), AXES)
    return jax.shard_map(
        body,
        mesh=fine,
        in_specs=(P(SMP, VAR), P(None, SMP + VAR), P(None, VAR + SMP)),
        out_specs=(P(None, SMP + VAR), P(None, VAR + SMP)),
        check_vma=False,
    )
```

```python
import jax
import jax.numpy as jnp
from jax import lax
from jax.experimental import pallas as pl
from jax.experimental.pallas import tpu as pltpu
from jax.sharding import Mesh, PartitionSpec as P

K = 12
PAD = 16
LANES = 128
ROWS = 256

AXES = ("y", "zq", "zp", "x", "zh", "c")
SIZES = (4, 4, 2, 4, 2, 2)
SMP = ("y", "zq", "zp")
VAR = ("x", "zh", "c")
NEAR = ("y", "x", "c")
FAR = ("zq", "zp", "zh")
WIDE = ("y", "zp", "x", "c")
LINE = ("zq", "zh")
N_NEAR, N_FAR, N_WIDE, N_LINE = 32, 16, 64, 8
N_Y, N_XC, N_ZL, N_ZH, N_ZQ, N_ROW = 4, 8, 8, 2, 4, 8
FAR_1 = LINE_1 = FAR_2 = 1
NEAR_1 = NEAR_2 = 21
WIDE_1 = WIDE_2 = 37

f32 = jnp.float32
bf16 = jnp.bfloat16


def tile(i):
    return slice(i * LANES, (i + 1) * LANES)


def var_of(idx):
    return idx[0] & 15


def smp_of(idx):
    return idx[0] >> 4


def zl_of(idx):
    return (idx[0] >> 4) & 7


def zh_of(idx):
    return (idx[0] >> 1) & 1


def lane():
    return lax.broadcasted_iota(jnp.int32, (8, LANES), 1)


def roll(x, shift):
    shift = shift % LANES
    return pltpu.roll(x, shift, 1) if shift else x


def two_parts(x):
    high = x.astype(bf16)
    return high, (x - high.astype(f32)).astype(bf16)


def three_parts(x):
    high = x.astype(bf16)
    return (high, *two_parts(x - high.astype(f32)))


def dot(a, b, over_a, over_b):
    return lax.dot_general(
        a, b, (((over_a,), (over_b,)), ((), ())), preferred_element_type=f32
    )


def fold(x):
    return x[:PAD] + x[PAD:]


def block_sums(dosage_ref, shares, freqs):
    qh, qm, ql = three_parts(shares)
    fh, fm, fl = three_parts(freqs)
    q_side = jnp.concatenate([qh, qh, qm, qh, ql, qm], 0)
    f_side = jnp.concatenate([fh, fm, fh, fl, fh, fm], 0)
    q_two = jnp.concatenate([qh, qm], 0)
    f_two = jnp.concatenate([fh, fm], 0)
    g_two = jnp.concatenate(two_parts(1.0 - freqs), 0)
    shift = 2 * lax.broadcasted_iota(jnp.int32, (16, freqs.shape[1]), 0)

    def ratios(at):
        probs = dot(q_side[:, at : at + ROWS], f_side, 0, 0)
        codes = jnp.concatenate(
            [
                jnp.bitwise_and(
                    jnp.right_shift(jnp.broadcast_to(dosage_ref[w : w + 1, :], shift.shape), shift), 3
                )
                for w in range(at // 16, (at + ROWS) // 16)
            ],
            0,
        )
        live = codes < 3
        allele = codes.astype(f32)
        ratio_alt = jnp.where(live, allele, 0.0) * (1.0 / probs)
        ratio_ref = jnp.where(live, 2.0 - allele, 0.0) * (1.0 / (1.0 - probs))
        return two_parts(ratio_alt) + two_parts(ratio_ref)

    sums_q, sum_a, sum_b = [], 0.0, 0.0
    starts = range(0, shares.shape[1], ROWS)
    ready = ratios(0)
    for at in starts:
        ah, al, bh, bl = ready
        if at + ROWS in starts:
            ready = ratios(at + ROWS)
        sums_q.append(
            dot(f_two, ah, 1, 1) + dot(f_two, al, 1, 1) + dot(g_two, bh, 1, 1) + dot(g_two, bl, 1, 1)
        )
        q_part = q_two[:, at : at + ROWS]
        sum_a = sum_a + (dot(q_part, ah, 1, 0) + dot(q_part, al, 1, 0))
        sum_b = sum_b + (dot(q_part, bh, 1, 0) + dot(q_part, bl, 1, 0))
    return fold(jnp.concatenate(sums_q, 1)), fold(sum_a), fold(sum_b)


def in_plane(y, g):
    return y * N_XC + g


def in_line(i, h):
    return i * N_ZH + h


def zq_of(idx):
    return (idx[0] >> 5) & 3


def near_of(idx):
    return ((idx[0] >> 1) & 6) | (idx[0] & 1)


def y_of(idx):
    return idx[0] >> 7


def halves(a, b):
    left = lax.broadcasted_iota(jnp.int32, a.shape, 1) < 64
    return jnp.where(left, a, roll(b, 64)), jnp.where(left, roll(a, 64), b)


def block_of_lane():
    return lax.broadcasted_iota(jnp.int32, (4, LANES), 1) // 16


def put_far(far_out, at, rows):
    for b in range(3):
        far_out[3 * at + b] = rows[2 * b : 2 * b + 2]


def get_far(far_in, at, pairs):
    return jnp.concatenate([far_in[3 * at + b] for b in range(pairs)], 0)


def first_kernel(idx, shares_ref, freqs_ref, far_out, q_out, f_tmp):
    raw = shares_ref[...]
    own = raw / jnp.sum(raw, axis=0, keepdims=True)
    q_out[...] = jnp.zeros_like(q_out)
    f_tmp[...] = jnp.zeros_like(f_tmp)
    q_out[0:6, 0:64] = own[0:6]
    q_out[0:6, 64:128] = own[6:12]
    for j in range(3):
        f_tmp[0:4, 16 * j : 16 * j + 16] = freqs_ref[4 * j : 4 * j + 4, :]
    turned = pltpu.roll(f_tmp[...], 16 * zl_of(idx), 1)
    for h in range(N_ZH):
        sent = jnp.where(zh_of(idx) == h, turned, q_out[...])
        for i in range(N_ZL):
            put_far(far_out, in_line(i, h) ^ FAR_1, sent)


def first_near_kernel(idx, far_in, q_in, near_out, f_out, q_tmp):
    zh = zh_of(idx)
    block = block_of_lane()
    freqs = [get_far(far_in, in_line(i, zh) ^ FAR_1, 2) for i in range(N_ZL)]
    for j in range(3):
        got = freqs[0]
        for i in range(1, N_ZL):
            got = jnp.where(block == (i + j) % 8, freqs[i], got)
        f_out[j] = roll(got, -16 * j)
    own, other = q_in[0:6], get_far(far_in, in_line(zl_of(idx), 1 - zh) ^ FAR_1, 3)
    q_tmp[0:6], q_tmp[6:12] = halves(jnp.where(zh == 0, own, other), jnp.where(zh == 0, other, own))
    for s in range(N_NEAR):
        near_out[3 * s : 3 * s + 3] = f_out[...]
    for g in range(N_XC):
        s = 3 * (in_plane(y_of(idx), g) ^ NEAR_1)
        for j in range(3):
            near_out[s + j] = q_tmp[4 * j : 4 * j + 4]


def shares_of(idx, near_in):
    rows = [[], [], []]
    for x in range(4):
        for j in range(3):
            a, b = (near_in[3 * (in_plane(y_of(idx), 2 * x + c) ^ NEAR_1) + j] for c in range(2))
            rows[j].extend(halves(a, b))
    return padded(rows)


def freqs_of(idx, near_in, f_in):
    rows = [[], [], []]
    for y in range(N_Y):
        for j in range(3):
            got = near_in[3 * (in_plane(y, near_of(idx)) ^ NEAR_1) + j]
            rows[j].append(jnp.where(y_of(idx) == y, f_in[j], got))
    return padded(rows)


def padded(rows):
    rows = [jnp.concatenate(row, 1) for row in rows]
    return jnp.concatenate([*rows, jnp.zeros_like(rows[0])], 0)


def turned_tiles(x):
    return jnp.concatenate([roll(x[:, tile(t)], 64) for t in range(x.shape[1] // LANES)], 1)


def left_of(rows):
    return lax.broadcasted_iota(jnp.int32, (rows, LANES), 1) < 64


def one_kernel(idx, dosage_ref, near_in, own_f_in, slots, q_out, f_out, sq_tmp, sa_tmp, sq_turn, sa_turn):
    shares = shares_of(idx, near_in)
    freqs = freqs_of(idx, near_in, own_f_in)
    q_out[...] = shares
    f_out[...] = freqs
    sum_q, sum_a, sum_b = block_sums(dosage_ref, shares, freqs)
    sq_tmp[...] = sum_q
    sa_tmp[0:12] = sum_a[0:12]
    sa_tmp[12:24] = sum_b[0:12]
    sq_turn[...] = turned_tiles(sum_q)
    sa_turn[...] = turned_tiles(sa_tmp[...])
    left = left_of(3)
    for w in range(N_WIDE):
        t, q = divmod(w, 4)
        a = (sq_turn if t % 2 else sq_tmp)[3 * q : 3 * q + 3, tile(t // 2)]
        t, q = divmod(w, 8)
        b = (sa_tmp if t % 2 else sa_turn)[3 * q : 3 * q + 3, tile(t // 2)]
        put_wide(slots, w ^ WIDE_1, jnp.where(left, a, b))


def put_wide(wide_out, at, rows):
    for r in range(3):
        wide_out[3 * at + r] = rows[r : r + 1]


def put_line(line_out, at, rows):
    for b in range(3):
        line_out[3 * at + b] = rows[4 * b : 4 * b + 4]


def wide_sums_kernel(idx, wide_in, line_out, q_out, a_tmp):
    left = left_of(1)
    for r in range(3):
        got = [[wide_in[3 * (in_plane(i, g) ^ WIDE_1) + r] for g in range(N_XC)] for i in range(N_ROW)]
        row_sums = [sum(row) for row in got]
        col_sums = [sum(row[g] for row in got) for g in range(N_XC)]
        for i in range(4):
            at = 3 * i + r
            q_out[at : at + 1] = jnp.where(left, row_sums[i], roll(row_sums[i + 4], 64))
            a_tmp[at : at + 1] = jnp.where(left, roll(col_sums[i], 64), col_sums[i + 4])
    for h in range(N_ZH):
        sent = jnp.where(zh_of(idx) == h, a_tmp[...], q_out[...])
        for i in range(N_ZQ):
            put_line(line_out, in_line(i, h) ^ LINE_1, sent)


def line_sums_kernel(idx, line_in, q_in, wide_out, q_tmp, a_tmp):
    zh = zh_of(idx)
    for b in range(3):
        a_tmp[4 * b : 4 * b + 4] = sum(line_in[3 * (in_line(i, zh) ^ LINE_1) + b] for i in range(N_ZQ))
        other = line_in[3 * (in_line(zq_of(idx), 1 - zh) ^ LINE_1) + b]
        q_tmp[4 * b : 4 * b + 4] = q_in[4 * b : 4 * b + 4] + other
    left = left_of(3)
    row_sums, col_sums = [], []
    for i in range(8):
        at = 3 * (i % 4)
        row_sums.append(roll(q_tmp[at : at + 3], 64 * (i // 4)))
        col_sums.append(roll(a_tmp[at : at + 3], 64 * (1 - i // 4)))
    for r in range(N_ROW):
        for g in range(N_XC):
            put_wide(wide_out, in_plane(r, g) ^ WIDE_2, jnp.where(left, row_sums[r], col_sums[g]))


def two_kernel(idx, dosage_ref, wide_in, q_in, f_in, near_out, sq_out, own_q, own_f, sq_tmp, sa_tmp, q_tmp, f_tmp):
    left = left_of(1)
    for t in range(8):
        for q in range(4):
            for r in range(3):
                a, b = (wide_in[3 * ((8 * t + 4 * half + q) ^ WIDE_2) + r] for half in range(2))
                sq_tmp[3 * q + r : 3 * q + r + 1, tile(t)] = jnp.where(left, a, roll(b, 64))
    for t in range(4):
        for q in range(8):
            for r in range(3):
                a, b = (wide_in[3 * ((16 * t + 8 * half + q) ^ WIDE_2) + r] for half in range(2))
                sa_tmp[3 * q + r : 3 * q + r + 1, tile(t)] = jnp.where(left, roll(a, 64), b)
    q_tmp[...] = q_in[...]
    f_tmp[...] = f_in[...]
    numer = q_tmp[0:12] * sq_tmp[0:12]
    q_tmp[0:12] = (numer + 0.5) / (jnp.sum(numer, axis=0, keepdims=True) + 0.5 * K)
    old = f_tmp[0:12]
    alt_part = old * sa_tmp[0:12]
    f_tmp[0:12] = (alt_part + 0.5) / (alt_part + (1.0 - old) * sa_tmp[12:24] + 1.0)

    t = pl.multiple_of((var_of(idx) >> 1) * LANES, LANES)
    even, odd = halves(q_tmp[0:6, pl.ds(t, LANES)], q_tmp[6:12, pl.ds(t, LANES)])
    own_q[...] = jnp.where((var_of(idx) & 1) == 0, even, odd)
    t = pl.multiple_of((smp_of(idx) >> 3) * LANES, LANES)
    block = block_of_lane()
    got = f_tmp[0:4, pl.ds(t, LANES)]
    for j in range(1, 3):
        got = jnp.where(
            block == ((zl_of(idx) + j) & 7), roll(f_tmp[4 * j : 4 * j + 4, pl.ds(t, LANES)], 16 * j), got
        )
    own_f[...] = got

    sum_q, sum_a, sum_b = block_sums(dosage_ref, q_tmp[...], f_tmp[...])
    for x in range(4):
        pair = halves(sum_q[:, tile(2 * x)], sum_q[:, tile(2 * x + 1)])
        for c in range(2):
            for y in range(N_Y):
                near_out[in_plane(y, 2 * x + c) ^ NEAR_2, 0:16] = pair[c]
    sq_out[...] = near_out[in_plane(0, near_of(idx)) ^ NEAR_2, 0:16]
    sa_tmp[0:12] = sum_a[0:12]
    sa_tmp[12:24] = sum_b[0:12]
    for y in range(N_Y):
        near_out[in_plane(y, near_of(idx)) ^ NEAR_2] = sa_tmp[:, tile(y)]


def last_far_kernel(idx, near_in, sq_in, far_out, q_out):
    zh, near = zh_of(idx), near_of(idx)
    sum_q = sq_in[...]
    for g in range(N_XC):
        got = near_in[in_plane(y_of(idx), g) ^ NEAR_2, 0:16]
        sum_q = sum_q + jnp.where(near == g, 0.0, got)
    sums = sum(near_in[in_plane(y, near) ^ NEAR_2] for y in range(N_Y))
    parts = halves(sum_q[0:6], sum_q[6:12])
    q_out[...] = jnp.where(zh == 0, parts[0], parts[1])
    block = block_of_lane()
    turned = [roll(sums[4 * j : 4 * j + 4], 16 * j) for j in range(6)]
    for i in range(N_ZL):
        got = turned[0]
        for j in range(1, 6):
            got = jnp.where(block == (i + j) % 8, turned[j], got)
        got = jnp.concatenate([got, got[0:2]], 0)
        for h in range(N_ZH):
            put_far(far_out, in_line(i, h) ^ FAR_2, jnp.where(zh == h, got, parts[h]))


def last_kernel(idx, far_in, sq_in, own_q, own_f, shares_out, freqs_out):
    zh = zh_of(idx)
    sum_q = sq_in[...] + get_far(far_in, in_line(zl_of(idx), 1 - zh) ^ FAR_2, 3)
    numer = own_q[...] * sum_q
    total = jnp.sum(numer, axis=0, keepdims=True)
    total = total + pltpu.roll(total, 64, 1)
    new = (numer + 0.5) / (total + 0.5 * K)
    shares_out[0:6] = new[:, 0:64]
    shares_out[6:12] = new[:, 64:128]
    sums = sum(get_far(far_in, in_line(i, zh) ^ FAR_2, 2) for i in range(N_ZL))
    alt_part = own_f[...] * sums
    ref_part = (1.0 - own_f[...]) * roll(sums, -48)
    new = (alt_part + 0.5) / (alt_part + ref_part + 1.0)
    new = pltpu.roll(jnp.concatenate([new, new], 0), (LANES - 16 * zl_of(idx)) & (LANES - 1), 1)
    for j in range(3):
        freqs_out[4 * j : 4 * j + 4] = new[0:4, 16 * j : 16 * j + 16]


def f32s(*shape):
    return jax.ShapeDtypeStruct(shape, f32)


def vmem(*shape):
    return pltpu.VMEM(shape, f32)


def call(kernel, scalars, n_in, outs, scratch, kept=True):
    spec = pl.BlockSpec(memory_space=pltpu.VMEM)
    run = pl.pallas_call(
        kernel,
        in_specs=[pl.BlockSpec(memory_space=pltpu.SMEM)] * scalars + [spec] * n_in,
        out_specs=[spec] * len(outs),
        out_shape=[pltpu.VMEM(o.shape, o.dtype) for o in outs] if kept else outs,
        scratch_shapes=scratch,
    )

    def placed(*args):
        args = args[:scalars] + tuple(
            pltpu.with_memory_space_constraint(a, pltpu.VMEM) for a in args[scalars:]
        )
        return run(*args)

    return placed


def exchange(x, axes, first):
    members = 1
    for axis in axes:
        members *= SIZES[AXES.index(axis)]
    order = [[i ^ first for i in range(members)]]
    return lax.all_to_all(x, axes, 0, 0, tiled=True, axis_index_groups=order)


def body(dosage, shares_init, freqs_init):
    idx = lax.axis_index(AXES).astype(jnp.int32).reshape(1)
    samples, variants = 16 * dosage.shape[0], dosage.shape[1]
    pairs = f32s(3 * N_FAR, 2, LANES)
    far_slots, own_q = call(first_kernel, 1, 2, [pairs, f32s(8, LANES)], [vmem(8, LANES)])(
        idx, shares_init, freqs_init
    )
    far_got = exchange(far_slots, FAR, FAR_1)
    near_slots, own_f = call(
        first_near_kernel, 1, 2, [f32s(3 * N_NEAR, 4, LANES), f32s(3, 4, LANES)], [vmem(12, LANES)]
    )(idx, far_got, own_q)
    near_got = exchange(near_slots, NEAR, NEAR_1)
    slots, shares, freqs = call(
        one_kernel, 1, 3, [f32s(3 * N_WIDE, 1, LANES), f32s(PAD, samples), f32s(PAD, variants)],
        [vmem(PAD, samples), vmem(24, variants), vmem(PAD, samples), vmem(24, variants)],
    )(idx, dosage, near_got, own_f)
    wide_got = exchange(slots, WIDE, WIDE_1)
    line_slots, own_sum = call(
        wide_sums_kernel, 1, 1, [f32s(3 * N_LINE, 4, LANES), f32s(12, LANES)], [vmem(12, LANES)]
    )(idx, wide_got)
    line_got = exchange(line_slots, LINE, LINE_1)
    (wide_slots,) = call(
        line_sums_kernel, 1, 2, [f32s(3 * N_WIDE, 1, LANES)], [vmem(12, LANES), vmem(12, LANES)]
    )(idx, line_got, own_sum)
    wide_got = exchange(wide_slots, WIDE, WIDE_2)
    near_slots, own_sum, own_q, own_f = call(
        two_kernel, 1, 4,
        [f32s(N_NEAR, 24, LANES), f32s(PAD, LANES), f32s(6, LANES), f32s(4, LANES)],
        [vmem(PAD, samples), vmem(24, variants), vmem(PAD, samples), vmem(PAD, variants)],
    )(idx, dosage, wide_got, shares, freqs)
    near_got = exchange(near_slots, NEAR, NEAR_2)
    far_slots, own_sum = call(last_far_kernel, 1, 2, [pairs, f32s(6, LANES)], [])(
        idx, near_got, own_sum
    )
    far_got = exchange(far_slots, FAR, FAR_2)
    return tuple(
        call(last_kernel, 1, 4, [f32s(*shares_init.shape), f32s(*freqs_init.shape)], [])(
            idx, far_got, own_sum, own_q, own_f
        )
    )


def solution(mesh):
    fine = Mesh(mesh.devices.reshape(SIZES), AXES)
    return jax.shard_map(
        body,
        mesh=fine,
        in_specs=(P(SMP, VAR), P(None, SMP + VAR), P(None, VAR + SMP)),
        out_specs=(P(None, SMP + VAR), P(None, VAR + SMP)),
        check_vma=False,
    )
```

```python
import jax
import jax.numpy as jnp
from jax import lax
from jax.experimental import pallas as pl
from jax.experimental.pallas import tpu as pltpu
from jax.sharding import Mesh, PartitionSpec as P

K = 12
PAD = 16
LANES = 128
ROWS = 256

AXES = ("y", "zq", "zp", "x", "zh", "c")
SIZES = (4, 4, 2, 4, 2, 2)
SMP = ("y", "zq", "zp")
VAR = ("x", "zh", "c")
NEAR = ("y", "x", "c")
FAR = ("zq", "zp", "zh")
WIDE = ("y", "zp", "x", "c")
LINE = ("zq", "zh")
N_NEAR, N_FAR, N_WIDE, N_LINE = 32, 16, 64, 8
N_Y, N_XC, N_ZL, N_ZH, N_ZQ, N_ROW = 4, 8, 8, 2, 4, 8
FAR_1 = LINE_1 = FAR_2 = 1
NEAR_1 = NEAR_2 = 21
WIDE_1 = WIDE_2 = 37

f32 = jnp.float32
bf16 = jnp.bfloat16


def tile(i):
    return slice(i * LANES, (i + 1) * LANES)


def var_of(idx):
    return idx[0] & 15


def smp_of(idx):
    return idx[0] >> 4


def zl_of(idx):
    return (idx[0] >> 4) & 7


def zh_of(idx):
    return (idx[0] >> 1) & 1


def lane():
    return lax.broadcasted_iota(jnp.int32, (8, LANES), 1)


def roll(x, shift):
    shift = shift % LANES
    return pltpu.roll(x, shift, 1) if shift else x


def two_parts(x):
    high = x.astype(bf16)
    return high, (x - high.astype(f32)).astype(bf16)


def three_parts(x):
    high = x.astype(bf16)
    return (high, *two_parts(x - high.astype(f32)))


def dot(a, b, over_a, over_b):
    return lax.dot_general(
        a, b, (((over_a,), (over_b,)), ((), ())), preferred_element_type=f32
    )


def fold(x):
    return x[:PAD] + x[PAD:]


def block_sums(dosage_ref, shares, freqs):
    qh, qm, ql = three_parts(shares)
    fh, fm, fl = three_parts(freqs)
    q_side = jnp.concatenate([qh, qh, qm, qh, ql, qm], 0)
    f_side = jnp.concatenate([fh, fm, fh, fl, fh, fm], 0)
    q_two = jnp.concatenate([qh, qm], 0)
    f_two = jnp.concatenate([fh, fm], 0)
    g_two = jnp.concatenate(two_parts(1.0 - freqs), 0)
    shift = 2 * lax.broadcasted_iota(jnp.int32, (16, freqs.shape[1]), 0)

    def ratios(at):
        probs = dot(q_side[:, at : at + ROWS], f_side, 0, 0)
        codes = jnp.concatenate(
            [
                jnp.bitwise_and(
                    jnp.right_shift(jnp.broadcast_to(dosage_ref[w : w + 1, :], shift.shape), shift), 3
                )
                for w in range(at // 16, (at + ROWS) // 16)
            ],
            0,
        )
        live = codes < 3
        allele = codes.astype(f32)
        ratio_alt = jnp.where(live, allele, 0.0) * (1.0 / probs)
        ratio_ref = jnp.where(live, 2.0 - allele, 0.0) * (1.0 / (1.0 - probs))
        return two_parts(ratio_alt) + two_parts(ratio_ref)

    sums_q, sum_a, sum_b = [], 0.0, 0.0
    starts = range(0, shares.shape[1], ROWS)
    ready = ratios(0)
    for at in starts:
        ah, al, bh, bl = ready
        if at + ROWS in starts:
            ready = ratios(at + ROWS)
        sums_q.append(
            dot(f_two, ah, 1, 1) + dot(f_two, al, 1, 1) + dot(g_two, bh, 1, 1) + dot(g_two, bl, 1, 1)
        )
        q_part = q_two[:, at : at + ROWS]
        sum_a = sum_a + (dot(q_part, ah, 1, 0) + dot(q_part, al, 1, 0))
        sum_b = sum_b + (dot(q_part, bh, 1, 0) + dot(q_part, bl, 1, 0))
    return fold(jnp.concatenate(sums_q, 1)), fold(sum_a), fold(sum_b)


def in_plane(y, g):
    return y * N_XC + g


def in_line(i, h):
    return i * N_ZH + h


def zq_of(idx):
    return (idx[0] >> 5) & 3


def near_of(idx):
    return ((idx[0] >> 1) & 6) | (idx[0] & 1)


def y_of(idx):
    return idx[0] >> 7


def halves(a, b):
    left = lax.broadcasted_iota(jnp.int32, a.shape, 1) < 64
    return jnp.where(left, a, roll(b, 64)), jnp.where(left, roll(a, 64), b)


def block_of_lane():
    return lax.broadcasted_iota(jnp.int32, (4, LANES), 1) // 16


def put_far(far_out, at, rows):
    for b in range(3):
        far_out[3 * at + b] = rows[2 * b : 2 * b + 2]


def get_far(far_in, at, pairs):
    return jnp.concatenate([far_in[3 * at + b] for b in range(pairs)], 0)


def first_kernel(idx, shares_ref, freqs_ref, far_out, q_out, f_tmp):
    raw = shares_ref[...]
    own = raw / jnp.sum(raw, axis=0, keepdims=True)
    q_out[...] = jnp.zeros_like(q_out)
    f_tmp[...] = jnp.zeros_like(f_tmp)
    q_out[0:6, 0:64] = own[0:6]
    q_out[0:6, 64:128] = own[6:12]
    for j in range(3):
        f_tmp[0:4, 16 * j : 16 * j + 16] = freqs_ref[4 * j : 4 * j + 4, :]
    turned = pltpu.roll(f_tmp[...], 16 * zl_of(idx), 1)
    for h in range(N_ZH):
        sent = jnp.where(zh_of(idx) == h, turned, q_out[...])
        for i in range(N_ZL):
            put_far(far_out, in_line(i, h) ^ FAR_1, sent)


def first_near_kernel(idx, far_in, q_in, near_out, f_out, q_tmp):
    zh = zh_of(idx)
    block = block_of_lane()
    freqs = [get_far(far_in, in_line(i, zh) ^ FAR_1, 2) for i in range(N_ZL)]
    for j in range(3):
        got = freqs[0]
        for i in range(1, N_ZL):
            got = jnp.where(block == (i + j) % 8, freqs[i], got)
        f_out[j] = roll(got, -16 * j)
    own, other = q_in[0:6], get_far(far_in, in_line(zl_of(idx), 1 - zh) ^ FAR_1, 3)
    q_tmp[0:6], q_tmp[6:12] = halves(jnp.where(zh == 0, own, other), jnp.where(zh == 0, other, own))
    for s in range(N_NEAR):
        near_out[3 * s : 3 * s + 3] = f_out[...]
    for g in range(N_XC):
        s = 3 * (in_plane(y_of(idx), g) ^ NEAR_1)
        for j in range(3):
            near_out[s + j] = q_tmp[4 * j : 4 * j + 4]


def shares_of(idx, near_in):
    rows = [[], [], []]
    for x in range(4):
        for j in range(3):
            a, b = (near_in[3 * (in_plane(y_of(idx), 2 * x + c) ^ NEAR_1) + j] for c in range(2))
            rows[j].extend(halves(a, b))
    return padded(rows)


def freqs_of(idx, near_in, f_in):
    rows = [[], [], []]
    for y in range(N_Y):
        for j in range(3):
            got = near_in[3 * (in_plane(y, near_of(idx)) ^ NEAR_1) + j]
            rows[j].append(jnp.where(y_of(idx) == y, f_in[j], got))
    return padded(rows)


def padded(rows):
    rows = [jnp.concatenate(row, 1) for row in rows]
    return jnp.concatenate([*rows, jnp.zeros_like(rows[0])], 0)


def turned_tiles(x):
    return jnp.concatenate([roll(x[:, tile(t)], 64) for t in range(x.shape[1] // LANES)], 1)


def left_of(rows):
    return lax.broadcasted_iota(jnp.int32, (rows, LANES), 1) < 64


def one_kernel(idx, dosage_ref, near_in, own_f_in, slots, q_out, f_out, sq_tmp, sa_tmp, sq_turn, sa_turn):
    shares = shares_of(idx, near_in)
    freqs = freqs_of(idx, near_in, own_f_in)
    q_out[...] = shares
    f_out[...] = freqs
    sum_q, sum_a, sum_b = block_sums(dosage_ref, shares, freqs)
    sq_tmp[...] = sum_q
    sa_tmp[0:12] = sum_a[0:12]
    sa_tmp[12:24] = sum_b[0:12]
    sq_turn[...] = turned_tiles(sum_q)
    sa_turn[...] = turned_tiles(sa_tmp[...])
    left = left_of(3)
    for w in range(N_WIDE):
        t, q = divmod(w, 4)
        a = (sq_turn if t % 2 else sq_tmp)[3 * q : 3 * q + 3, tile(t // 2)]
        t, q = divmod(w, 8)
        b = (sa_tmp if t % 2 else sa_turn)[3 * q : 3 * q + 3, tile(t // 2)]
        put_wide(slots, w ^ WIDE_1, jnp.where(left, a, b))


def put_wide(wide_out, at, rows):
    for r in range(3):
        wide_out[3 * at + r] = rows[r : r + 1]


def put_line(line_out, at, rows):
    for b in range(3):
        line_out[3 * at + b] = rows[4 * b : 4 * b + 4]


def wide_sums_kernel(idx, wide_in, line_out, q_out, a_tmp):
    left = left_of(1)
    for r in range(3):
        got = [[wide_in[3 * (in_plane(i, g) ^ WIDE_1) + r] for g in range(N_XC)] for i in range(N_ROW)]
        row_sums = [sum(row) for row in got]
        col_sums = [sum(row[g] for row in got) for g in range(N_XC)]
        for i in range(4):
            at = 3 * i + r
            q_out[at : at + 1] = jnp.where(left, row_sums[i], roll(row_sums[i + 4], 64))
            a_tmp[at : at + 1] = jnp.where(left, roll(col_sums[i], 64), col_sums[i + 4])
    for h in range(N_ZH):
        sent = jnp.where(zh_of(idx) == h, a_tmp[...], q_out[...])
        for i in range(N_ZQ):
            put_line(line_out, in_line(i, h) ^ LINE_1, sent)


def line_sums_kernel(idx, line_in, q_in, wide_out, q_tmp, a_tmp):
    zh = zh_of(idx)
    for b in range(3):
        a_tmp[4 * b : 4 * b + 4] = sum(line_in[3 * (in_line(i, zh) ^ LINE_1) + b] for i in range(N_ZQ))
        other = line_in[3 * (in_line(zq_of(idx), 1 - zh) ^ LINE_1) + b]
        q_tmp[4 * b : 4 * b + 4] = q_in[4 * b : 4 * b + 4] + other
    left = left_of(3)
    row_sums, col_sums = [], []
    for i in range(8):
        at = 3 * (i % 4)
        row_sums.append(roll(q_tmp[at : at + 3], 64 * (i // 4)))
        col_sums.append(roll(a_tmp[at : at + 3], 64 * (1 - i // 4)))
    for r in range(N_ROW):
        for g in range(N_XC):
            put_wide(wide_out, in_plane(r, g) ^ WIDE_2, jnp.where(left, row_sums[r], col_sums[g]))


def two_kernel(idx, dosage_ref, wide_in, q_in, f_in, near_out, sq_out, own_q, own_f, sq_tmp, sa_tmp, q_tmp, f_tmp):
    left = left_of(1)
    for t in range(8):
        for q in range(4):
            for r in range(3):
                a, b = (wide_in[3 * ((8 * t + 4 * half + q) ^ WIDE_2) + r] for half in range(2))
                sq_tmp[3 * q + r : 3 * q + r + 1, tile(t)] = jnp.where(left, a, roll(b, 64))
    for t in range(4):
        for q in range(8):
            for r in range(3):
                a, b = (wide_in[3 * ((16 * t + 8 * half + q) ^ WIDE_2) + r] for half in range(2))
                sa_tmp[3 * q + r : 3 * q + r + 1, tile(t)] = jnp.where(left, roll(a, 64), b)
    q_tmp[...] = q_in[...]
    f_tmp[...] = f_in[...]
    numer = q_tmp[0:12] * sq_tmp[0:12]
    q_tmp[0:12] = (numer + 0.5) / (jnp.sum(numer, axis=0, keepdims=True) + 0.5 * K)
    old = f_tmp[0:12]
    alt_part = old * sa_tmp[0:12]
    f_tmp[0:12] = (alt_part + 0.5) / (alt_part + (1.0 - old) * sa_tmp[12:24] + 1.0)

    t = pl.multiple_of((var_of(idx) >> 1) * LANES, LANES)
    even, odd = halves(q_tmp[0:6, pl.ds(t, LANES)], q_tmp[6:12, pl.ds(t, LANES)])
    own_q[...] = jnp.where((var_of(idx) & 1) == 0, even, odd)
    t = pl.multiple_of((smp_of(idx) >> 3) * LANES, LANES)
    block = block_of_lane()
    got = f_tmp[0:4, pl.ds(t, LANES)]
    for j in range(1, 3):
        got = jnp.where(
            block == ((zl_of(idx) + j) & 7), roll(f_tmp[4 * j : 4 * j + 4, pl.ds(t, LANES)], 16 * j), got
        )
    own_f[...] = got

    sum_q, sum_a, sum_b = block_sums(dosage_ref, q_tmp[...], f_tmp[...])
    for x in range(4):
        pair = halves(sum_q[:, tile(2 * x)], sum_q[:, tile(2 * x + 1)])
        for c in range(2):
            for y in range(N_Y):
                near_out[in_plane(y, 2 * x + c) ^ NEAR_2, 0:16] = pair[c]
    sq_out[...] = near_out[in_plane(0, near_of(idx)) ^ NEAR_2, 0:16]
    sa_tmp[0:12] = sum_a[0:12]
    sa_tmp[12:24] = sum_b[0:12]
    for y in range(N_Y):
        near_out[in_plane(y, near_of(idx)) ^ NEAR_2] = sa_tmp[:, tile(y)]


def last_far_kernel(idx, near_in, sq_in, far_out, q_out):
    zh, near = zh_of(idx), near_of(idx)
    sum_q = sq_in[...]
    for g in range(N_XC):
        got = near_in[in_plane(y_of(idx), g) ^ NEAR_2, 0:16]
        sum_q = sum_q + jnp.where(near == g, 0.0, got)
    sums = sum(near_in[in_plane(y, near) ^ NEAR_2] for y in range(N_Y))
    parts = halves(sum_q[0:6], sum_q[6:12])
    q_out[...] = jnp.where(zh == 0, parts[0], parts[1])
    block = block_of_lane()
    turned = [roll(sums[4 * j : 4 * j + 4], 16 * j) for j in range(6)]
    for i in range(N_ZL):
        got = turned[0]
        for j in range(1, 6):
            got = jnp.where(block == (i + j) % 8, turned[j], got)
        got = jnp.concatenate([got, got[0:2]], 0)
        for h in range(N_ZH):
            put_far(far_out, in_line(i, h) ^ FAR_2, jnp.where(zh == h, got, parts[h]))


def last_kernel(idx, far_in, sq_in, own_q, own_f, shares_out, freqs_out):
    zh = zh_of(idx)
    sum_q = sq_in[...] + get_far(far_in, in_line(zl_of(idx), 1 - zh) ^ FAR_2, 3)
    numer = own_q[...] * sum_q
    total = jnp.sum(numer, axis=0, keepdims=True)
    total = total + pltpu.roll(total, 64, 1)
    new = (numer + 0.5) / (total + 0.5 * K)
    shares_out[0:6] = new[:, 0:64]
    shares_out[6:12] = new[:, 64:128]
    sums = sum(get_far(far_in, in_line(i, zh) ^ FAR_2, 2) for i in range(N_ZL))
    alt_part = own_f[...] * sums
    ref_part = (1.0 - own_f[...]) * roll(sums, -48)
    new = (alt_part + 0.5) / (alt_part + ref_part + 1.0)
    new = pltpu.roll(jnp.concatenate([new, new], 0), (LANES - 16 * zl_of(idx)) & (LANES - 1), 1)
    for j in range(3):
        freqs_out[4 * j : 4 * j + 4] = new[0:4, 16 * j : 16 * j + 16]


def f32s(*shape):
    return jax.ShapeDtypeStruct(shape, f32)


def vmem(*shape):
    return pltpu.VMEM(shape, f32)


def call(kernel, scalars, n_in, outs, scratch, kept=True, ready=True):
    spec = pl.BlockSpec(memory_space=pltpu.VMEM)
    run = pl.pallas_call(
        kernel,
        in_specs=[pl.BlockSpec(memory_space=pltpu.SMEM)] * scalars + [spec] * n_in,
        out_specs=[spec] * len(outs),
        out_shape=[pltpu.VMEM(o.shape, o.dtype) for o in outs] if kept else outs,
        scratch_shapes=scratch,
    )

    def placed(*args):
        args = args[:scalars] + tuple(
            pltpu.with_memory_space_constraint(a, pltpu.VMEM) for a in args[scalars:]
        )
        return run(*args)

    return placed if ready else run


def exchange(x, axes, first):
    members = 1
    for axis in axes:
        members *= SIZES[AXES.index(axis)]
    order = [[i ^ first for i in range(members)]]
    return lax.all_to_all(x, axes, 0, 0, tiled=True, axis_index_groups=order)


def body(dosage, shares_init, freqs_init):
    idx = lax.axis_index(AXES).astype(jnp.int32).reshape(1)
    samples, variants = 16 * dosage.shape[0], dosage.shape[1]
    pairs = f32s(3 * N_FAR, 2, LANES)
    far_slots, own_q = call(first_kernel, 1, 2, [pairs, f32s(8, LANES)], [vmem(8, LANES)], ready=False)(
        idx, shares_init, freqs_init
    )
    far_got = exchange(far_slots, FAR, FAR_1)
    near_slots, own_f = call(
        first_near_kernel, 1, 2, [f32s(3 * N_NEAR, 4, LANES), f32s(3, 4, LANES)], [vmem(12, LANES)]
    )(idx, far_got, own_q)
    near_got = exchange(near_slots, NEAR, NEAR_1)
    slots, shares, freqs = call(
        one_kernel, 1, 3, [f32s(3 * N_WIDE, 1, LANES), f32s(PAD, samples), f32s(PAD, variants)],
        [vmem(PAD, samples), vmem(24, variants), vmem(PAD, samples), vmem(24, variants)],
    )(idx, dosage, near_got, own_f)
    wide_got = exchange(slots, WIDE, WIDE_1)
    line_slots, own_sum = call(
        wide_sums_kernel, 1, 1, [f32s(3 * N_LINE, 4, LANES), f32s(12, LANES)], [vmem(12, LANES)]
    )(idx, wide_got)
    line_got = exchange(line_slots, LINE, LINE_1)
    (wide_slots,) = call(
        line_sums_kernel, 1, 2, [f32s(3 * N_WIDE, 1, LANES)], [vmem(12, LANES), vmem(12, LANES)]
    )(idx, line_got, own_sum)
    wide_got = exchange(wide_slots, WIDE, WIDE_2)
    near_slots, own_sum, own_q, own_f = call(
        two_kernel, 1, 4,
        [f32s(N_NEAR, 24, LANES), f32s(PAD, LANES), f32s(6, LANES), f32s(4, LANES)],
        [vmem(PAD, samples), vmem(24, variants), vmem(PAD, samples), vmem(PAD, variants)],
    )(idx, dosage, wide_got, shares, freqs)
    near_got = exchange(near_slots, NEAR, NEAR_2)
    far_slots, own_sum = call(last_far_kernel, 1, 2, [pairs, f32s(6, LANES)], [])(
        idx, near_got, own_sum
    )
    far_got = exchange(far_slots, FAR, FAR_2)
    return tuple(
        call(last_kernel, 1, 4, [f32s(*shares_init.shape), f32s(*freqs_init.shape)], [], False)(
            idx, far_got, own_sum, own_q, own_f
        )
    )


def solution(mesh):
    fine = Mesh(mesh.devices.reshape(SIZES), AXES)
    return jax.shard_map(
        body,
        mesh=fine,
        in_specs=(P(SMP, VAR), P(None, SMP + VAR), P(None, VAR + SMP)),
        out_specs=(P(None, SMP + VAR), P(None, VAR + SMP)),
        check_vma=False,
    )
```
